128 devices in a mesh: batch: 4 (over y_hi, core), tm: 8 (over x, y_lo), space: 4 (over z).
Axes of the slice: x: 4, y: 4 (y_hi: 2, y_lo: 2; y = y_hi * 2 + y_lo), z: 4, core: 2. Of those that a mesh axis runs over, the one named last changes fastest.
Arguments:
- clip_tokens: bfloat16 [4, 16, 32, 32, 1024], P('batch', None, 'space', 'tm'), may hold values from -6 to 6
- frame_order: int32 [4, 16], P('batch'), may hold values from 0 to 15, each once within a row
- row_reach: int32 [4, 16], P('batch', 'tm'), may hold values from 1 to 4
- spatial_gain: float32 [1024], replicated, may hold values from 0.1 to 1.9
- spatial_heads: bfloat16 [1024, 3072], replicated, may hold values from -2 to 2
- spatial_merge: bfloat16 [1024, 1024], replicated, may hold values from -0.1875 to 0.1875
- temporal_gain: float32 [1024], replicated, may hold values from 0.1 to 1.9
- temporal_heads: bfloat16 [1024, 3072], replicated, may hold values from -2 to 2
- temporal_merge: bfloat16 [1024, 1024], replicated, may hold values from -0.1875 to 0.1875
- cotangent: bfloat16 [4, 16, 32, 32, 1024], P('batch', 'tm', 'space'), may hold values from -0.059814453 to 0.059814453
Outputs:
- output: bfloat16 [4, 16, 32, 32, 1024], P('batch', 'tm', 'space')
- weight_grad: float32 [1024, 1024], P(('tm', 'space'))
The draws below stay inside these ranges and needn't reach their ends.
Inputs may be any that keep to these rules, and one draw needn't show every extreme that they name: Each row of frame_order names every number from 0 to 15 once.
All inputs are finite; a program needn't handle non-finite values.
Results may differ from the reference program's by a relative error of at most 0.025.
Values may be sent and summed in bfloat16 or wider, within the bound.
No kernel may reach another device: no remote copies, remote signals or barrier semaphores. Data moves between devices by JAX's collectives and lax.ppermute only.
A program may use at most 128 MiB of HBM per device.

```python
import jax
import jax.numpy as jnp
from jax import lax

COLS = 32
HALO = 4
D = 1024
HEADS = 16
HEAD_DIM = 64
CLIPS = 4
FRAMES = 16
ROWS = 32


def projection_draw(key):
    key_one, key_two, key_three = jax.random.split(key, 3)
    plain_part = jnp.clip(jax.random.normal(key_one, (D, 3 * D), jnp.float32), -6.0, 6.0) * D ** (-0.5)
    return plain_part.astype(jnp.bfloat16)


def draw_spatial_heads(key, part):
    return projection_draw(jax.random.fold_in(key, 11))


def draw_temporal_heads(key, part):
    return projection_draw(jax.random.fold_in(key, 23))


def with_ends(drawn, own_key, smallest, high):
    index_at = [jax.random.randint(jax.random.fold_in(own_key, axis), (), 0, length) for axis, length in enumerate(drawn.shape)]
    longest = drawn.shape.index(max(drawn.shape))
    beside = index_at[:longest] + [(index_at[longest] + 1) % drawn.shape[longest]] + index_at[longest + 1:]
    return drawn.at[tuple(index_at)].set(smallest).at[tuple(beside)].set(high)


def block_levels(own_key, dims, cuts, low, high):
    factor_of, own = 1.0, jax.random.fold_in(own_key, 6)
    for dim, shards_of in cuts:
        steps = jnp.exp(jax.random.uniform(jax.random.fold_in(own, dim), (shards_of,), jnp.float32, low / len(cuts), high / len(cuts)))
        factor_of = factor_of * jnp.repeat(steps, dims[dim] // shards_of).reshape([-1 if axis == dim else 1 for axis in range(len(dims))])
    return factor_of


def gaussian(stream_key, extent, spread, bound, cuts=(), kind=jnp.bfloat16):
    entries = spread * jax.random.normal(stream_key, extent, jnp.float32)
    if cuts:
        entries = entries * block_levels(stream_key, extent, cuts, -0.22, 0.18)
    return jnp.clip(entries, -bound, bound).astype(kind)


def setup_inputs(seed: int = 0) -> dict:
    seeds = jax.random.split(jax.random.key(seed), 11)
    return {
        "clip_tokens": gaussian(seeds[0], (CLIPS, FRAMES, ROWS, COLS, D), 1.0, 6.0, ((0, 4), (2, 4), (3, 8))),
        "frame_order": jax.vmap(lambda own: jax.random.permutation(own, FRAMES))(jax.random.split(seeds[1], CLIPS)).reshape((CLIPS, FRAMES)).astype(jnp.int32),
        "row_reach": with_ends(jax.random.randint(seeds[2], (CLIPS, FRAMES), 1, HALO + 1), jax.random.fold_in(seeds[2], 1), 1, HALO).astype(jnp.int32),
        "spatial_gain": jnp.clip(1.0 + 0.18 * jax.random.normal(seeds[3], (D,), jnp.float32), 0.1, 1.9),
        "spatial_heads": draw_spatial_heads(jax.random.fold_in(seeds[10], 71), 0),
        "spatial_merge": gaussian(seeds[5], (D, D), D ** -0.5, 0.1875),
        "temporal_gain": jnp.clip(1.0 + 0.18 * jax.random.normal(seeds[6], (D,), jnp.float32), 0.1, 1.9),
        "temporal_heads": draw_temporal_heads(jax.random.fold_in(seeds[10], 71), 0),
        "temporal_merge": gaussian(seeds[8], (D, D), D ** -0.5, 0.1875),
        "cotangent": gaussian(seeds[9], (CLIPS, FRAMES, ROWS, COLS, D), 0.01, 0.059814453, ((0, 4), (1, 8), (2, 4))),
    }


floor_term = 0.5

def normalize(values, gain_vector):
    widened = values.astype(jnp.float32)
    scaled = widened * lax.rsqrt(lax.optimization_barrier(jnp.mean(widened * widened, axis=-1, keepdims=True)) + floor_term)
    return (scaled * gain_vector).astype(jnp.bfloat16)

def softmax_rounded(scores, allowed):
    masked = jnp.where(allowed, scores, -1e+30)
    top_score = lax.optimization_barrier(jnp.max(masked, axis=-1, keepdims=True))
    exponent = jnp.exp(masked - top_score)
    return (exponent / lax.optimization_barrier(jnp.sum(exponent, axis=-1, keepdims=True))).astype(jnp.bfloat16)

def spatial_frame(inputs):
    queries, keys_all, values_all, reach_now = inputs
    token_rows = jnp.arange(ROWS * COLS, dtype=jnp.int32) // COLS
    allowed = jnp.abs(token_rows[:, None] - token_rows[None, :]) <= reach_now
    query_heads = queries.astype(jnp.float32).reshape(-1, HEADS, HEAD_DIM)
    key_heads = keys_all.astype(jnp.float32).reshape(-1, HEADS, HEAD_DIM)
    value_heads = values_all.astype(jnp.float32).reshape(-1, HEADS, HEAD_DIM)
    scores = jnp.einsum('qhd,khd->hqk', query_heads, key_heads) * HEAD_DIM ** (-0.5)
    weights = softmax_rounded(scores, allowed[None])
    context = jnp.einsum('hqk,khd->qhd', weights.astype(jnp.float32), value_heads)
    return context.reshape(-1, D).astype(jnp.bfloat16)

def temporal_clip(queries, keys_all, values_all, order_row):
    query_heads = queries.astype(jnp.float32).reshape(FRAMES, -1, HEADS, HEAD_DIM)
    key_heads = keys_all.astype(jnp.float32).reshape(FRAMES, -1, HEADS, HEAD_DIM)
    value_heads = values_all.astype(jnp.float32).reshape(FRAMES, -1, HEADS, HEAD_DIM)
    scores = jnp.einsum('fthd,gthd->thfg', query_heads, key_heads) * HEAD_DIM ** (-0.5)
    allowed = order_row[None, :] <= order_row[:, None]
    weights = softmax_rounded(scores, allowed[None, None])
    context = jnp.einsum('thfg,gthd->fthd', weights.astype(jnp.float32), value_heads)
    return context.reshape(FRAMES, -1, D).astype(jnp.bfloat16)

def reference(clip_tokens, frame_order, row_reach, spatial_gain, spatial_heads, spatial_merge, temporal_gain, temporal_heads, temporal_merge, cotangent):
    tokens = ROWS * COLS

    def one_clip(running, inputs):
        frames_in, order_row, reach_row, cotangent_clip = inputs
        flat_input = frames_in.reshape(FRAMES, tokens, D)
        normed = normalize(flat_input, spatial_gain)
        projected = jnp.dot(normed, spatial_heads, preferred_element_type=jnp.float32).astype(jnp.bfloat16)
        spatial_context = lax.map(spatial_frame, (projected[..., :D], projected[..., D:2 * D], projected[..., 2 * D:], reach_row))
        middle = (flat_input.astype(jnp.float32) + jnp.dot(spatial_context, spatial_merge, preferred_element_type=jnp.float32)).astype(jnp.bfloat16)
        normed_two = normalize(middle, temporal_gain)
        projected_two = jnp.dot(normed_two, temporal_heads, preferred_element_type=jnp.float32).astype(jnp.bfloat16)
        temporal_context = temporal_clip(projected_two[..., :D], projected_two[..., D:2 * D], projected_two[..., 2 * D:], order_row)
        output_clip = (middle.astype(jnp.float32) + jnp.dot(temporal_context, temporal_merge, preferred_element_type=jnp.float32)).astype(jnp.bfloat16)
        gradient = running + lax.dot_general(temporal_context.reshape(-1, D), cotangent_clip.reshape(-1, D), (((0,), (0,)), ((), ())), preferred_element_type=jnp.float32)
        return (gradient, output_clip.reshape(FRAMES, ROWS, COLS, D))
    zero_grad = jnp.zeros((D, D), jnp.float32)
    weight_grad, output = lax.scan(one_clip, zero_grad, (clip_tokens, frame_order, row_reach, cotangent))
    return (output, weight_grad)
```

```python
import jax
import jax.numpy as jnp
from jax import lax
from jax.experimental import pallas as pl
from jax.experimental.pallas import tpu as pltpu
from jax.sharding import PartitionSpec as P

HALO = 4
D = 1024
HEADS = 16
HEAD_DIM = 64
PAIRS = HEADS // 2
WIDE = 2 * HEAD_DIM
FLOOR = 0.5
SCALE = HEAD_DIM ** (-0.5) * 1.4426950408889634
BF = jnp.bfloat16
F32 = jnp.float32
MASKED = -1e30


def normalized(x, gain):
    return x * lax.rsqrt(jnp.mean(x * x, axis=-1, keepdims=True) + FLOOR) * gain


def norm_kernel(x_ref, gain_ref, tok_ref, normed_ref):
    sources, _, rows, cols, _ = x_ref.shape
    gain = gain_ref[...]
    for r in range(rows):
        for s in range(sources):
            x = x_ref[s, 0, r]
            y = normalized(x.astype(F32), gain).astype(BF)
            tok_ref[0, r, s * cols:(s + 1) * cols, :] = x
            normed_ref[0, r, s * cols:(s + 1) * cols, :] = y


def norm_reorder(arrived, gain):
    sources, frames, rows, cols, _ = arrived.shape
    half = rows // 2
    wide = sources * cols
    out = pl.BlockSpec((1, half, wide, D), lambda f, h: (f, h, 0, 0))
    shape = jax.ShapeDtypeStruct((frames, rows, wide, D), BF)
    return pl.pallas_call(
        norm_kernel,
        grid=(frames, 2),
        in_specs=[
            pl.BlockSpec((sources, 1, half, cols, D), lambda f, h: (0, f, h, 0, 0)),
            pl.BlockSpec((1, D), lambda f, h: (0, 0)),
        ],
        out_specs=[out, out],
        out_shape=[shape, shape],
        name="norm_reorder",
    )(arrived, gain.reshape(1, D))


def pair_attention(q, k, v, bias):
    n = q.shape[0]
    lane = lax.broadcasted_iota(jnp.int32, (n, WIDE), 1)
    low = lane < HEAD_DIM
    zero = jnp.zeros_like(q)
    both = jnp.concatenate([jnp.where(low, q, zero), jnp.where(low, zero, q)], axis=0)
    scores = lax.dot_general(both, k, (((1,), (1,)), ((), ())), preferred_element_type=F32)
    scores = scores * SCALE + jnp.concatenate([bias, bias], axis=0)
    top = jnp.max(scores, axis=-1, keepdims=True)
    p = jnp.exp2(scores - top).astype(BF)
    widened = jnp.concatenate([v, jnp.ones_like(v)], axis=1)
    o = jnp.dot(p, widened, preferred_element_type=F32)
    o = o[:, :WIDE] / o[:, WIDE:]
    return jnp.where(low, o[:n], o[n:]).astype(BF)


def spatial_kernel(info_ref, qkv_ref, up_ref, down_ref, tok_ref, wk_ref, wv_ref, wm_ref, mid_ref,
                   k_ref, v_ref, ctx_ref, bias_ref, *, rows, all_rows):
    f = pl.program_id(0)
    reach = info_ref[f]
    first_row = info_ref[pl.num_programs(0)] * rows
    tokens = qkv_ref.shape[1]
    cols = tokens // rows
    edge = HALO * cols
    extent = tokens + 2 * edge
    halo = jnp.concatenate([up_ref[0], down_ref[0]], axis=0)
    for w_ref, buf, at in ((wk_ref, k_ref, D), (wv_ref, v_ref, 2 * D)):
        side = jnp.dot(halo, w_ref[...], preferred_element_type=F32).astype(BF)
        buf[0:edge] = side[:edge]
        buf[edge:edge + tokens] = qkv_ref[0, :, at:at + D]
        buf[edge + tokens:] = side[edge:]
    qrow = lax.broadcasted_iota(jnp.int32, (tokens, extent), 0) // cols
    krow = lax.broadcasted_iota(jnp.int32, (tokens, extent), 1) // cols - HALO
    allowed = (jnp.abs(krow - qrow) <= reach) & (krow + first_row >= 0) & (krow + first_row < all_rows)
    bias_ref[...] = jnp.where(allowed, 0.0, MASKED)
    for pair in range(PAIRS):
        at = slice(pair * WIDE, (pair + 1) * WIDE)
        half = tokens // 2
        for side in range(2):
            keys = slice(side * edge, side * edge + half + 2 * edge)
            own = slice(side * half, (side + 1) * half)
            ctx_ref[own, at] = pair_attention(qkv_ref[0, own, at], k_ref[keys, at], v_ref[keys, at], bias_ref[own, keys])
    mid = tok_ref[0].astype(F32) + jnp.dot(ctx_ref[...], wm_ref[...], preferred_element_type=F32)
    mid_ref[:, 0] = mid.astype(BF).reshape(rows, cols, D)


def spatial_phase(info, qkv, up, down, tok, heads, merge, rows, all_rows):
    import functools
    frames, tokens, _ = qkv.shape
    cols = tokens // rows
    edge = HALO * cols
    extent = tokens + 2 * edge
    per_frame = lambda n, d: pl.BlockSpec((1, n, d), lambda f, info: (f, 0, 0))
    column = lambda c: pl.BlockSpec((D, D), lambda f, info: (0, c))
    return pl.pallas_call(
        functools.partial(spatial_kernel, rows=rows, all_rows=all_rows),
        grid_spec=pltpu.PrefetchScalarGridSpec(
            num_scalar_prefetch=1,
            grid=(frames,),
            in_specs=[per_frame(tokens, 3 * D), per_frame(edge, D), per_frame(edge, D), per_frame(tokens, D),
                      column(1), column(2), column(0)],
            out_specs=pl.BlockSpec((rows, 1, cols, D), lambda f, info: (0, f, 0, 0)),
            scratch_shapes=[pltpu.VMEM((extent, D), BF), pltpu.VMEM((extent, D), BF),
                            pltpu.VMEM((tokens, D), BF), pltpu.VMEM((tokens, extent), F32)],
        ),
        out_shape=jax.ShapeDtypeStruct((rows, frames, cols, D), BF),
        compiler_params=pltpu.CompilerParams(vmem_limit_bytes=56 * 2**20),
        name="spatial_phase",
    )(info, qkv, up, down, tok, heads, heads, merge)


GROUP = 8


def temporal_kernel(core_ref, mid_ref, order_q_ref, order_k_ref, gain_ref, cot_ref, heads_ref, merge_ref,
                    out_ref, send_ref, keep_ref,
                    w_ref, wm_ref, normed_ref, q_ref, k_ref, v_ref, ctx_ref, cotb_ref, sems):
    frames, cols, _ = mid_ref.shape
    groups = cols // GROUP
    n = frames * GROUP
    copies = [pltpu.make_async_copy(heads_ref.at[:, i * D:(i + 1) * D], w_ref.at[i], sems.at[i]) for i in range(3)]
    copies.append(pltpu.make_async_copy(merge_ref, wm_ref, sems.at[3]))
    for c in copies:
        c.start()
    gain = gain_ref[...]
    for g in range(groups):
        x = mid_ref[:, g * GROUP:(g + 1) * GROUP, :].astype(F32).reshape(n, D)
        normed_ref[g * n:(g + 1) * n] = normalized(x, gain).astype(BF)
        cotb_ref[g * n:(g + 1) * n] = cot_ref[:, g * GROUP:(g + 1) * GROUP, :].astype(F32).reshape(n, D).astype(BF)
    for i, buf in enumerate((q_ref, k_ref, v_ref)):
        copies[i].wait()
        buf[...] = jnp.dot(normed_ref[...], w_ref[i], preferred_element_type=F32).astype(BF)
    place_q = lax.broadcasted_iota(jnp.int32, (n, n), 0) % GROUP
    place_k = lax.broadcasted_iota(jnp.int32, (n, n), 1) % GROUP
    allowed = (place_q == place_k) & (order_k_ref[...] <= order_q_ref[...])
    bias = jnp.where(allowed, 0.0, MASKED)
    for g in range(groups):
        own = slice(g * n, (g + 1) * n)
        for pair in range(PAIRS):
            at = slice(pair * WIDE, (pair + 1) * WIDE)
            ctx_ref[own, at] = pair_attention(q_ref[own, at], k_ref[own, at], v_ref[own, at], bias)
    core = core_ref[0]
    half = D // 2
    for ref, which in ((send_ref, 1 - core), (keep_ref, core)):
        cot = cotb_ref[:, pl.ds(pl.multiple_of(which * half, half), half)]
        grad = lax.dot_general(ctx_ref[...], cot, (((0,), (0,)), ((), ())), preferred_element_type=F32).astype(BF)
        spaces, times, block, _ = ref.shape
        for t in range(times):
            for s in range(spaces):
                row = (t * spaces + s) * block
                ref[s, t] = grad[row:row + block]
    copies[3].wait()
    for g in range(groups):
        y = jnp.dot(ctx_ref[g * n:(g + 1) * n], wm_ref[...], preferred_element_type=F32)
        x = mid_ref[:, g * GROUP:(g + 1) * GROUP, :].astype(F32) + y.reshape(frames, GROUP, D)
        out_ref[:, g * GROUP:(g + 1) * GROUP, :] = x.astype(BF)


def temporal_phase(core, mid, order, gain, cot, heads, merge, spaces, times):
    frames, cols, _ = mid.shape
    n = frames * GROUP
    tokens = frames * cols
    spread = jnp.repeat(order, GROUP)
    block = D // (spaces * times)
    part = jax.ShapeDtypeStruct((spaces, times, block, D // 2), BF)
    vmem = pl.BlockSpec(memory_space=pltpu.VMEM)
    hbm = pl.BlockSpec(memory_space=pl.ANY)
    return pl.pallas_call(
        temporal_kernel,
        in_specs=[pl.BlockSpec(memory_space=pltpu.SMEM), vmem, vmem, vmem, vmem, vmem, hbm, hbm],
        out_specs=[vmem, vmem, vmem],
        out_shape=[jax.ShapeDtypeStruct((frames, cols, D), BF), part, part],
        scratch_shapes=[pltpu.VMEM((3, D, D), BF), pltpu.VMEM((D, D), BF)]
        + [pltpu.VMEM((tokens, D), BF)] * 6
        + [pltpu.SemaphoreType.DMA((4,))],
        compiler_params=pltpu.CompilerParams(vmem_limit_bytes=56 * 2**20),
        name="temporal_phase",
    )(core, mid, spread.reshape(n, 1), spread.reshape(1, n), gain.reshape(1, D), cot, heads, merge)


def per_device(
    clip_tokens,
    frame_order,
    row_reach,
    spatial_gain,
    spatial_heads,
    spatial_merge,
    temporal_gain,
    temporal_heads,
    temporal_merge,
    cotangent,
):
    tm, space = lax.axis_size("tm"), lax.axis_size("space")
    _, frame_count, rows, cols, _ = clip_tokens.shape
    frames = frame_count // tm
    wide = tm * cols
    tokens = rows * wide
    exchange = lambda v, axis: lax.all_to_all(v, axis, split_axis=0, concat_axis=0, tiled=True)

    arrived = exchange(clip_tokens.reshape(tm, frames, rows, cols, D), "tm")
    cot = exchange(cotangent.reshape(frames, rows, wide, D).swapaxes(0, 1), "tm")
    tok, normed = norm_reorder(arrived, spatial_gain)
    up = [(i, i + 1) for i in range(space - 1)]
    down = [(j, i) for i, j in up]
    above = lax.ppermute(normed[:, rows - HALO:], "space", up)
    below = lax.ppermute(normed[:, :HALO], "space", down)
    qkv = jnp.dot(normed.reshape(frames * tokens, D), spatial_heads, preferred_element_type=F32).astype(BF)
    here = lax.axis_index("space").astype(jnp.int32)
    info = jnp.concatenate([row_reach.reshape(frames), here.reshape(1)])
    middle = spatial_phase(
        info,
        qkv.reshape(frames, tokens, 3 * D),
        above.reshape(frames, HALO * wide, D),
        below.reshape(frames, HALO * wide, D),
        tok.reshape(frames, tokens, D),
        spatial_heads,
        spatial_merge,
        rows,
        rows * space,
    )
    mid = exchange(middle, "tm").reshape(frame_count, wide, D)
    core = (lax.axis_index("batch") % 2).astype(jnp.int32).reshape(1)
    out, send, keep = temporal_phase(
        core, mid, frame_order.reshape(frame_count), temporal_gain, cot.reshape(frame_count, wide, D),
        temporal_heads, temporal_merge, space, tm,
    )
    batch = lax.axis_size("batch")
    got = lax.ppermute(send, "batch", [(i, i ^ 1) for i in range(batch)])
    output = exchange(out.reshape(tm, frames, wide, D), "tm").swapaxes(0, 1)
    chip = (keep.astype(F32) + got.astype(F32)).astype(BF)
    over_space = exchange(chip, "space").astype(F32).sum(0).astype(BF)
    over_tm = exchange(over_space, "tm").astype(F32).sum(0).astype(BF)
    block = over_tm.shape[0]
    parts = lax.all_gather(over_tm, "batch").astype(F32).reshape(batch // 2, 2, block, D // 2).sum(0)
    weight_grad = parts.swapaxes(0, 1).reshape(block, D)
    return (output.reshape(1, frames, rows, wide, D), weight_grad)


def solution(mesh):
    in_specs = (
        P("batch", None, "space", "tm", None),
        P("batch", None),
        P("batch", "tm"),
        P(),
        P(),
        P(),
        P(),
        P(),
        P(),
        P("batch", "tm", "space", None, None),
    )
    out_specs = (P("batch", "tm", "space", None, None), P(("tm", "space"), None))
    return jax.shard_map(
        per_device, mesh=mesh, in_specs=in_specs, out_specs=out_specs, check_vma=False
    )
```

```python
import functools

import jax
import jax.numpy as jnp
from jax import lax
from jax.experimental import pallas as pl
from jax.experimental.pallas import tpu as pltpu
from jax.sharding import PartitionSpec as P


HALO = 4
D = 1024
HEADS = 16
HEAD_DIM = 64
PAIRS = HEADS // 2
WIDE = 2 * HEAD_DIM
FLOOR = 0.5
SCALE = HEAD_DIM ** (-0.5) * 1.4426950408889634
BF = jnp.bfloat16
F32 = jnp.float32
MASKED = -1e30


def normalized(x, gain):
    return x * lax.rsqrt(jnp.mean(x * x, axis=-1, keepdims=True) + FLOOR) * gain


def in_vmem(x):
    return pltpu.with_memory_space_constraint(x, pltpu.VMEM)


def in_hbm(x):
    return pltpu.with_memory_space_constraint(x, pltpu.HBM)


VMEM = pl.BlockSpec(memory_space=pltpu.VMEM)
SMEM = pl.BlockSpec(memory_space=pltpu.SMEM)
HBM = pl.BlockSpec(memory_space=pltpu.HBM)


def norm_kernel(x_ref, gain_ref, tok_out, *refs):
    part_refs, (tok_ref, sems) = refs[:-2], refs[-2:]
    sources, frames, rows, cols, _ = x_ref.shape
    half = rows // 2
    gain = gain_ref[...]
    for f in range(frames):
        for h in range(2):
            part_ref = part_refs[2 * f + h]

            def one_row(r, carry):
                for s in range(sources):
                    x = x_ref[s, f, h * half + r]
                    y = normalized(x.astype(F32), gain).astype(BF)
                    tok_ref[f, h * half + r, s * cols:(s + 1) * cols, :] = x
                    part_ref[r, s * cols:(s + 1) * cols, :] = y
                return carry

            lax.fori_loop(0, half, one_row, 0)
        pltpu.make_async_copy(tok_ref.at[f], tok_out.at[f], sems.at[f]).start()
    for f in range(frames):
        pltpu.make_async_copy(tok_ref.at[f], tok_out.at[f], sems.at[f]).wait()


def norm_reorder(arrived, gain):
    sources, frames, rows, cols, _ = arrived.shape
    wide = sources * cols
    return pl.pallas_call(
        norm_kernel,
        in_specs=[VMEM, VMEM],
        out_specs=[HBM] + [VMEM] * (2 * frames),
        scratch_shapes=[pltpu.VMEM((frames, rows, wide, D), BF), pltpu.SemaphoreType.DMA((frames,))],
        out_shape=[pltpu.HBM((frames, rows, wide, D), BF)] + [pltpu.VMEM((rows // 2, wide, D), BF)] * (2 * frames),
        compiler_params=pltpu.CompilerParams(vmem_limit_bytes=8 * 2**20),
        name="norm_reorder",
    )(in_vmem(arrived), gain.reshape(1, D))


def column_copies(w_ref, buf, sems, columns):
    return [pltpu.make_async_copy(w_ref.at[:, c * D:(c + 1) * D], buf.at[i], sems.at[i]) for i, c in enumerate(columns)]


def qkv_kernel(*refs):
    parts, (w_ref, out_ref, x_ref, buf, y_ref, sems) = refs[:-6], refs[-6:]
    copies = column_copies(w_ref, buf, sems, range(3))
    for c in copies:
        c.start()
    n = parts[0].shape[0]
    for i, p in enumerate(parts):
        x_ref[i * n:(i + 1) * n] = p[...]
    for i, c in enumerate(copies):
        c.wait()
        y_ref[i] = jnp.dot(x_ref[...], buf[i], preferred_element_type=F32).astype(BF)
        pltpu.make_async_copy(y_ref.at[i], out_ref.at[i], sems.at[3 + i]).start()
    for i in range(3):
        pltpu.make_async_copy(y_ref.at[i], out_ref.at[i], sems.at[3 + i]).wait()


def qkv_own(parts, heads):
    n = parts[0].shape[0]
    tokens = n * len(parts)
    return pl.pallas_call(
        qkv_kernel,
        in_specs=[VMEM] * len(parts) + [HBM],
        out_specs=HBM,
        out_shape=pltpu.HBM((3, tokens, D), BF),
        scratch_shapes=[pltpu.VMEM((tokens, D), BF), pltpu.VMEM((3, D, D), BF), pltpu.VMEM((3, tokens, D), BF),
                        pltpu.SemaphoreType.DMA((6,))],
        compiler_params=pltpu.CompilerParams(vmem_limit_bytes=24 * 2**20),
        name="qkv_own",
    )(*[in_vmem(p) for p in parts], in_hbm(heads))


def pair_attention(q, k, v, bias):
    n = q.shape[0]
    lane = lax.broadcasted_iota(jnp.int32, (n, WIDE), 1)
    low = lane < HEAD_DIM
    zero = jnp.zeros_like(q)
    both = jnp.concatenate([jnp.where(low, q, zero), jnp.where(low, zero, q)], axis=0)
    scores = lax.dot_general(both, k, (((1,), (1,)), ((), ())), preferred_element_type=F32)
    scores = scores * SCALE + jnp.concatenate([bias, bias], axis=0)
    top = jnp.max(scores, axis=-1, keepdims=True)
    p = jnp.exp2(scores - top).astype(BF)
    widened = jnp.concatenate([v, jnp.ones_like(v)], axis=1)
    o = jnp.dot(p, widened, preferred_element_type=F32)
    o = o[:, :WIDE] / o[:, WIDE:]
    return jnp.where(low, o[:n], o[n:]).astype(BF)


def spatial_kernel(*refs, frame, rows, all_rows):
    info_ref, up_ref, down_ref, qkv_ref, tok_ref, w_ref, wm_ref = refs[:7]
    mid_out, q_buf, tok_buf, mid_buf, wkv_buf, wm_buf, k_ref, v_ref, ctx_ref, bias_ref, sems = refs[-11:]
    tokens = ctx_ref.shape[0]
    copies = column_copies(w_ref, wkv_buf, sems, (1, 2))
    cols = tokens // rows
    edge = HALO * cols
    mine = pl.ds(frame * tokens, tokens)
    for i, buf in enumerate((q_buf, k_ref.at[edge:edge + tokens], v_ref.at[edge:edge + tokens])):
        copies.append(pltpu.make_async_copy(qkv_ref.at[i, mine], buf, sems.at[5 + i]))
    copies.append(pltpu.make_async_copy(wm_ref, wm_buf, sems.at[3]))
    copies.append(pltpu.make_async_copy(tok_ref.at[frame], tok_buf, sems.at[4]))
    for c in copies:
        c.start()
    reach = info_ref[frame]
    first_row = info_ref[info_ref.shape[0] - 1] * rows
    extent = tokens + 2 * edge
    qrow = lax.broadcasted_iota(jnp.int32, (tokens, extent), 0) // cols
    krow = lax.broadcasted_iota(jnp.int32, (tokens, extent), 1) // cols - HALO
    allowed = (jnp.abs(krow - qrow) <= reach) & (krow + first_row >= 0) & (krow + first_row < all_rows)
    bias_ref[...] = jnp.where(allowed, 0.0, MASKED)
    halo = jnp.concatenate([up_ref[...], down_ref[...]], axis=0)
    for i, buf in enumerate((k_ref, v_ref)):
        copies[i].wait()
        side = jnp.dot(halo, wkv_buf[i], preferred_element_type=F32).astype(BF)
        buf[0:edge] = side[:edge]
        buf[edge + tokens:] = side[edge:]
    for c in copies[2:5]:
        c.wait()
    half = tokens // 2
    for pair in range(PAIRS):
        at = slice(pair * WIDE, (pair + 1) * WIDE)
        for side in range(2):
            keys = slice(side * edge, side * edge + half + 2 * edge)
            own = slice(side * half, (side + 1) * half)
            ctx_ref[own, at] = pair_attention(q_buf[own, at], k_ref[keys, at], v_ref[keys, at], bias_ref[own, keys])
    copies[5].wait()
    copies[6].wait()
    mid = tok_buf[...].reshape(tokens, D).astype(F32) + jnp.dot(ctx_ref[...], wm_buf[...], preferred_element_type=F32)
    mid_buf[...] = mid.astype(BF).reshape(rows, cols, D)
    out = pltpu.make_async_copy(mid_buf, mid_out.at[:, frame], sems.at[8])
    out.start()
    out.wait()


def spatial_phase(info, qkv, halos, tok, heads, merge, all_rows):
    frames, rows, cols, _ = tok.shape
    tokens = rows * cols
    extent = tokens + 2 * HALO * cols
    mid = None
    for f in range(frames):
        up, down = halos[f]
        operands = [info, in_vmem(up), in_vmem(down)] + [in_hbm(v) for v in (qkv, tok, heads, merge)]
        specs = [SMEM, VMEM, VMEM, HBM, HBM, HBM, HBM]
        if mid is not None:
            operands.append(in_hbm(mid))
            specs.append(HBM)
        mid = pl.pallas_call(
            functools.partial(spatial_kernel, frame=f, rows=rows, all_rows=all_rows),
            in_specs=specs,
            out_specs=HBM,
            out_shape=pltpu.HBM((rows, frames, cols, D), BF),
            scratch_shapes=[pltpu.VMEM((tokens, D), BF), pltpu.VMEM((rows, cols, D), BF), pltpu.VMEM((rows, cols, D), BF),
                            pltpu.VMEM((2, D, D), BF), pltpu.VMEM((D, D), BF),
                            pltpu.VMEM((extent, D), BF), pltpu.VMEM((extent, D), BF),
                            pltpu.VMEM((tokens, D), BF), pltpu.VMEM((tokens, extent), F32),
                            pltpu.SemaphoreType.DMA((9,))],
            input_output_aliases={} if f == 0 else {len(operands) - 1: 0},
            compiler_params=pltpu.CompilerParams(vmem_limit_bytes=32 * 2**20),
            name="spatial_phase",
        )(*operands)
    return mid


GROUP = 8


def temporal_kernel(core_ref, mid_ref, order_q_ref, order_k_ref, gain_ref, cot_ref, w_ref, wm_ref,
                    out_hbm, send_ref, keep_hbm,
                    out_ref, keep_ref, wqkv_buf, wm_buf, cot_buf, normed_ref, q_ref, k_ref, v_ref, ctx_ref, cotb_ref, sems):
    frames, cols, _ = mid_ref.shape
    groups = cols // GROUP
    n = frames * GROUP
    copies = column_copies(w_ref, wqkv_buf, sems, range(3))
    copies.append(pltpu.make_async_copy(cot_ref, cot_buf, sems.at[3]))
    copies.append(pltpu.make_async_copy(wm_ref, wm_buf, sems.at[4]))
    for c in copies:
        c.start()
    gain = gain_ref[...]
    for g in range(groups):
        x = mid_ref[:, g * GROUP:(g + 1) * GROUP, :].astype(F32).reshape(n, D)
        normed_ref[g * n:(g + 1) * n] = normalized(x, gain).astype(BF)
    for i, buf in enumerate((q_ref, k_ref, v_ref)):
        copies[i].wait()
        buf[...] = jnp.dot(normed_ref[...], wqkv_buf[i], preferred_element_type=F32).astype(BF)
    copies[3].wait()
    for g in range(groups):
        cotb_ref[g * n:(g + 1) * n] = cot_buf[:, g * GROUP:(g + 1) * GROUP, :].astype(F32).reshape(n, D).astype(BF)
    place_q = lax.broadcasted_iota(jnp.int32, (n, n), 0) % GROUP
    place_k = lax.broadcasted_iota(jnp.int32, (n, n), 1) % GROUP
    allowed = (place_q == place_k) & (order_k_ref[...] <= order_q_ref[...])
    bias = jnp.where(allowed, 0.0, MASKED)
    for g in range(groups):
        own = slice(g * n, (g + 1) * n)
        for pair in range(PAIRS):
            at = slice(pair * WIDE, (pair + 1) * WIDE)
            ctx_ref[own, at] = pair_attention(q_ref[own, at], k_ref[own, at], v_ref[own, at], bias)
    core = core_ref[0]
    here = core_ref[1]
    half = D // 2
    for ref, which in ((send_ref, 1 - core), (keep_ref, core)):
        cot = cotb_ref[:, pl.ds(pl.multiple_of(which * half, half), half)]
        grad = lax.dot_general(ctx_ref[...], cot, (((0,), (0,)), ((), ())), preferred_element_type=F32).astype(BF)
        spaces, times, block, _ = ref.shape
        for s in range(spaces):
            slot = lax.rem(s + spaces - here, spaces)
            for t in range(times):
                row = (t * spaces + s) * block
                ref[slot, t] = grad[row:row + block]
    kept = pltpu.make_async_copy(keep_ref, keep_hbm, sems.at[5])
    kept.start()
    copies[4].wait()
    y = jnp.dot(ctx_ref[...], wm_buf[...], preferred_element_type=F32)
    for g in range(groups):
        x = mid_ref[:, g * GROUP:(g + 1) * GROUP, :].astype(F32) + y[g * n:(g + 1) * n].reshape(frames, GROUP, D)
        out_ref[:, g * GROUP:(g + 1) * GROUP, :] = x.astype(BF)
    done = pltpu.make_async_copy(out_ref, out_hbm, sems.at[6])
    done.start()
    done.wait()
    kept.wait()


def temporal_phase(core, mid, order, gain, cot, heads, merge, spaces, times):
    frames, cols, _ = mid.shape
    n = frames * GROUP
    tokens = frames * cols
    spread = jnp.repeat(order, GROUP)
    block = D // (spaces * times)
    part = (spaces, times, block, D // 2)
    return pl.pallas_call(
        temporal_kernel,
        in_specs=[SMEM] + [VMEM] * 4 + [HBM] * 3,
        out_specs=[HBM, VMEM, HBM],
        out_shape=[pltpu.HBM((frames, cols, D), BF), pltpu.VMEM(part, BF), pltpu.HBM(part, BF)],
        scratch_shapes=[pltpu.VMEM((frames, cols, D), BF), pltpu.VMEM(part, BF), pltpu.VMEM((3, D, D), BF), pltpu.VMEM((D, D), BF), pltpu.VMEM((frames, cols, D), BF)]
        + [pltpu.VMEM((tokens, D), BF)] * 6
        + [pltpu.SemaphoreType.DMA((7,))],
        compiler_params=pltpu.CompilerParams(vmem_limit_bytes=40 * 2**20),
        name="temporal_phase",
    )(core, in_vmem(mid), spread.reshape(n, 1), spread.reshape(1, n), gain.reshape(1, D),
      in_hbm(cot), in_hbm(heads), in_hbm(merge))


def per_device(
    clip_tokens,
    frame_order,
    row_reach,
    spatial_gain,
    spatial_heads,
    spatial_merge,
    temporal_gain,
    temporal_heads,
    temporal_merge,
    cotangent,
):
    tm, space = lax.axis_size("tm"), lax.axis_size("space")
    _, frame_count, rows, cols, _ = clip_tokens.shape
    frames = frame_count // tm
    wide = tm * cols
    exchange = lambda v, axis: lax.all_to_all(v, axis, split_axis=0, concat_axis=0, tiled=True)

    arrived = exchange(clip_tokens.reshape(tm, frames, rows, cols, D), "tm")
    cot = cotangent.reshape(frames, rows, wide, D).swapaxes(0, 1)
    tok, *parts = norm_reorder(arrived, spatial_gain)
    up = [(i, i + 1) for i in range(space - 1)]
    down = [(j, i) for i, j in up]
    edge = HALO * wide
    halos = []
    for f in range(frames):
        above = lax.ppermute(parts[2 * f + 1], "space", up)
        below = lax.ppermute(parts[2 * f], "space", down)
        halos.append((above.reshape(edge, D), below.reshape(edge, D)))
    qkv = qkv_own([p.reshape(edge, D) for p in parts], spatial_heads)
    cot, qkv = lax.optimization_barrier((cot, qkv))
    cot = exchange(cot, "tm")
    here = lax.axis_index("space").astype(jnp.int32)
    info = jnp.concatenate([row_reach.reshape(frames), here.reshape(1)])
    middle = spatial_phase(info, qkv, halos, tok, spatial_heads, spatial_merge, rows * space)
    mid = exchange(middle, "tm").reshape(frame_count, wide, D)
    core = jnp.stack([lax.axis_index("batch") & 1, here]).astype(jnp.int32)
    out, send, keep = temporal_phase(
        core, mid, frame_order.reshape(frame_count), temporal_gain, cot.reshape(frame_count, wide, D),
        temporal_heads, temporal_merge, space, tm,
    )
    batch = lax.axis_size("batch")
    got = lax.ppermute(send, "batch", [(i, i ^ 1) for i in range(batch)])
    output = exchange(out.reshape(tm, frames, wide, D), "tm").swapaxes(0, 1)
    chip = [keep[k].astype(F32) + got[k].astype(F32) for k in range(space)]
    total = chip[0]
    moved = [lax.ppermute(chip[k].astype(BF), "space", [(i, (i + k) % space) for i in range(space)])
             for k in range(1, space)]
    for part in moved:
        total = total + part.astype(F32)
    over_space = total.astype(BF)
    over_tm = exchange(over_space, "tm")
    over_tm = over_tm.astype(F32).sum(0).astype(BF)
    block = over_tm.shape[0]
    parts = lax.all_gather(over_tm, "batch").astype(F32).reshape(batch // 2, 2, block, D // 2).sum(0)
    weight_grad = parts.swapaxes(0, 1).reshape(block, D)
    return (output.reshape(1, frames, rows, wide, D), weight_grad)


def solution(mesh):
    in_specs = (
        P("batch", None, "space", "tm", None),
        P("batch", None),
        P("batch", "tm"),
        P(),
        P(),
        P(),
        P(),
        P(),
        P(),
        P("batch", "tm", "space", None, None),
    )
    out_specs = (P("batch", "tm", "space", None, None), P(("tm", "space"), None))

    return jax.shard_map(per_device, mesh=mesh, in_specs=in_specs, out_specs=out_specs, check_vma=False)
```

```python
import functools

import jax
import jax.numpy as jnp
from jax import lax
from jax.experimental import pallas as pl
from jax.experimental.pallas import tpu as pltpu
from jax.sharding import PartitionSpec as P


HALO = 4
D = 1024
HEADS = 16
HEAD_DIM = 64
PAIRS = HEADS // 2
WIDE = 2 * HEAD_DIM
FLOOR = 0.5
SCALE = HEAD_DIM ** (-0.5) * 1.4426950408889634
BF = jnp.bfloat16
F32 = jnp.float32
MASKED = -1e30


def normalized(x, gain):
    return x * lax.rsqrt(jnp.mean(x * x, axis=-1, keepdims=True) + FLOOR) * gain


def in_vmem(x):
    return pltpu.with_memory_space_constraint(x, pltpu.VMEM)


def in_hbm(x):
    return pltpu.with_memory_space_constraint(x, pltpu.HBM)


VMEM = pl.BlockSpec(memory_space=pltpu.VMEM)
SMEM = pl.BlockSpec(memory_space=pltpu.SMEM)
HBM = pl.BlockSpec(memory_space=pltpu.HBM)


def norm_kernel(x_ref, gain_ref, tok_out, low_ref, high_ref, tok_ref, sems):
    sources, frames, rows, cols, _ = x_ref.shape
    half = rows // 2
    gain = gain_ref[...]
    for f in range(frames):
        for h, part_ref in enumerate((low_ref, high_ref)):

            def one_row(r, carry):
                for s in range(sources):
                    x = x_ref[s, f, h * half + r]
                    y = normalized(x.astype(F32), gain).astype(BF)
                    tok_ref[f, h * half + r, s * cols:(s + 1) * cols, :] = x
                    part_ref[f, r, s * cols:(s + 1) * cols, :] = y
                return carry

            lax.fori_loop(0, half, one_row, 0)
        pltpu.make_async_copy(tok_ref.at[f], tok_out.at[f], sems.at[f]).start()
    for f in range(frames):
        pltpu.make_async_copy(tok_ref.at[f], tok_out.at[f], sems.at[f]).wait()


def norm_reorder(arrived, gain):
    sources, frames, rows, cols, _ = arrived.shape
    wide = sources * cols
    return pl.pallas_call(
        norm_kernel,
        in_specs=[VMEM, VMEM],
        out_specs=[HBM, VMEM, VMEM],
        scratch_shapes=[pltpu.VMEM((frames, rows, wide, D), BF), pltpu.SemaphoreType.DMA((frames,))],
        out_shape=[pltpu.HBM((frames, rows, wide, D), BF)] + [pltpu.VMEM((frames, rows // 2, wide, D), BF)] * 2,
        compiler_params=pltpu.CompilerParams(vmem_limit_bytes=8 * 2**20),
        name="norm_reorder",
    )(in_vmem(arrived), gain.reshape(1, D))


def column_copies(w_ref, buf, sems, columns):
    return [pltpu.make_async_copy(w_ref.at[:, c * D:(c + 1) * D], buf.at[i], sems.at[i]) for i, c in enumerate(columns)]


def qkv_kernel(low_ref, high_ref, w_ref, out_ref, x_ref, buf, y_ref, sems):
    copies = column_copies(w_ref, buf, sems, range(3))
    for c in copies:
        c.start()
    frames, edge, _ = low_ref.shape
    for f in range(frames):
        for h, part in enumerate((low_ref, high_ref)):
            at = (2 * f + h) * edge
            x_ref[at:at + edge] = part[f]
    for i, c in enumerate(copies):
        c.wait()
        y_ref[i] = jnp.dot(x_ref[...], buf[i], preferred_element_type=F32).astype(BF)
        pltpu.make_async_copy(y_ref.at[i], out_ref.at[i], sems.at[3 + i]).start()
    for i in range(3):
        pltpu.make_async_copy(y_ref.at[i], out_ref.at[i], sems.at[3 + i]).wait()


def qkv_own(low, high, heads):
    frames, edge, _ = low.shape
    tokens = 2 * frames * edge
    return pl.pallas_call(
        qkv_kernel,
        in_specs=[VMEM, VMEM, HBM],
        out_specs=HBM,
        out_shape=pltpu.HBM((3, tokens, D), BF),
        scratch_shapes=[pltpu.VMEM((tokens, D), BF), pltpu.VMEM((3, D, D), BF), pltpu.VMEM((3, tokens, D), BF),
                        pltpu.SemaphoreType.DMA((6,))],
        compiler_params=pltpu.CompilerParams(vmem_limit_bytes=24 * 2**20),
        name="qkv_own",
    )(in_vmem(low), in_vmem(high), in_hbm(heads))


def staged_attention(items):
    n = items[0][0]().shape[0]
    low = lax.broadcasted_iota(jnp.int32, (n, WIDE), 1) < HEAD_DIM
    scores, weights = [], []
    for q, k, v, bias, ref, at in items:
        q = q()
        zero = jnp.zeros_like(q)
        both = jnp.concatenate([jnp.where(low, q, zero), jnp.where(low, zero, q)], axis=0)
        scores.append(lax.dot_general(both, k(), (((1,), (1,)), ((), ())), preferred_element_type=F32))
    for s, (q, k, v, bias, ref, at) in zip(scores, items):
        b = bias()
        s = s * SCALE + jnp.concatenate([b, b], axis=0)
        weights.append(jnp.exp2(s - jnp.max(s, axis=-1, keepdims=True)).astype(BF))
    for p, (q, k, v, bias, ref, at) in zip(weights, items):
        v = v()
        o = jnp.dot(p, jnp.concatenate([v, jnp.ones_like(v)], axis=1), preferred_element_type=F32)
        o = o[:, :WIDE] / o[:, WIDE:]
        ref[at] = jnp.where(low, o[:n], o[n:]).astype(BF)


def reader(ref, *at):
    return lambda: ref[at]


SPATIAL_STAGE = 4
TEMPORAL_STAGE = 8


def spatial_kernel(info_ref, up_ref, down_ref, qkv_ref, tok_ref, w_ref, wm_ref, mid_out,
                   q_ref, tok_buf, mid_buf, wkv_buf, wm_buf, k_ref, v_ref, ctx_ref, bias_ref, sems, *, rows, all_rows):
    frames, extent, _ = k_ref.shape
    tokens = ctx_ref.shape[0] // frames
    cols = tokens // rows
    edge = HALO * cols
    weights = column_copies(w_ref, wkv_buf, sems, (1, 2))
    own = [pltpu.make_async_copy(qkv_ref.at[0], q_ref, sems.at[2])]
    for f in range(frames):
        mine = pl.ds(f * tokens, tokens)
        for i, buf in ((1, k_ref), (2, v_ref)):
            own.append(pltpu.make_async_copy(qkv_ref.at[i, mine], buf.at[f, edge:edge + tokens], sems.at[2 + 2 * f + i]))
    last = [pltpu.make_async_copy(wm_ref, wm_buf, sems.at[7]), pltpu.make_async_copy(tok_ref, tok_buf, sems.at[8])]
    for c in weights + own + last:
        c.start()
    first_row = info_ref[frames] * rows
    qrow = lax.broadcasted_iota(jnp.int32, (tokens, extent), 0) // cols
    krow = lax.broadcasted_iota(jnp.int32, (tokens, extent), 1) // cols - HALO
    inside = (krow + first_row >= 0) & (krow + first_row < all_rows)
    distance = jnp.where(inside, jnp.abs(krow - qrow), all_rows)
    for f in range(frames):
        bias_ref[f] = jnp.where(distance <= info_ref[f], 0.0, MASKED)
    halo = jnp.concatenate([up_ref[...].reshape(frames * edge, D), down_ref[...].reshape(frames * edge, D)], axis=0)
    for c, w, buf in zip(weights, range(2), (k_ref, v_ref)):
        c.wait()
        side = jnp.dot(halo, wkv_buf[w], preferred_element_type=F32).astype(BF)
        for f in range(frames):
            buf[f, 0:edge] = side[f * edge:(f + 1) * edge]
            buf[f, edge + tokens:] = side[(frames + f) * edge:(frames + f + 1) * edge]
    for c in own:
        c.wait()
    half = tokens // 2
    items = []
    for f in range(frames):
        for pair in range(PAIRS):
            at = slice(pair * WIDE, (pair + 1) * WIDE)
            for side in range(2):
                keys = slice(side * edge, side * edge + half + 2 * edge)
                rows_in = slice(side * half, (side + 1) * half)
                mine = slice(f * tokens + side * half, f * tokens + (side + 1) * half)
                items.append((reader(q_ref, mine, at), reader(k_ref, f, keys, at), reader(v_ref, f, keys, at),
                              reader(bias_ref, f, rows_in, keys), ctx_ref, (mine, at)))
    for i in range(0, len(items), SPATIAL_STAGE):
        staged_attention(items[i:i + SPATIAL_STAGE])
    for c in last:
        c.wait()
    sent = []
    for f in range(frames):
        mid = jnp.dot(ctx_ref[f * tokens:(f + 1) * tokens], wm_buf[...], preferred_element_type=F32)
        mid = mid + tok_buf[f].reshape(tokens, D).astype(F32)
        mid_buf[:, f] = mid.astype(BF).reshape(rows, cols, D)
        sent.append(pltpu.make_async_copy(mid_buf.at[:, f], mid_out.at[:, f], sems.at[9 + f]))
        sent[f].start()
    for c in sent:
        c.wait()


def spatial_phase(info, up, down, qkv, tok, heads, merge, all_rows):
    frames, rows, cols, _ = tok.shape
    tokens = rows * cols
    extent = tokens + 2 * HALO * cols
    return pl.pallas_call(
        functools.partial(spatial_kernel, rows=rows, all_rows=all_rows),
        in_specs=[SMEM, VMEM, VMEM, HBM, HBM, HBM, HBM],
        out_specs=HBM,
        out_shape=pltpu.HBM((rows, frames, cols, D), BF),
        scratch_shapes=[pltpu.VMEM((frames * tokens, D), BF), pltpu.VMEM((frames, rows, cols, D), BF),
                        pltpu.VMEM((rows, frames, cols, D), BF),
                        pltpu.VMEM((2, D, D), BF), pltpu.VMEM((D, D), BF),
                        pltpu.VMEM((frames, extent, D), BF), pltpu.VMEM((frames, extent, D), BF),
                        pltpu.VMEM((frames * tokens, D), BF), pltpu.VMEM((frames, tokens, extent), F32),
                        pltpu.SemaphoreType.DMA((9 + frames,))],
        compiler_params=pltpu.CompilerParams(vmem_limit_bytes=40 * 2**20),
        name="spatial_phase",
    )(info, in_vmem(up), in_vmem(down), *[in_hbm(v) for v in (qkv, tok, heads, merge)])


GROUP = 8


def temporal_kernel(core_ref, mid_ref, order_q_ref, order_k_ref, gain_ref, cot_ref, w_ref, wm_ref,
                    out_hbm, send_ref, keep_hbm,
                    out_ref, keep_ref, wqkv_buf, wm_buf, cot_buf, normed_ref, q_ref, k_ref, v_ref, ctx_ref, cotb_ref, sems):
    frames, cols, _ = mid_ref.shape
    groups = cols // GROUP
    n = frames * GROUP
    copies = column_copies(w_ref, wqkv_buf, sems, range(3))
    copies.append(pltpu.make_async_copy(cot_ref, cot_buf, sems.at[3]))
    copies.append(pltpu.make_async_copy(wm_ref, wm_buf, sems.at[4]))
    for c in copies:
        c.start()
    gain = gain_ref[...]
    for g in range(groups):
        x = mid_ref[:, g * GROUP:(g + 1) * GROUP, :].astype(F32).reshape(n, D)
        normed_ref[g * n:(g + 1) * n] = normalized(x, gain).astype(BF)
    for i, buf in enumerate((q_ref, k_ref, v_ref)):
        copies[i].wait()
        buf[...] = jnp.dot(normed_ref[...], wqkv_buf[i], preferred_element_type=F32).astype(BF)
    copies[3].wait()
    for g in range(groups):
        cotb_ref[g * n:(g + 1) * n] = cot_buf[:, g * GROUP:(g + 1) * GROUP, :].astype(F32).reshape(n, D).astype(BF)
    place_q = lax.broadcasted_iota(jnp.int32, (n, n), 0) % GROUP
    place_k = lax.broadcasted_iota(jnp.int32, (n, n), 1) % GROUP
    allowed = (place_q == place_k) & (order_k_ref[...] <= order_q_ref[...])
    bias = jnp.where(allowed, 0.0, MASKED)
    items = []
    for g in range(groups):
        own = slice(g * n, (g + 1) * n)
        for pair in range(PAIRS):
            at = slice(pair * WIDE, (pair + 1) * WIDE)
            items.append((reader(q_ref, own, at), reader(k_ref, own, at), reader(v_ref, own, at), lambda: bias,
                          ctx_ref, (own, at)))
    for i in range(0, len(items), TEMPORAL_STAGE):
        staged_attention(items[i:i + TEMPORAL_STAGE])
    core = core_ref[0]
    here = core_ref[1]
    half = D // 2
    for ref, which in ((send_ref, 1 - core), (keep_ref, core)):
        cot = cotb_ref[:, pl.ds(pl.multiple_of(which * half, half), half)]
        grad = lax.dot_general(ctx_ref[...], cot, (((0,), (0,)), ((), ())), preferred_element_type=F32).astype(BF)
        spaces, times, block, _ = ref.shape
        for s in range(spaces):
            slot = lax.rem(s + spaces - here, spaces)
            for t in range(times):
                row = (t * spaces + s) * block
                ref[slot, t] = grad[row:row + block]
    kept = pltpu.make_async_copy(keep_ref, keep_hbm, sems.at[5])
    kept.start()
    copies[4].wait()
    y = jnp.dot(ctx_ref[...], wm_buf[...], preferred_element_type=F32)
    for g in range(groups):
        x = mid_ref[:, g * GROUP:(g + 1) * GROUP, :].astype(F32) + y[g * n:(g + 1) * n].reshape(frames, GROUP, D)
        out_ref[:, g * GROUP:(g + 1) * GROUP, :] = x.astype(BF)
    done = pltpu.make_async_copy(out_ref, out_hbm, sems.at[6])
    done.start()
    done.wait()
    kept.wait()


def temporal_phase(core, mid, order, gain, cot, heads, merge, spaces, times):
    frames, cols, _ = mid.shape
    n = frames * GROUP
    tokens = frames * cols
    spread = jnp.repeat(order, GROUP)
    block = D // (spaces * times)
    part = (spaces, times, block, D // 2)
    return pl.pallas_call(
        temporal_kernel,
        in_specs=[SMEM] + [VMEM] * 4 + [HBM] * 3,
        out_specs=[HBM, VMEM, HBM],
        out_shape=[pltpu.HBM((frames, cols, D), BF), pltpu.VMEM(part, BF), pltpu.HBM(part, BF)],
        scratch_shapes=[pltpu.VMEM((frames, cols, D), BF), pltpu.VMEM(part, BF), pltpu.VMEM((3, D, D), BF), pltpu.VMEM((D, D), BF), pltpu.VMEM((frames, cols, D), BF)]
        + [pltpu.VMEM((tokens, D), BF)] * 6
        + [pltpu.SemaphoreType.DMA((7,))],
        compiler_params=pltpu.CompilerParams(vmem_limit_bytes=40 * 2**20),
        name="temporal_phase",
    )(core, in_vmem(mid), spread.reshape(n, 1), spread.reshape(1, n), gain.reshape(1, D),
      in_hbm(cot), in_hbm(heads), in_hbm(merge))


def per_device(
    clip_tokens,
    frame_order,
    row_reach,
    spatial_gain,
    spatial_heads,
    spatial_merge,
    temporal_gain,
    temporal_heads,
    temporal_merge,
    cotangent,
):
    tm, space = lax.axis_size("tm"), lax.axis_size("space")
    _, frame_count, rows, cols, _ = clip_tokens.shape
    frames = frame_count // tm
    wide = tm * cols
    exchange = lambda v, axis: lax.all_to_all(v, axis, split_axis=0, concat_axis=0, tiled=True)

    arrived = exchange(clip_tokens.reshape(tm, frames, rows, cols, D), "tm")
    cot = cotangent.reshape(frames, rows, wide, D).swapaxes(0, 1)
    tok, low, high = norm_reorder(arrived, spatial_gain)
    up = [(i, i + 1) for i in range(space - 1)]
    down = [(j, i) for i, j in up]
    edge = HALO * wide
    above = lax.ppermute(high, "space", up)
    below = lax.ppermute(low, "space", down)
    qkv = qkv_own(low.reshape(frames, edge, D), high.reshape(frames, edge, D), spatial_heads)
    cot, qkv = lax.optimization_barrier((cot, qkv))
    cot = exchange(cot, "tm")
    here = lax.axis_index("space").astype(jnp.int32)
    info = jnp.concatenate([row_reach.reshape(frames), here.reshape(1)])
    middle = spatial_phase(info, above, below, qkv, tok, spatial_heads, spatial_merge, rows * space)
    mid = exchange(middle, "tm").reshape(frame_count, wide, D)
    core = jnp.stack([lax.axis_index("batch") & 1, here]).astype(jnp.int32)
    out, send, keep = temporal_phase(
        core, mid, frame_order.reshape(frame_count), temporal_gain, cot.reshape(frame_count, wide, D),
        temporal_heads, temporal_merge, space, tm,
    )
    batch = lax.axis_size("batch")
    got = lax.ppermute(send, "batch", [(i, i ^ 1) for i in range(batch)])
    output = exchange(out.reshape(tm, frames, wide, D), "tm").swapaxes(0, 1)
    chip = [keep[k].astype(F32) + got[k].astype(F32) for k in range(space)]
    total = chip[0]
    moved = [lax.ppermute(chip[k].astype(BF), "space", [(i, (i + k) % space) for i in range(space)])
             for k in range(1, space)]
    for part in moved:
        total = total + part.astype(F32)
    over_space = total.astype(BF)
    over_tm = exchange(over_space, "tm")
    over_tm = over_tm.astype(F32).sum(0).astype(BF)
    block = over_tm.shape[0]
    parts = lax.all_gather(over_tm, "batch").astype(F32).reshape(batch // 2, 2, block, D // 2).sum(0)
    weight_grad = parts.swapaxes(0, 1).reshape(block, D)
    return (output.reshape(1, frames, rows, wide, D), weight_grad)


def solution(mesh):
    in_specs = (
        P("batch", None, "space", "tm", None),
        P("batch", None),
        P("batch", "tm"),
        P(),
        P(),
        P(),
        P(),
        P(),
        P(),
        P("batch", "tm", "space", None, None),
    )
    out_specs = (P("batch", "tm", "space", None, None), P(("tm", "space"), None))

    return jax.shard_map(per_device, mesh=mesh, in_specs=in_specs, out_specs=out_specs, check_vma=False)
```

```python
import functools

import jax
import jax.numpy as jnp
from jax import lax
from jax.experimental import pallas as pl
from jax.experimental.pallas import tpu as pltpu
from jax.sharding import PartitionSpec as P


HALO = 4
D = 1024
HEADS = 16
HEAD_DIM = 64
PAIRS = HEADS // 2
WIDE = 2 * HEAD_DIM
FLOOR = 0.5
SCALE = HEAD_DIM ** (-0.5) * 1.4426950408889634
BF = jnp.bfloat16
F32 = jnp.float32
MASKED = -1e30


def normalized(x, gain):
    return x * lax.rsqrt(jnp.mean(x * x, axis=-1, keepdims=True) + FLOOR) * gain


def in_vmem(x):
    return pltpu.with_memory_space_constraint(x, pltpu.VMEM)


def in_hbm(x):
    return pltpu.with_memory_space_constraint(x, pltpu.HBM)


VMEM = pl.BlockSpec(memory_space=pltpu.VMEM)
SMEM = pl.BlockSpec(memory_space=pltpu.SMEM)
HBM = pl.BlockSpec(memory_space=pltpu.HBM)


def norm_kernel(x_ref, gain_ref, tok_out, low_ref, high_ref, tok_ref, sems):
    sources, frames, rows, cols, _ = x_ref.shape
    half = rows // 2
    gain = gain_ref[...]
    for f in range(frames):
        for h, part_ref in enumerate((low_ref, high_ref)):

            def one_row(r, carry):
                for s in range(sources):
                    x = x_ref[s, f, h * half + r]
                    y = normalized(x.astype(F32), gain).astype(BF)
                    tok_ref[f, h * half + r, s * cols:(s + 1) * cols, :] = x
                    part_ref[f, r, s * cols:(s + 1) * cols, :] = y
                return carry

            lax.fori_loop(0, half, one_row, 0)
        pltpu.make_async_copy(tok_ref.at[f], tok_out.at[f], sems.at[f]).start()
    for f in range(frames):
        pltpu.make_async_copy(tok_ref.at[f], tok_out.at[f], sems.at[f]).wait()


def norm_reorder(arrived, gain):
    sources, frames, rows, cols, _ = arrived.shape
    wide = sources * cols
    return pl.pallas_call(
        norm_kernel,
        in_specs=[VMEM, VMEM],
        out_specs=[HBM, VMEM, VMEM],
        scratch_shapes=[pltpu.VMEM((frames, rows, wide, D), BF), pltpu.SemaphoreType.DMA((frames,))],
        out_shape=[pltpu.HBM((frames, rows, wide, D), BF)] + [pltpu.VMEM((frames, rows // 2, wide, D), BF)] * 2,
        compiler_params=pltpu.CompilerParams(vmem_limit_bytes=8 * 2**20),
        name="norm_reorder",
    )(in_vmem(arrived), gain.reshape(1, D))


def column_copies(w_ref, buf, sems, columns):
    return [pltpu.make_async_copy(w_ref.at[:, c * D:(c + 1) * D], buf.at[i], sems.at[i]) for i, c in enumerate(columns)]


def qkv_kernel(low_ref, high_ref, w_ref, out_ref, x_ref, buf, y_ref, sems):
    copies = column_copies(w_ref, buf, sems, range(3))
    for c in copies:
        c.start()
    frames, edge, _ = low_ref.shape
    for f in range(frames):
        for h, part in enumerate((low_ref, high_ref)):
            at = (2 * f + h) * edge
            x_ref[at:at + edge] = part[f]
    for i, c in enumerate(copies):
        c.wait()
        y_ref[i] = jnp.dot(x_ref[...], buf[i], preferred_element_type=F32).astype(BF)
        pltpu.make_async_copy(y_ref.at[i], out_ref.at[i], sems.at[3 + i]).start()
    for i in range(3):
        pltpu.make_async_copy(y_ref.at[i], out_ref.at[i], sems.at[3 + i]).wait()


def qkv_own(low, high, heads):
    frames, edge, _ = low.shape
    tokens = 2 * frames * edge
    return pl.pallas_call(
        qkv_kernel,
        in_specs=[VMEM, VMEM, HBM],
        out_specs=HBM,
        out_shape=pltpu.HBM((3, tokens, D), BF),
        scratch_shapes=[pltpu.VMEM((tokens, D), BF), pltpu.VMEM((3, D, D), BF), pltpu.VMEM((3, tokens, D), BF),
                        pltpu.SemaphoreType.DMA((6,))],
        compiler_params=pltpu.CompilerParams(vmem_limit_bytes=24 * 2**20),
        name="qkv_own",
    )(in_vmem(low), in_vmem(high), in_hbm(heads))


def staged_attention(items):
    n = items[0][0]().shape[0]
    low = lax.broadcasted_iota(jnp.int32, (n, WIDE), 1) < HEAD_DIM
    scores, weights = [], []
    for q, k, v, bias, ref, at in items:
        q = q()
        zero = jnp.zeros_like(q)
        both = jnp.concatenate([jnp.where(low, q, zero), jnp.where(low, zero, q)], axis=0)
        scores.append(lax.dot_general(both, k(), (((1,), (1,)), ((), ())), preferred_element_type=F32))
    for s, (q, k, v, bias, ref, at) in zip(scores, items):
        b = bias()
        s = s * SCALE + jnp.concatenate([b, b], axis=0)
        weights.append(jnp.exp2(s - jnp.max(s, axis=-1, keepdims=True)).astype(BF))
    for p, (q, k, v, bias, ref, at) in zip(weights, items):
        v = v()
        o = jnp.dot(p, jnp.concatenate([v, jnp.ones_like(v)], axis=1), preferred_element_type=F32)
        o = o[:, :WIDE] / o[:, WIDE:]
        ref[at] = jnp.where(low, o[:n], o[n:]).astype(BF)


def reader(ref, *at):
    return lambda: ref[at]


SPATIAL_STAGE = 4
TEMPORAL_STAGE = 8


def spatial_kernel(info_ref, up_ref, down_ref, qkv_ref, tok_ref, w_ref, wm_ref, mid_out,
                   q_ref, tok_buf, mid_buf, wkv_buf, wm_buf, k_ref, v_ref, ctx_ref, bias_ref, sems, *, rows, all_rows):
    frames, extent, _ = k_ref.shape
    tokens = ctx_ref.shape[0] // frames
    cols = tokens // rows
    edge = HALO * cols
    weights = column_copies(w_ref, wkv_buf, sems, (1, 2))
    own = [pltpu.make_async_copy(qkv_ref.at[0], q_ref, sems.at[2])]
    for f in range(frames):
        mine = pl.ds(f * tokens, tokens)
        for i, buf in ((1, k_ref), (2, v_ref)):
            own.append(pltpu.make_async_copy(qkv_ref.at[i, mine], buf.at[f, edge:edge + tokens], sems.at[2 + 2 * f + i]))
    last = [pltpu.make_async_copy(wm_ref, wm_buf, sems.at[7]), pltpu.make_async_copy(tok_ref, tok_buf, sems.at[8])]
    for c in weights + own + last:
        c.start()
    first_row = info_ref[frames] * rows
    qrow = lax.broadcasted_iota(jnp.int32, (tokens, extent), 0) // cols
    krow = lax.broadcasted_iota(jnp.int32, (tokens, extent), 1) // cols - HALO
    inside = (krow + first_row >= 0) & (krow + first_row < all_rows)
    distance = jnp.where(inside, jnp.abs(krow - qrow), all_rows)
    for f in range(frames):
        bias_ref[f] = jnp.where(distance <= info_ref[f], 0.0, MASKED)
    halo = jnp.concatenate([up_ref[...].reshape(frames * edge, D), down_ref[...].reshape(frames * edge, D)], axis=0)
    for c, w, buf in zip(weights, range(2), (k_ref, v_ref)):
        c.wait()
        side = jnp.dot(halo, wkv_buf[w], preferred_element_type=F32).astype(BF)
        for f in range(frames):
            buf[f, 0:edge] = side[f * edge:(f + 1) * edge]
            buf[f, edge + tokens:] = side[(frames + f) * edge:(frames + f + 1) * edge]
    for c in own:
        c.wait()
    half = tokens // 2
    items = []
    for f in range(frames):
        for pair in range(PAIRS):
            at = slice(pair * WIDE, (pair + 1) * WIDE)
            for side in range(2):
                keys = slice(side * edge, side * edge + half + 2 * edge)
                rows_in = slice(side * half, (side + 1) * half)
                mine = slice(f * tokens + side * half, f * tokens + (side + 1) * half)
                items.append((reader(q_ref, mine, at), reader(k_ref, f, keys, at), reader(v_ref, f, keys, at),
                              reader(bias_ref, f, rows_in, keys), ctx_ref, (mine, at)))
    for i in range(0, len(items), SPATIAL_STAGE):
        staged_attention(items[i:i + SPATIAL_STAGE])
    for c in last:
        c.wait()
    sent = []
    for f in range(frames):
        mid = jnp.dot(ctx_ref[f * tokens:(f + 1) * tokens], wm_buf[...], preferred_element_type=F32)
        mid = mid + tok_buf[f].reshape(tokens, D).astype(F32)
        mid_buf[:, f] = mid.astype(BF).reshape(rows, cols, D)
        sent.append(pltpu.make_async_copy(mid_buf.at[:, f], mid_out.at[:, f], sems.at[9 + f]))
        sent[f].start()
    for c in sent:
        c.wait()


def spatial_phase(info, up, down, qkv, tok, heads, merge, all_rows):
    frames, rows, cols, _ = tok.shape
    tokens = rows * cols
    extent = tokens + 2 * HALO * cols
    return pl.pallas_call(
        functools.partial(spatial_kernel, rows=rows, all_rows=all_rows),
        in_specs=[SMEM, VMEM, VMEM, HBM, HBM, HBM, HBM],
        out_specs=HBM,
        out_shape=pltpu.HBM((rows, frames, cols, D), BF),
        scratch_shapes=[pltpu.VMEM((frames * tokens, D), BF), pltpu.VMEM((frames, rows, cols, D), BF),
                        pltpu.VMEM((rows, frames, cols, D), BF),
                        pltpu.VMEM((2, D, D), BF), pltpu.VMEM((D, D), BF),
                        pltpu.VMEM((frames, extent, D), BF), pltpu.VMEM((frames, extent, D), BF),
                        pltpu.VMEM((frames * tokens, D), BF), pltpu.VMEM((frames, tokens, extent), F32),
                        pltpu.SemaphoreType.DMA((9 + frames,))],
        compiler_params=pltpu.CompilerParams(vmem_limit_bytes=40 * 2**20),
        name="spatial_phase",
    )(info, in_vmem(up), in_vmem(down), *[in_hbm(v) for v in (qkv, tok, heads, merge)])


GROUP = 8


def temporal_kernel(core_ref, mid_ref, order_q_ref, order_k_ref, gain_ref, cot_ref, w_ref, wm_ref,
                    out_hbm, send_ref, keep_hbm,
                    out_ref, keep_ref, wqkv_buf, wm_buf, cot_buf, normed_ref, q_ref, k_ref, v_ref, ctx_ref, cotb_ref, sems):
    frames, cols, _ = mid_ref.shape
    groups = cols // GROUP
    n = frames * GROUP
    copies = column_copies(w_ref, wqkv_buf, sems, range(3))
    copies.append(pltpu.make_async_copy(cot_ref, cot_buf, sems.at[3]))
    copies.append(pltpu.make_async_copy(wm_ref, wm_buf, sems.at[4]))
    for c in copies:
        c.start()
    gain = gain_ref[...]
    for g in range(groups):
        x = mid_ref[:, g * GROUP:(g + 1) * GROUP, :].astype(F32).reshape(n, D)
        normed_ref[g * n:(g + 1) * n] = normalized(x, gain).astype(BF)
    for i, buf in enumerate((q_ref, k_ref, v_ref)):
        copies[i].wait()
        buf[...] = jnp.dot(normed_ref[...], wqkv_buf[i], preferred_element_type=F32).astype(BF)
    copies[3].wait()
    for g in range(groups):
        cotb_ref[g * n:(g + 1) * n] = cot_buf[:, g * GROUP:(g + 1) * GROUP, :].astype(F32).reshape(n, D).astype(BF)
    place_q = lax.broadcasted_iota(jnp.int32, (n, n), 0) % GROUP
    place_k = lax.broadcasted_iota(jnp.int32, (n, n), 1) % GROUP
    allowed = (place_q == place_k) & (order_k_ref[...] <= order_q_ref[...])
    bias = jnp.where(allowed, 0.0, MASKED)
    items = []
    for g in range(groups):
        own = slice(g * n, (g + 1) * n)
        for pair in range(PAIRS):
            at = slice(pair * WIDE, (pair + 1) * WIDE)
            items.append((reader(q_ref, own, at), reader(k_ref, own, at), reader(v_ref, own, at), lambda: bias,
                          ctx_ref, (own, at)))
    for i in range(0, len(items), TEMPORAL_STAGE):
        staged_attention(items[i:i + TEMPORAL_STAGE])
    core = core_ref[0]
    here = core_ref[1]
    half = D // 2
    for ref, which in ((send_ref, 1 - core), (keep_ref, core)):
        cot = cotb_ref[:, pl.ds(pl.multiple_of(which * half, half), half)]
        grad = lax.dot_general(ctx_ref[...], cot, (((0,), (0,)), ((), ())), preferred_element_type=F32).astype(BF)
        spaces, times, block, _ = ref.shape
        for s in range(spaces):
            slot = lax.rem(s + spaces - here, spaces)
            for t in range(times):
                row = (t * spaces + s) * block
                ref[slot, t] = grad[row:row + block]
    kept = pltpu.make_async_copy(keep_ref, keep_hbm, sems.at[5])
    kept.start()
    copies[4].wait()
    y = jnp.dot(ctx_ref[...], wm_buf[...], preferred_element_type=F32)
    for g in range(groups):
        x = mid_ref[:, g * GROUP:(g + 1) * GROUP, :].astype(F32) + y[g * n:(g + 1) * n].reshape(frames, GROUP, D)
        out_ref[:, g * GROUP:(g + 1) * GROUP, :] = x.astype(BF)
    done = pltpu.make_async_copy(out_ref, out_hbm, sems.at[6])
    done.start()
    done.wait()
    kept.wait()


def temporal_phase(core, mid, order, gain, cot, heads, merge, spaces, times):
    frames, cols, _ = mid.shape
    n = frames * GROUP
    tokens = frames * cols
    spread = jnp.repeat(order, GROUP)
    block = D // (spaces * times)
    part = (spaces, times, block, D // 2)
    return pl.pallas_call(
        temporal_kernel,
        in_specs=[SMEM] + [VMEM] * 4 + [HBM] * 3,
        out_specs=[HBM, VMEM, HBM],
        out_shape=[pltpu.HBM((frames, cols, D), BF), pltpu.VMEM(part, BF), pltpu.HBM(part, BF)],
        scratch_shapes=[pltpu.VMEM((frames, cols, D), BF), pltpu.VMEM(part, BF), pltpu.VMEM((3, D, D), BF), pltpu.VMEM((D, D), BF), pltpu.VMEM((frames, cols, D), BF)]
        + [pltpu.VMEM((tokens, D), BF)] * 6
        + [pltpu.SemaphoreType.DMA((7,))],
        compiler_params=pltpu.CompilerParams(vmem_limit_bytes=40 * 2**20),
        name="temporal_phase",
    )(core, in_vmem(mid), spread.reshape(n, 1), spread.reshape(1, n), gain.reshape(1, D),
      in_hbm(cot), in_hbm(heads), in_hbm(merge))


def per_device(
    clip_tokens,
    frame_order,
    row_reach,
    spatial_gain,
    spatial_heads,
    spatial_merge,
    temporal_gain,
    temporal_heads,
    temporal_merge,
    cotangent,
):
    tm, space = lax.axis_size("tm"), lax.axis_size("space")
    _, frame_count, rows, cols, _ = clip_tokens.shape
    frames = frame_count // tm
    wide = tm * cols
    exchange = lambda v, axis: lax.all_to_all(v, axis, split_axis=0, concat_axis=0, tiled=True)

    arrived = exchange(clip_tokens.reshape(tm, frames, rows, cols, D), "tm")
    cot = cotangent.reshape(frames, rows, wide, D).swapaxes(0, 1)
    tok, low, high = norm_reorder(arrived, spatial_gain)
    up = [(i, i + 1) for i in range(space - 1)]
    down = [(j, i) for i, j in up]
    edge = HALO * wide
    above = lax.ppermute(high, "space", up)
    below = lax.ppermute(low, "space", down)
    qkv = qkv_own(low.reshape(frames, edge, D), high.reshape(frames, edge, D), spatial_heads)
    cot, qkv = lax.optimization_barrier((cot, qkv))
    cot = exchange(cot, "tm")
    here = lax.axis_index("space").astype(jnp.int32)
    info = jnp.concatenate([row_reach.reshape(frames), here.reshape(1)])
    middle = spatial_phase(info, above, below, qkv, tok, spatial_heads, spatial_merge, rows * space)
    mid = exchange(middle, "tm").reshape(frame_count, wide, D)
    core = jnp.stack([lax.axis_index("batch") & 1, here]).astype(jnp.int32)
    out, send, keep = temporal_phase(
        core, mid, frame_order.reshape(frame_count), temporal_gain, cot.reshape(frame_count, wide, D),
        temporal_heads, temporal_merge, space, tm,
    )
    batch = lax.axis_size("batch")
    got = lax.ppermute(send, "batch", [(i, i ^ 1) for i in range(batch)])
    output = exchange(out.reshape(tm, frames, wide, D), "tm").swapaxes(0, 1)
    chip = [keep[k].astype(F32) + got[k].astype(F32) for k in range(space)]
    middle_blocks = tm // 2
    ahead = [(i, (i + 1) % space) for i in range(space)]
    back = [(j, i) for i, j in ahead]
    far = [(keep[2, at].astype(F32) + got[2, at].astype(F32)).astype(BF)
           for at in (slice(0, middle_blocks), slice(middle_blocks, tm))]
    via_before = lax.ppermute(far[0], "space", ahead)
    via_after = lax.ppermute(far[1], "space", back)
    none = jnp.zeros_like(via_before)
    to_next = chip[1] + jnp.concatenate([via_before, none]).astype(F32)
    to_last = chip[3] + jnp.concatenate([none, via_after]).astype(F32)
    from_before = lax.ppermute(to_next.astype(BF), "space", ahead)
    from_after = lax.ppermute(to_last.astype(BF), "space", back)
    over_space = (chip[0] + from_before.astype(F32) + from_after.astype(F32)).astype(BF)
    over_tm = exchange(over_space, "tm")
    over_tm = over_tm.astype(F32).sum(0).astype(BF)
    block = over_tm.shape[0]
    parts = lax.all_gather(over_tm, "batch").astype(F32).reshape(batch // 2, 2, block, D // 2).sum(0)
    weight_grad = parts.swapaxes(0, 1).reshape(block, D)
    return (output.reshape(1, frames, rows, wide, D), weight_grad)


def solution(mesh):
    in_specs = (
        P("batch", None, "space", "tm", None),
        P("batch", None),
        P("batch", "tm"),
        P(),
        P(),
        P(),
        P(),
        P(),
        P(),
        P("batch", "tm", "space", None, None),
    )
    out_specs = (P("batch", "tm", "space", None, None), P(("tm", "space"), None))

    return jax.shard_map(per_device, mesh=mesh, in_specs=in_specs, out_specs=out_specs, check_vma=False)
```

```python
import functools

import jax
import jax.numpy as jnp
from jax import lax
from jax.experimental import pallas as pl
from jax.experimental.pallas import tpu as pltpu
from jax.sharding import PartitionSpec as P


HALO = 4
D = 1024
HEADS = 16
HEAD_DIM = 64
PAIRS = HEADS // 2
WIDE = 2 * HEAD_DIM
FLOOR = 0.5
SCALE = HEAD_DIM ** (-0.5) * 1.4426950408889634
BF = jnp.bfloat16
F32 = jnp.float32
MASKED = -1e30


def normalized(x, gain):
    return x * lax.rsqrt(jnp.mean(x * x, axis=-1, keepdims=True) + FLOOR) * gain


def in_vmem(x):
    return pltpu.with_memory_space_constraint(x, pltpu.VMEM)


def in_hbm(x):
    return pltpu.with_memory_space_constraint(x, pltpu.HBM)


VMEM = pl.BlockSpec(memory_space=pltpu.VMEM)
SMEM = pl.BlockSpec(memory_space=pltpu.SMEM)
HBM = pl.BlockSpec(memory_space=pltpu.HBM)


def norm_kernel(x_ref, gain_ref, tok_out, low_ref, high_ref, tok_ref, sems):
    sources, frames, rows, cols, _ = x_ref.shape
    half = rows // 2
    gain = gain_ref[...]
    for f in range(frames):
        for h, part_ref in enumerate((low_ref, high_ref)):

            def one_row(r, carry):
                for s in range(sources):
                    x = x_ref[s, f, h * half + r]
                    y = normalized(x.astype(F32), gain).astype(BF)
                    tok_ref[f, h * half + r, s * cols:(s + 1) * cols, :] = x
                    part_ref[f, r, s * cols:(s + 1) * cols, :] = y
                return carry

            lax.fori_loop(0, half, one_row, 0)
        pltpu.make_async_copy(tok_ref.at[f], tok_out.at[f], sems.at[f]).start()
    for f in range(frames):
        pltpu.make_async_copy(tok_ref.at[f], tok_out.at[f], sems.at[f]).wait()


def norm_reorder(arrived, gain):
    sources, frames, rows, cols, _ = arrived.shape
    wide = sources * cols
    return pl.pallas_call(
        norm_kernel,
        in_specs=[VMEM, VMEM],
        out_specs=[HBM, VMEM, VMEM],
        scratch_shapes=[pltpu.VMEM((frames, rows, wide, D), BF), pltpu.SemaphoreType.DMA((frames,))],
        out_shape=[pltpu.HBM((frames, rows, wide, D), BF)] + [pltpu.VMEM((frames, rows // 2, wide, D), BF)] * 2,
        compiler_params=pltpu.CompilerParams(vmem_limit_bytes=8 * 2**20),
        name="norm_reorder",
    )(in_vmem(arrived), gain.reshape(1, D))


def column_copies(w_ref, buf, sems, columns):
    return [pltpu.make_async_copy(w_ref.at[:, c * D:(c + 1) * D], buf.at[i], sems.at[i]) for i, c in enumerate(columns)]


def qkv_kernel(low_ref, high_ref, w_ref, out_ref, x_ref, buf, y_ref, sems):
    copies = column_copies(w_ref, buf, sems, range(3))
    for c in copies:
        c.start()
    frames, edge, _ = low_ref.shape
    for f in range(frames):
        for h, part in enumerate((low_ref, high_ref)):
            at = (2 * f + h) * edge
            x_ref[at:at + edge] = part[f]
    for i, c in enumerate(copies):
        c.wait()
        y_ref[i] = jnp.dot(x_ref[...], buf[i], preferred_element_type=F32).astype(BF)
        pltpu.make_async_copy(y_ref.at[i], out_ref.at[i], sems.at[3 + i]).start()
    for i in range(3):
        pltpu.make_async_copy(y_ref.at[i], out_ref.at[i], sems.at[3 + i]).wait()


def qkv_own(low, high, heads):
    frames, edge, _ = low.shape
    tokens = 2 * frames * edge
    return pl.pallas_call(
        qkv_kernel,
        in_specs=[VMEM, VMEM, HBM],
        out_specs=HBM,
        out_shape=pltpu.HBM((3, tokens, D), BF),
        scratch_shapes=[pltpu.VMEM((tokens, D), BF), pltpu.VMEM((3, D, D), BF), pltpu.VMEM((3, tokens, D), BF),
                        pltpu.SemaphoreType.DMA((6,))],
        compiler_params=pltpu.CompilerParams(vmem_limit_bytes=24 * 2**20),
        name="qkv_own",
    )(in_vmem(low), in_vmem(high), in_hbm(heads))


def staged_attention(items):
    n = items[0][0]().shape[0]
    low = lax.broadcasted_iota(jnp.int32, (n, WIDE), 1) < HEAD_DIM
    scores, weights = [], []
    for q, k, v, bias, ref, at in items:
        q = q()
        zero = jnp.zeros_like(q)
        both = jnp.concatenate([jnp.where(low, q, zero), jnp.where(low, zero, q)], axis=0)
        scores.append(lax.dot_general(both, k(), (((1,), (1,)), ((), ())), preferred_element_type=F32))
    for s, (q, k, v, bias, ref, at) in zip(scores, items):
        b = bias()
        s = s * SCALE + jnp.concatenate([b, b], axis=0)
        weights.append(jnp.exp2(s - jnp.max(s, axis=-1, keepdims=True)).astype(BF))
    for p, (q, k, v, bias, ref, at) in zip(weights, items):
        v = v()
        o = jnp.dot(p, jnp.concatenate([v, jnp.ones_like(v)], axis=1), preferred_element_type=F32)
        o = o[:, :WIDE] / o[:, WIDE:]
        ref[at] = jnp.where(low, o[:n], o[n:]).astype(BF)


def reader(ref, *at):
    return lambda: ref[at]


SPATIAL_STAGE = 4
TEMPORAL_STAGE = 8


def spatial_kernel(info_ref, up_ref, down_ref, qkv_ref, tok_ref, w_ref, wm_ref, mid_out,
                   q_ref, tok_buf, mid_buf, wkv_buf, wm_buf, k_ref, v_ref, ctx_ref, bias_ref, sems, *, rows, all_rows):
    frames, extent, _ = k_ref.shape
    tokens = ctx_ref.shape[0] // frames
    cols = tokens // rows
    edge = HALO * cols
    weights = column_copies(w_ref, wkv_buf, sems, (1, 2))
    own = [pltpu.make_async_copy(qkv_ref.at[0], q_ref, sems.at[2])]
    for f in range(frames):
        mine = pl.ds(f * tokens, tokens)
        for i, buf in ((1, k_ref), (2, v_ref)):
            own.append(pltpu.make_async_copy(qkv_ref.at[i, mine], buf.at[f, edge:edge + tokens], sems.at[2 + 2 * f + i]))
    last = [pltpu.make_async_copy(wm_ref, wm_buf, sems.at[7]), pltpu.make_async_copy(tok_ref, tok_buf, sems.at[8])]
    for c in weights + own + last:
        c.start()
    first_row = info_ref[frames] * rows
    qrow = lax.broadcasted_iota(jnp.int32, (tokens, extent), 0) // cols
    krow = lax.broadcasted_iota(jnp.int32, (tokens, extent), 1) // cols - HALO
    inside = (krow + first_row >= 0) & (krow + first_row < all_rows)
    distance = jnp.where(inside, jnp.abs(krow - qrow), all_rows)
    for f in range(frames):
        bias_ref[f] = jnp.where(distance <= info_ref[f], 0.0, MASKED)
    halo = jnp.concatenate([up_ref[...].reshape(frames * edge, D), down_ref[...].reshape(frames * edge, D)], axis=0)
    for c, w, buf in zip(weights, range(2), (k_ref, v_ref)):
        c.wait()
        side = jnp.dot(halo, wkv_buf[w], preferred_element_type=F32).astype(BF)
        for f in range(frames):
            buf[f, 0:edge] = side[f * edge:(f + 1) * edge]
            buf[f, edge + tokens:] = side[(frames + f) * edge:(frames + f + 1) * edge]
    for c in own:
        c.wait()
    half = tokens // 2
    items = []
    for f in range(frames):
        for pair in range(PAIRS):
            at = slice(pair * WIDE, (pair + 1) * WIDE)
            for side in range(2):
                keys = slice(side * edge, side * edge + half + 2 * edge)
                rows_in = slice(side * half, (side + 1) * half)
                mine = slice(f * tokens + side * half, f * tokens + (side + 1) * half)
                items.append((reader(q_ref, mine, at), reader(k_ref, f, keys, at), reader(v_ref, f, keys, at),
                              reader(bias_ref, f, rows_in, keys), ctx_ref, (mine, at)))
    for i in range(0, len(items), SPATIAL_STAGE):
        staged_attention(items[i:i + SPATIAL_STAGE])
    for c in last:
        c.wait()
    sent = []
    for f in range(frames):
        mid = jnp.dot(ctx_ref[f * tokens:(f + 1) * tokens], wm_buf[...], preferred_element_type=F32)
        mid = mid + tok_buf[f].reshape(tokens, D).astype(F32)
        mid_buf[:, f] = mid.astype(BF).reshape(rows, cols, D)
        sent.append(pltpu.make_async_copy(mid_buf.at[:, f], mid_out.at[:, f], sems.at[9 + f]))
        sent[f].start()
    for c in sent:
        c.wait()


def spatial_phase(info, up, down, qkv, tok, heads, merge, all_rows):
    frames, rows, cols, _ = tok.shape
    tokens = rows * cols
    extent = tokens + 2 * HALO * cols
    return pl.pallas_call(
        functools.partial(spatial_kernel, rows=rows, all_rows=all_rows),
        in_specs=[SMEM, VMEM, VMEM, HBM, HBM, HBM, HBM],
        out_specs=HBM,
        out_shape=pltpu.HBM((rows, frames, cols, D), BF),
        scratch_shapes=[pltpu.VMEM((frames * tokens, D), BF), pltpu.VMEM((frames, rows, cols, D), BF),
                        pltpu.VMEM((rows, frames, cols, D), BF),
                        pltpu.VMEM((2, D, D), BF), pltpu.VMEM((D, D), BF),
                        pltpu.VMEM((frames, extent, D), BF), pltpu.VMEM((frames, extent, D), BF),
                        pltpu.VMEM((frames * tokens, D), BF), pltpu.VMEM((frames, tokens, extent), F32),
                        pltpu.SemaphoreType.DMA((9 + frames,))],
        compiler_params=pltpu.CompilerParams(vmem_limit_bytes=40 * 2**20),
        name="spatial_phase",
    )(info, in_vmem(up), in_vmem(down), *[in_hbm(v) for v in (qkv, tok, heads, merge)])


GROUP = 8


def temporal_kernel(core_ref, mid_ref, order_q_ref, order_k_ref, gain_ref, cot_ref, w_ref, wm_ref,
                    out_hbm, send_ref, keep_hbm,
                    out_ref, keep_ref, wqkv_buf, wm_buf, cot_buf, normed_ref, q_ref, k_ref, v_ref, ctx_ref, cotb_ref, sems):
    frames, cols, _ = mid_ref.shape
    groups = cols // GROUP
    n = frames * GROUP
    copies = column_copies(w_ref, wqkv_buf, sems, range(3))
    copies.append(pltpu.make_async_copy(cot_ref, cot_buf, sems.at[3]))
    copies.append(pltpu.make_async_copy(wm_ref, wm_buf, sems.at[4]))
    for c in copies:
        c.start()
    gain = gain_ref[...]
    for g in range(groups):
        x = mid_ref[:, g * GROUP:(g + 1) * GROUP, :].astype(F32).reshape(n, D)
        normed_ref[g * n:(g + 1) * n] = normalized(x, gain).astype(BF)
    for i, buf in enumerate((q_ref, k_ref, v_ref)):
        copies[i].wait()
        buf[...] = jnp.dot(normed_ref[...], wqkv_buf[i], preferred_element_type=F32).astype(BF)
    copies[3].wait()
    for g in range(groups):
        cotb_ref[g * n:(g + 1) * n] = cot_buf[:, g * GROUP:(g + 1) * GROUP, :].astype(F32).reshape(n, D).astype(BF)
    place_q = lax.broadcasted_iota(jnp.int32, (n, n), 0) % GROUP
    place_k = lax.broadcasted_iota(jnp.int32, (n, n), 1) % GROUP
    allowed = (place_q == place_k) & (order_k_ref[...] <= order_q_ref[...])
    bias = jnp.where(allowed, 0.0, MASKED)
    items = []
    for g in range(groups):
        own = slice(g * n, (g + 1) * n)
        for pair in range(PAIRS):
            at = slice(pair * WIDE, (pair + 1) * WIDE)
            items.append((reader(q_ref, own, at), reader(k_ref, own, at), reader(v_ref, own, at), lambda: bias,
                          ctx_ref, (own, at)))
    for i in range(0, len(items), TEMPORAL_STAGE):
        staged_attention(items[i:i + TEMPORAL_STAGE])
    core = core_ref[0]
    half = D // 2
    for ref, which in ((send_ref, 1 - core), (keep_ref, core)):
        cot = cotb_ref[:, pl.ds(pl.multiple_of(which * half, half), half)]
        grad = lax.dot_general(ctx_ref[...], cot, (((0,), (0,)), ((), ())), preferred_element_type=F32).astype(BF)
        ref[...] = grad.reshape(ref.shape)
    kept = pltpu.make_async_copy(keep_ref, keep_hbm, sems.at[5])
    kept.start()
    copies[4].wait()
    y = jnp.dot(ctx_ref[...], wm_buf[...], preferred_element_type=F32)
    for g in range(groups):
        x = mid_ref[:, g * GROUP:(g + 1) * GROUP, :].astype(F32) + y[g * n:(g + 1) * n].reshape(frames, GROUP, D)
        out_ref[:, g * GROUP:(g + 1) * GROUP, :] = x.astype(BF)
    done = pltpu.make_async_copy(out_ref, out_hbm, sems.at[6])
    done.start()
    done.wait()
    kept.wait()


def temporal_phase(core, mid, order, gain, cot, heads, merge, spaces, times):
    frames, cols, _ = mid.shape
    n = frames * GROUP
    tokens = frames * cols
    spread = jnp.repeat(order, GROUP)
    block = D // (spaces * times)
    part = (D // block, block, D // 2)
    return pl.pallas_call(
        temporal_kernel,
        in_specs=[SMEM] + [VMEM] * 4 + [HBM] * 3,
        out_specs=[HBM, VMEM, HBM],
        out_shape=[pltpu.HBM((frames, cols, D), BF), pltpu.VMEM(part, BF), pltpu.HBM(part, BF)],
        scratch_shapes=[pltpu.VMEM((frames, cols, D), BF), pltpu.VMEM(part, BF), pltpu.VMEM((3, D, D), BF), pltpu.VMEM((D, D), BF), pltpu.VMEM((frames, cols, D), BF)]
        + [pltpu.VMEM((tokens, D), BF)] * 6
        + [pltpu.SemaphoreType.DMA((7,))],
        compiler_params=pltpu.CompilerParams(vmem_limit_bytes=40 * 2**20),
        name="temporal_phase",
    )(core, in_vmem(mid), spread.reshape(n, 1), spread.reshape(1, n), gain.reshape(1, D),
      in_hbm(cot), in_hbm(heads), in_hbm(merge))


def per_device(
    clip_tokens,
    frame_order,
    row_reach,
    spatial_gain,
    spatial_heads,
    spatial_merge,
    temporal_gain,
    temporal_heads,
    temporal_merge,
    cotangent,
):
    tm, space = lax.axis_size("tm"), lax.axis_size("space")
    _, frame_count, rows, cols, _ = clip_tokens.shape
    frames = frame_count // tm
    wide = tm * cols
    exchange = lambda v, axis: lax.all_to_all(v, axis, split_axis=0, concat_axis=0, tiled=True)

    arrived = exchange(clip_tokens.reshape(tm, frames, rows, cols, D), "tm")
    cot = cotangent.reshape(frames, rows, wide, D).swapaxes(0, 1)
    tok, low, high = norm_reorder(arrived, spatial_gain)
    up = [(i, i + 1) for i in range(space - 1)]
    down = [(j, i) for i, j in up]
    edge = HALO * wide
    above = lax.ppermute(high, "space", up)
    below = lax.ppermute(low, "space", down)
    qkv = qkv_own(low.reshape(frames, edge, D), high.reshape(frames, edge, D), spatial_heads)
    cot, qkv = lax.optimization_barrier((cot, qkv))
    cot = exchange(cot, "tm")
    here = lax.axis_index("space").astype(jnp.int32)
    info = jnp.concatenate([row_reach.reshape(frames), here.reshape(1)])
    middle = spatial_phase(info, above, below, qkv, tok, spatial_heads, spatial_merge, rows * space)
    mid = exchange(middle, "tm").reshape(frame_count, wide, D)
    core = (lax.axis_index("batch") & 1).astype(jnp.int32).reshape(1)
    out, send, keep = temporal_phase(
        core, mid, frame_order.reshape(frame_count), temporal_gain, cot.reshape(frame_count, wide, D),
        temporal_heads, temporal_merge, space, tm,
    )
    batch = lax.axis_size("batch")
    got = lax.ppermute(send, "batch", [(i, i ^ 1) for i in range(batch)])
    chip = (keep.astype(F32) + got.astype(F32)).astype(BF)
    pieces = exchange(chip, ("tm", "space"))
    output = exchange(out.reshape(tm, frames, wide, D), "tm").swapaxes(0, 1)
    own_sum = pieces.astype(F32).sum(0).astype(BF)
    block = own_sum.shape[0]
    parts = lax.all_gather(own_sum, "batch").astype(F32).reshape(batch // 2, 2, block, D // 2).sum(0)
    weight_grad = parts.swapaxes(0, 1).reshape(block, D)
    return (output.reshape(1, frames, rows, wide, D), weight_grad)


def solution(mesh):
    in_specs = (
        P("batch", None, "space", "tm", None),
        P("batch", None),
        P("batch", "tm"),
        P(),
        P(),
        P(),
        P(),
        P(),
        P(),
        P("batch", "tm", "space", None, None),
    )
    out_specs = (P("batch", "tm", "space", None, None), P(("tm", "space"), None))

    return jax.shard_map(per_device, mesh=mesh, in_specs=in_specs, out_specs=out_specs, check_vma=False)
```

```python
import jax
import jax.numpy as jnp
from jax import lax
from jax.experimental import pallas as pl
from jax.experimental.pallas import tpu as pltpu
from jax.sharding import PartitionSpec as P


HALO = 4
D = 1024
HEADS = 16
HEAD_DIM = 64
PAIRS = HEADS // 2
WIDE = 2 * HEAD_DIM
FLOOR = 0.5
SCALE = HEAD_DIM ** (-0.5) * 1.4426950408889634
BF = jnp.bfloat16
F32 = jnp.float32
MASKED = -1e30


def normalized(x, gain):
    return x * lax.rsqrt(jnp.mean(x * x, axis=-1, keepdims=True) + FLOOR) * gain


def in_vmem(x):
    return pltpu.with_memory_space_constraint(x, pltpu.VMEM)


def in_hbm(x):
    return pltpu.with_memory_space_constraint(x, pltpu.HBM)


VMEM = pl.BlockSpec(memory_space=pltpu.VMEM)
SMEM = pl.BlockSpec(memory_space=pltpu.SMEM)
HBM = pl.BlockSpec(memory_space=pltpu.HBM)


def norm_kernel(info_ref, x_ref, gain_ref, tok_out, normed_ref, edge_ref, tok_ref, sem):
    times, parities, rows, cols, _ = x_ref.shape
    half = info_ref[1]
    gain = gain_ref[...]
    for o in range(parities):
        first = jnp.where(half == 0, 1 - o, o) * rows

        def one_row(r, carry):
            for t in range(times):
                x = x_ref[t, o, r]
                y = normalized(x.astype(F32), gain).astype(BF)
                tok_ref[first + r, t * cols:(t + 1) * cols, :] = x
                normed_ref[first + r, t * cols:(t + 1) * cols, :] = y
            return carry

        lax.fori_loop(0, rows, one_row, 0)
    out = pltpu.make_async_copy(tok_ref, tok_out, sem)
    out.start()
    start = jnp.where(half == 0, parities * rows - HALO, 0)
    edge_ref[...] = normed_ref[pl.ds(start, HALO)]
    out.wait()


def norm_reorder(info, arrived, gain):
    times, parities, rows, cols, _ = arrived.shape
    shape = (parities * rows, times * cols, D)
    return pl.pallas_call(
        norm_kernel,
        in_specs=[SMEM, VMEM, VMEM],
        out_specs=[HBM, VMEM, VMEM],
        out_shape=[pltpu.HBM(shape, BF), pltpu.VMEM(shape, BF), pltpu.VMEM((HALO,) + shape[1:], BF)],
        scratch_shapes=[pltpu.VMEM(shape, BF), pltpu.SemaphoreType.DMA],
        compiler_params=pltpu.CompilerParams(vmem_limit_bytes=8 * 2**20),
        name="norm_reorder",
    )(info, in_vmem(arrived), gain.reshape(1, D))


def column_copies(w_ref, buf, sems, columns):
    return [pltpu.make_async_copy(w_ref.at[:, c * D:(c + 1) * D], buf.at[i], sems.at[i]) for i, c in enumerate(columns)]


def qkv_kernel(x_ref, w_ref, out_ref, buf, y_ref, sems):
    copies = column_copies(w_ref, buf, sems, range(3))
    for c in copies:
        c.start()
    for i, c in enumerate(copies):
        c.wait()
        y_ref[i] = jnp.dot(x_ref[...], buf[i], preferred_element_type=F32).astype(BF)
        pltpu.make_async_copy(y_ref.at[i], out_ref.at[i], sems.at[3 + i]).start()
    for i in range(3):
        pltpu.make_async_copy(y_ref.at[i], out_ref.at[i], sems.at[3 + i]).wait()


def qkv_own(x, heads):
    tokens = x.shape[0]
    return pl.pallas_call(
        qkv_kernel,
        in_specs=[VMEM, HBM],
        out_specs=HBM,
        out_shape=pltpu.HBM((3, tokens, D), BF),
        scratch_shapes=[pltpu.VMEM((3, D, D), BF), pltpu.VMEM((3, tokens, D), BF), pltpu.SemaphoreType.DMA((6,))],
        compiler_params=pltpu.CompilerParams(vmem_limit_bytes=24 * 2**20),
        name="qkv_own",
    )(in_vmem(x), in_hbm(heads))


def staged_attention(items):
    n = items[0][0]().shape[0]
    low = lax.broadcasted_iota(jnp.int32, (n, WIDE), 1) < HEAD_DIM
    scores, weights = [], []
    for q, k, v, bias, ref, at in items:
        q = q()
        zero = jnp.zeros_like(q)
        both = jnp.concatenate([jnp.where(low, q, zero), jnp.where(low, zero, q)], axis=0)
        scores.append(lax.dot_general(both, k(), (((1,), (1,)), ((), ())), preferred_element_type=F32))
    for s, (q, k, v, bias, ref, at) in zip(scores, items):
        b = bias()
        s = s * SCALE + jnp.concatenate([b, b], axis=0)
        weights.append(jnp.exp2(s - jnp.max(s, axis=-1, keepdims=True)).astype(BF))
    for p, (q, k, v, bias, ref, at) in zip(weights, items):
        v = v()
        o = jnp.dot(p, jnp.concatenate([v, jnp.ones_like(v)], axis=1), preferred_element_type=F32)
        o = o[:, :WIDE] / o[:, WIDE:]
        ref[at] = jnp.where(low, o[:n], o[n:]).astype(BF)


def reader(ref, *at):
    return lambda: ref[at]


SPATIAL_STAGE = 4
TEMPORAL_STAGE = 8


def spatial_kernel(info_ref, halo_ref, qkv_ref, tok_ref, w_ref, wm_ref, mid_out,
                   q_ref, tok_buf, mid_buf, wkv_buf, wm_buf, k_ref, v_ref, ctx_ref, bias_ref, sems):
    rows, cols, _ = tok_buf.shape
    tokens = rows * cols
    edge = HALO * cols
    reach, half = info_ref[0], info_ref[1]
    weights = column_copies(w_ref, wkv_buf, sems, (1, 2))
    own = [pltpu.make_async_copy(qkv_ref.at[0], q_ref, sems.at[2])]
    for i, buf in ((1, k_ref), (2, v_ref)):
        own.append(pltpu.make_async_copy(qkv_ref.at[i], buf.at[edge:edge + tokens], sems.at[2 + i]))
    last = [pltpu.make_async_copy(wm_ref, wm_buf, sems.at[5]), pltpu.make_async_copy(tok_ref, tok_buf, sems.at[6])]
    for c in weights + own + last:
        c.start()
    blocks, n, extent = bias_ref.shape
    qrow = lax.broadcasted_iota(jnp.int32, (n, extent), 0) // cols
    krow = lax.broadcasted_iota(jnp.int32, (n, extent), 1) // cols - HALO
    near = jnp.abs(krow - qrow) <= reach
    for j in range(blocks):
        at = krow + (j * HALO + half * rows)
        bias_ref[j] = jnp.where(near & (at >= 0) & (at < 2 * rows), 0.0, MASKED)
    there = jnp.where(half == 0, edge + tokens, 0)
    empty = jnp.where(half == 0, 0, edge + tokens)
    halo = halo_ref[...].reshape(edge, D)
    for c, w, buf in zip(weights, range(2), (k_ref, v_ref)):
        c.wait()
        side = jnp.dot(halo, wkv_buf[w], preferred_element_type=F32).astype(BF)
        buf[pl.ds(pl.multiple_of(there, edge), edge)] = side
        buf[pl.ds(pl.multiple_of(empty, edge), edge)] = jnp.zeros_like(side)
    for c in own:
        c.wait()
    items = []
    for pair in range(PAIRS):
        at = slice(pair * WIDE, (pair + 1) * WIDE)
        for j in range(blocks):
            keys = slice(j * edge, j * edge + extent)
            mine = slice(j * n, (j + 1) * n)
            items.append((reader(q_ref, mine, at), reader(k_ref, keys, at), reader(v_ref, keys, at),
                          reader(bias_ref, j), ctx_ref, (mine, at)))
    for i in range(0, len(items), SPATIAL_STAGE):
        staged_attention(items[i:i + SPATIAL_STAGE])
    for c in last:
        c.wait()
    sent = []
    part, strip = rows // 2, tokens // 2
    for i in range(2):
        mid = jnp.dot(ctx_ref[i * strip:(i + 1) * strip], wm_buf[...], preferred_element_type=F32)
        mid = mid + tok_buf[i * part:(i + 1) * part].reshape(strip, D).astype(F32)
        mid_buf[i] = mid.astype(BF).reshape(part, cols, D)
        parity = jnp.where(half == 0, 1 - i, i)
        sent.append(pltpu.make_async_copy(mid_buf.at[i], mid_out.at[:, parity], sems.at[7 + i]))
        sent[i].start()
    for c in sent:
        c.wait()


def spatial_phase(info, halo, qkv, tok, heads, merge):
    rows, cols, _ = tok.shape
    tokens = rows * cols
    edge = HALO * cols
    extent = tokens + 2 * edge
    return pl.pallas_call(
        spatial_kernel,
        in_specs=[SMEM, VMEM, HBM, HBM, HBM, HBM],
        out_specs=HBM,
        out_shape=pltpu.HBM((rows // 2, 2, cols, D), BF),
        scratch_shapes=[pltpu.VMEM((tokens, D), BF), pltpu.VMEM((rows, cols, D), BF),
                        pltpu.VMEM((2, rows // 2, cols, D), BF),
                        pltpu.VMEM((2, D, D), BF), pltpu.VMEM((D, D), BF),
                        pltpu.VMEM((extent, D), BF), pltpu.VMEM((extent, D), BF),
                        pltpu.VMEM((tokens, D), BF), pltpu.VMEM((tokens // edge, edge, 3 * edge), F32),
                        pltpu.SemaphoreType.DMA((9,))],
        compiler_params=pltpu.CompilerParams(vmem_limit_bytes=40 * 2**20),
        name="spatial_phase",
    )(info, in_vmem(halo), *[in_hbm(v) for v in (qkv, tok, heads, merge)])


GROUP = 8


def temporal_kernel(core_ref, mid_ref, order_q_ref, order_k_ref, gain_ref, cot_ref, w_ref, wm_ref,
                    out_hbm, send_ref, keep_hbm,
                    out_ref, keep_ref, wqkv_buf, wm_buf, cot_buf, normed_ref, q_ref, k_ref, v_ref, ctx_ref, cotb_ref, sems):
    frames, cols, _ = mid_ref.shape
    groups = cols // GROUP
    n = frames * GROUP
    copies = column_copies(w_ref, wqkv_buf, sems, range(3))
    copies.append(pltpu.make_async_copy(cot_ref, cot_buf, sems.at[3]))
    copies.append(pltpu.make_async_copy(wm_ref, wm_buf, sems.at[4]))
    for c in copies:
        c.start()
    gain = gain_ref[...]
    for g in range(groups):
        x = mid_ref[:, g * GROUP:(g + 1) * GROUP, :].astype(F32).reshape(n, D)
        normed_ref[g * n:(g + 1) * n] = normalized(x, gain).astype(BF)
    for i, buf in enumerate((q_ref, k_ref, v_ref)):
        copies[i].wait()
        buf[...] = jnp.dot(normed_ref[...], wqkv_buf[i], preferred_element_type=F32).astype(BF)
    copies[3].wait()
    for g in range(groups):
        cotb_ref[g * n:(g + 1) * n] = cot_buf[:, g * GROUP:(g + 1) * GROUP, :].astype(F32).reshape(n, D).astype(BF)
    place_q = lax.broadcasted_iota(jnp.int32, (n, n), 0) % GROUP
    place_k = lax.broadcasted_iota(jnp.int32, (n, n), 1) % GROUP
    allowed = (place_q == place_k) & (order_k_ref[...] <= order_q_ref[...])
    bias = jnp.where(allowed, 0.0, MASKED)
    items = []
    for g in range(groups):
        own = slice(g * n, (g + 1) * n)
        for pair in range(PAIRS):
            at = slice(pair * WIDE, (pair + 1) * WIDE)
            items.append((reader(q_ref, own, at), reader(k_ref, own, at), reader(v_ref, own, at), lambda: bias,
                          ctx_ref, (own, at)))
    for i in range(0, len(items), TEMPORAL_STAGE):
        staged_attention(items[i:i + TEMPORAL_STAGE])
    core = core_ref[0]
    here = core_ref[1]
    half = D // 2
    for ref, which in ((send_ref, 1 - core), (keep_ref, core)):
        cot = cotb_ref[:, pl.ds(pl.multiple_of(which * half, half), half)]
        grad = lax.dot_general(ctx_ref[...], cot, (((0,), (0,)), ((), ())), preferred_element_type=F32).astype(BF)
        spaces, times, block, _ = ref.shape
        for s in range(spaces):
            slot = lax.rem(s + spaces - here, spaces)
            for t in range(times):
                row = (t * spaces + s) * block
                ref[slot, t] = grad[row:row + block]
    kept = pltpu.make_async_copy(keep_ref, keep_hbm, sems.at[5])
    kept.start()
    copies[4].wait()
    y = jnp.dot(ctx_ref[...], wm_buf[...], preferred_element_type=F32)
    for g in range(groups):
        x = mid_ref[:, g * GROUP:(g + 1) * GROUP, :].astype(F32) + y[g * n:(g + 1) * n].reshape(frames, GROUP, D)
        out_ref[:, g * GROUP:(g + 1) * GROUP, :] = x.astype(BF)
    done = pltpu.make_async_copy(out_ref, out_hbm, sems.at[6])
    done.start()
    done.wait()
    kept.wait()


def temporal_phase(core, mid, order, gain, cot, heads, merge, spaces, times):
    frames, cols, _ = mid.shape
    n = frames * GROUP
    tokens = frames * cols
    spread = jnp.repeat(order, GROUP)
    block = D // (spaces * times)
    part = (spaces, times, block, D // 2)
    return pl.pallas_call(
        temporal_kernel,
        in_specs=[SMEM] + [VMEM] * 4 + [HBM] * 3,
        out_specs=[HBM, VMEM, HBM],
        out_shape=[pltpu.HBM((frames, cols, D), BF), pltpu.VMEM(part, BF), pltpu.HBM(part, BF)],
        scratch_shapes=[pltpu.VMEM((frames, cols, D), BF), pltpu.VMEM(part, BF), pltpu.VMEM((3, D, D), BF), pltpu.VMEM((D, D), BF), pltpu.VMEM((frames, cols, D), BF)]
        + [pltpu.VMEM((tokens, D), BF)] * 6
        + [pltpu.SemaphoreType.DMA((7,))],
        compiler_params=pltpu.CompilerParams(vmem_limit_bytes=40 * 2**20),
        name="temporal_phase",
    )(core, in_vmem(mid), spread.reshape(n, 1), spread.reshape(1, n), gain.reshape(1, D),
      in_hbm(cot), in_hbm(heads), in_hbm(merge))


def per_device(
    clip_tokens,
    frame_order,
    row_reach,
    spatial_gain,
    spatial_heads,
    spatial_merge,
    temporal_gain,
    temporal_heads,
    temporal_merge,
    cotangent,
):
    tm, space = lax.axis_size("tm"), lax.axis_size("space")
    _, frame_count, rows, cols, _ = clip_tokens.shape
    frames = frame_count // tm
    wide = tm * cols
    tokens = rows * wide
    exchange = lambda v, axis: lax.all_to_all(v, axis, split_axis=0, concat_axis=0, tiled=True)

    here = lax.axis_index("space").astype(jnp.int32)
    half = here >> 1
    parity = (here & 1) ^ (1 - half)
    reach = jnp.where(parity == 0, row_reach[0, 0], row_reach[0, 1])
    info = jnp.stack([reach, half]).astype(jnp.int32)
    halves = [[t * space + s for t in range(tm) for s in pair] for pair in ((1, 0), (2, 3))]
    swap = lambda v: lax.all_to_all(v, ("tm", "space"), split_axis=0, concat_axis=0, axis_index_groups=halves, tiled=True)
    arrived = swap(clip_tokens.reshape(frame_count, rows, cols, D))
    cot = cotangent.reshape(frames, rows, wide, D).swapaxes(0, 1)
    tok, normed, edge_rows = norm_reorder(info, arrived.reshape(tm, frames, rows, cols, D), spatial_gain)
    halo = lax.ppermute(edge_rows, "space", [(i, space - 1 - i) for i in range(space)])
    qkv = qkv_own(normed.reshape(frames * tokens, D), spatial_heads)
    cot, qkv = lax.optimization_barrier((cot, qkv))
    cot = exchange(cot, "tm")
    middle = spatial_phase(info, halo, qkv, tok, spatial_heads, spatial_merge)
    mid = swap(middle.reshape(frame_count, wide, D))
    core = jnp.stack([lax.axis_index("batch") & 1, here]).astype(jnp.int32)
    out, send, keep = temporal_phase(
        core, mid, frame_order.reshape(frame_count), temporal_gain, cot.reshape(frame_count, wide, D),
        temporal_heads, temporal_merge, space, tm,
    )
    batch = lax.axis_size("batch")
    got = lax.ppermute(send, "batch", [(i, i ^ 1) for i in range(batch)])
    output = exchange(out.reshape(tm, frames, wide, D), "tm").swapaxes(0, 1)
    chip = [keep[k].astype(F32) + got[k].astype(F32) for k in range(space)]
    total = chip[0]
    moved = [lax.ppermute(chip[k].astype(BF), "space", [(i, (i + k) % space) for i in range(space)])
             for k in range(1, space)]
    for part in moved:
        total = total + part.astype(F32)
    over_space = total.astype(BF)
    over_tm = exchange(over_space, "tm")
    over_tm = over_tm.astype(F32).sum(0).astype(BF)
    block = over_tm.shape[0]
    parts = lax.all_gather(over_tm, "batch").astype(F32).reshape(batch // 2, 2, block, D // 2).sum(0)
    weight_grad = parts.swapaxes(0, 1).reshape(block, D)
    return (output.reshape(1, frames, rows, wide, D), weight_grad)


def solution(mesh):
    in_specs = (
        P("batch", None, "space", "tm", None),
        P("batch", None),
        P("batch", "tm"),
        P(),
        P(),
        P(),
        P(),
        P(),
        P(),
        P("batch", "tm", "space", None, None),
    )
    out_specs = (P("batch", "tm", "space", None, None), P(("tm", "space"), None))

    return jax.shard_map(per_device, mesh=mesh, in_specs=in_specs, out_specs=out_specs, check_vma=False)
```

```python
import jax
import jax.numpy as jnp
from jax import lax
from jax.experimental import pallas as pl
from jax.experimental.pallas import tpu as pltpu
from jax.sharding import PartitionSpec as P


HALO = 4
D = 1024
HEADS = 16
HEAD_DIM = 64
PAIRS = HEADS // 2
WIDE = 2 * HEAD_DIM
FLOOR = 0.5
SCALE = HEAD_DIM ** (-0.5) * 1.4426950408889634
BF = jnp.bfloat16
F32 = jnp.float32
MASKED = -1e30


def normalized(x, gain):
    return x * lax.rsqrt(jnp.mean(x * x, axis=-1, keepdims=True) + FLOOR) * gain


def in_vmem(x):
    return pltpu.with_memory_space_constraint(x, pltpu.VMEM)


def in_hbm(x):
    return pltpu.with_memory_space_constraint(x, pltpu.HBM)


VMEM = pl.BlockSpec(memory_space=pltpu.VMEM)
SMEM = pl.BlockSpec(memory_space=pltpu.SMEM)
HBM = pl.BlockSpec(memory_space=pltpu.HBM)


def norm_kernel(info_ref, x_ref, gain_ref, tok_out, normed_ref, edge_ref, tok_ref, sem):
    times, parities, rows, cols, _ = x_ref.shape
    half = info_ref[1]
    gain = gain_ref[...]
    for o in range(parities):
        first = jnp.where(half == 0, 1 - o, o) * rows

        def one_row(r, carry):
            for t in range(times):
                x = x_ref[t, o, r]
                y = normalized(x.astype(F32), gain).astype(BF)
                tok_ref[first + r, t * cols:(t + 1) * cols, :] = x
                normed_ref[first + r, t * cols:(t + 1) * cols, :] = y
            return carry

        lax.fori_loop(0, rows, one_row, 0)
        done = pl.ds(first, rows)
        pltpu.make_async_copy(tok_ref.at[done], tok_out.at[done], sem.at[o]).start()
    start = jnp.where(half == 0, parities * rows - HALO, 0)
    edge_ref[...] = normed_ref[pl.ds(start, HALO)]
    for o in range(parities):
        done = pl.ds(jnp.where(half == 0, 1 - o, o) * rows, rows)
        pltpu.make_async_copy(tok_ref.at[done], tok_out.at[done], sem.at[o]).wait()


def norm_reorder(info, arrived, gain):
    times, parities, rows, cols, _ = arrived.shape
    shape = (parities * rows, times * cols, D)
    return pl.pallas_call(
        norm_kernel,
        in_specs=[SMEM, VMEM, VMEM],
        out_specs=[HBM, VMEM, VMEM],
        out_shape=[pltpu.HBM(shape, BF), pltpu.VMEM(shape, BF), pltpu.VMEM((HALO,) + shape[1:], BF)],
        scratch_shapes=[pltpu.VMEM(shape, BF), pltpu.SemaphoreType.DMA((2,))],
        compiler_params=pltpu.CompilerParams(vmem_limit_bytes=8 * 2**20),
        name="norm_reorder",
    )(info, in_vmem(arrived), gain.reshape(1, D))


def column_copies(w_ref, buf, sems, columns):
    return [pltpu.make_async_copy(w_ref.at[:, c * D:(c + 1) * D], buf.at[i], sems.at[i]) for i, c in enumerate(columns)]


QKV_PIECE = 512


def qkv_kernel(x_ref, w_ref, out_ref, buf, y_ref, sems, out_sems):
    pieces = buf.shape[0]
    copies = [pltpu.make_async_copy(w_ref.at[:, i * QKV_PIECE:(i + 1) * QKV_PIECE], buf.at[i], sems.at[i])
              for i in range(pieces)]
    for c in copies:
        c.start()
    sent = []
    for i, c in enumerate(copies):
        c.wait()
        y_ref[i] = jnp.dot(x_ref[...], buf[i], preferred_element_type=F32).astype(BF)
        third, at = divmod(i * QKV_PIECE, D)
        sent.append(pltpu.make_async_copy(y_ref.at[i], out_ref.at[third, :, at:at + QKV_PIECE], out_sems.at[i]))
        sent[i].start()
    for c in sent:
        c.wait()


def qkv_own(x, heads):
    tokens = x.shape[0]
    pieces = 3 * D // QKV_PIECE
    return pl.pallas_call(
        qkv_kernel,
        in_specs=[VMEM, HBM],
        out_specs=HBM,
        out_shape=pltpu.HBM((3, tokens, D), BF),
        scratch_shapes=[pltpu.VMEM((pieces, D, QKV_PIECE), BF), pltpu.VMEM((pieces, tokens, QKV_PIECE), BF),
                        pltpu.SemaphoreType.DMA((pieces,)), pltpu.SemaphoreType.DMA((pieces,))],
        compiler_params=pltpu.CompilerParams(vmem_limit_bytes=24 * 2**20),
        name="qkv_own",
    )(in_vmem(x), in_hbm(heads))


def staged_attention(items):
    n = items[0][0]().shape[0]
    low = lax.broadcasted_iota(jnp.int32, (n, WIDE), 1) < HEAD_DIM
    scores, weights = [], []
    for q, k, v, bias, ref, at in items:
        q = q()
        zero = jnp.zeros_like(q)
        both = jnp.concatenate([jnp.where(low, q, zero), jnp.where(low, zero, q)], axis=0)
        scores.append(lax.dot_general(both, k(), (((1,), (1,)), ((), ())), preferred_element_type=F32))
    for s, (q, k, v, bias, ref, at) in zip(scores, items):
        b = bias()
        s = s * SCALE + jnp.concatenate([b, b], axis=0)
        weights.append(jnp.exp2(s - jnp.max(s, axis=-1, keepdims=True)).astype(BF))
    for p, (q, k, v, bias, ref, at) in zip(weights, items):
        v = v()
        o = jnp.dot(p, jnp.concatenate([v, jnp.ones_like(v)], axis=1), preferred_element_type=F32)
        o = o[:, :WIDE] / o[:, WIDE:]
        ref[at] = jnp.where(low, o[:n], o[n:]).astype(BF)


def reader(ref, *at):
    return lambda: ref[at]


SPATIAL_STAGE = 4
TEMPORAL_STAGE = 8


def spatial_kernel(info_ref, halo_ref, qkv_ref, tok_ref, w_ref, wm_ref, mid_out,
                   q_ref, tok_buf, mid_buf, wkv_buf, wm_buf, k_ref, v_ref, ctx_ref, bias_ref, sems):
    rows, cols, _ = tok_buf.shape
    tokens = rows * cols
    edge = HALO * cols
    reach, half = info_ref[0], info_ref[1]
    weights = column_copies(w_ref, wkv_buf, sems, (1, 2))
    own = [pltpu.make_async_copy(qkv_ref.at[0], q_ref, sems.at[2])]
    for i, buf in ((1, k_ref), (2, v_ref)):
        own.append(pltpu.make_async_copy(qkv_ref.at[i], buf.at[edge:edge + tokens], sems.at[2 + i]))
    last = [pltpu.make_async_copy(wm_ref, wm_buf, sems.at[5]), pltpu.make_async_copy(tok_ref, tok_buf, sems.at[6])]
    for c in weights + own + last:
        c.start()
    blocks, n, extent = bias_ref.shape
    qrow = lax.broadcasted_iota(jnp.int32, (n, extent), 0) // cols
    krow = lax.broadcasted_iota(jnp.int32, (n, extent), 1) // cols - HALO
    near = jnp.abs(krow - qrow) <= reach
    for j in range(blocks):
        at = krow + (j * HALO + half * rows)
        bias_ref[j] = jnp.where(near & (at >= 0) & (at < 2 * rows), 0.0, MASKED)
    there = jnp.where(half == 0, edge + tokens, 0)
    empty = jnp.where(half == 0, 0, edge + tokens)
    halo = halo_ref[...].reshape(edge, D)
    for c, w, buf in zip(weights, range(2), (k_ref, v_ref)):
        c.wait()
        side = jnp.dot(halo, wkv_buf[w], preferred_element_type=F32).astype(BF)
        buf[pl.ds(pl.multiple_of(there, edge), edge)] = side
        buf[pl.ds(pl.multiple_of(empty, edge), edge)] = jnp.zeros_like(side)
    for c in own:
        c.wait()
    items = []
    for pair in range(PAIRS):
        at = slice(pair * WIDE, (pair + 1) * WIDE)
        for j in range(blocks):
            keys = slice(j * edge, j * edge + extent)
            mine = slice(j * n, (j + 1) * n)
            items.append((reader(q_ref, mine, at), reader(k_ref, keys, at), reader(v_ref, keys, at),
                          reader(bias_ref, j), ctx_ref, (mine, at)))
    for i in range(0, len(items), SPATIAL_STAGE):
        staged_attention(items[i:i + SPATIAL_STAGE])
    for c in last:
        c.wait()
    sent = []
    part, strip = rows // 2, tokens // 2
    for i in range(2):
        mid = jnp.dot(ctx_ref[i * strip:(i + 1) * strip], wm_buf[...], preferred_element_type=F32)
        mid = mid + tok_buf[i * part:(i + 1) * part].reshape(strip, D).astype(F32)
        mid_buf[i] = mid.astype(BF).reshape(part, cols, D)
        parity = jnp.where(half == 0, 1 - i, i)
        sent.append(pltpu.make_async_copy(mid_buf.at[i], mid_out.at[:, parity], sems.at[7 + i]))
        sent[i].start()
    for c in sent:
        c.wait()


def spatial_phase(info, halo, qkv, tok, heads, merge):
    rows, cols, _ = tok.shape
    tokens = rows * cols
    edge = HALO * cols
    extent = tokens + 2 * edge
    return pl.pallas_call(
        spatial_kernel,
        in_specs=[SMEM, VMEM, HBM, HBM, HBM, HBM],
        out_specs=HBM,
        out_shape=pltpu.HBM((rows // 2, 2, cols, D), BF),
        scratch_shapes=[pltpu.VMEM((tokens, D), BF), pltpu.VMEM((rows, cols, D), BF),
                        pltpu.VMEM((2, rows // 2, cols, D), BF),
                        pltpu.VMEM((2, D, D), BF), pltpu.VMEM((D, D), BF),
                        pltpu.VMEM((extent, D), BF), pltpu.VMEM((extent, D), BF),
                        pltpu.VMEM((tokens, D), BF), pltpu.VMEM((tokens // edge, edge, 3 * edge), F32),
                        pltpu.SemaphoreType.DMA((9,))],
        compiler_params=pltpu.CompilerParams(vmem_limit_bytes=40 * 2**20),
        name="spatial_phase",
    )(info, in_vmem(halo), *[in_hbm(v) for v in (qkv, tok, heads, merge)])


GROUP = 8


def temporal_kernel(core_ref, mid_ref, order_q_ref, order_k_ref, gain_ref, cot_ref, w_ref, wm_ref,
                    out_hbm, send_ref, keep_hbm,
                    out_ref, keep_ref, wqkv_buf, wm_buf, cot_buf, normed_ref, q_ref, k_ref, v_ref, ctx_ref, cotb_ref, sems):
    frames, cols, _ = mid_ref.shape
    groups = cols // GROUP
    n = frames * GROUP
    copies = column_copies(w_ref, wqkv_buf, sems, range(3))
    copies.append(pltpu.make_async_copy(cot_ref, cot_buf, sems.at[3]))
    copies.append(pltpu.make_async_copy(wm_ref, wm_buf, sems.at[4]))
    for c in copies:
        c.start()
    gain = gain_ref[...]
    for g in range(groups):
        x = mid_ref[:, g * GROUP:(g + 1) * GROUP, :].astype(F32).reshape(n, D)
        normed_ref[g * n:(g + 1) * n] = normalized(x, gain).astype(BF)
    for i, buf in enumerate((q_ref, k_ref, v_ref)):
        copies[i].wait()
        buf[...] = jnp.dot(normed_ref[...], wqkv_buf[i], preferred_element_type=F32).astype(BF)
    copies[3].wait()
    for g in range(groups):
        cotb_ref[g * n:(g + 1) * n] = cot_buf[:, g * GROUP:(g + 1) * GROUP, :].astype(F32).reshape(n, D).astype(BF)
    place_q = lax.broadcasted_iota(jnp.int32, (n, n), 0) % GROUP
    place_k = lax.broadcasted_iota(jnp.int32, (n, n), 1) % GROUP
    allowed = (place_q == place_k) & (order_k_ref[...] <= order_q_ref[...])
    bias = jnp.where(allowed, 0.0, MASKED)
    items = []
    for g in range(groups):
        own = slice(g * n, (g + 1) * n)
        for pair in range(PAIRS):
            at = slice(pair * WIDE, (pair + 1) * WIDE)
            items.append((reader(q_ref, own, at), reader(k_ref, own, at), reader(v_ref, own, at), lambda: bias,
                          ctx_ref, (own, at)))
    for i in range(0, len(items), TEMPORAL_STAGE):
        staged_attention(items[i:i + TEMPORAL_STAGE])
    core = core_ref[0]
    here = core_ref[1]
    half = D // 2
    for ref, which in ((send_ref, 1 - core), (keep_ref, core)):
        cot = cotb_ref[:, pl.ds(pl.multiple_of(which * half, half), half)]
        grad = lax.dot_general(ctx_ref[...], cot, (((0,), (0,)), ((), ())), preferred_element_type=F32).astype(BF)
        spaces, times, block, _ = ref.shape
        for s in range(spaces):
            slot = lax.rem(s + spaces - here, spaces)
            for t in range(times):
                row = (t * spaces + s) * block
                ref[slot, t] = grad[row:row + block]
    kept = pltpu.make_async_copy(keep_ref, keep_hbm, sems.at[5])
    kept.start()
    copies[4].wait()
    y = jnp.dot(ctx_ref[...], wm_buf[...], preferred_element_type=F32)
    for g in range(groups):
        x = mid_ref[:, g * GROUP:(g + 1) * GROUP, :].astype(F32) + y[g * n:(g + 1) * n].reshape(frames, GROUP, D)
        out_ref[:, g * GROUP:(g + 1) * GROUP, :] = x.astype(BF)
    done = pltpu.make_async_copy(out_ref, out_hbm, sems.at[6])
    done.start()
    done.wait()
    kept.wait()


def temporal_phase(core, mid, order, gain, cot, heads, merge, spaces, times):
    frames, cols, _ = mid.shape
    n = frames * GROUP
    tokens = frames * cols
    spread = jnp.repeat(order, GROUP)
    block = D // (spaces * times)
    part = (spaces, times, block, D // 2)
    return pl.pallas_call(
        temporal_kernel,
        in_specs=[SMEM] + [VMEM] * 4 + [HBM] * 3,
        out_specs=[HBM, VMEM, HBM],
        out_shape=[pltpu.HBM((frames, cols, D), BF), pltpu.VMEM(part, BF), pltpu.HBM(part, BF)],
        scratch_shapes=[pltpu.VMEM((frames, cols, D), BF), pltpu.VMEM(part, BF), pltpu.VMEM((3, D, D), BF), pltpu.VMEM((D, D), BF), pltpu.VMEM((frames, cols, D), BF)]
        + [pltpu.VMEM((tokens, D), BF)] * 6
        + [pltpu.SemaphoreType.DMA((7,))],
        compiler_params=pltpu.CompilerParams(vmem_limit_bytes=40 * 2**20),
        name="temporal_phase",
    )(core, in_vmem(mid), spread.reshape(n, 1), spread.reshape(1, n), gain.reshape(1, D),
      in_hbm(cot), in_hbm(heads), in_hbm(merge))


def sum_kernel(keep_ref, got_ref, *refs):
    parts, (out_ref, own_ref, sems) = refs[:-3], refs[-3:]
    copies = [pltpu.make_async_copy(r.at[0], own_ref.at[i], sems.at[i]) for i, r in enumerate((keep_ref, got_ref))]
    for c in copies:
        c.start()
    total = parts[0][...].astype(F32)
    for p in parts[1:]:
        total = total + p[...].astype(F32)
    for c in copies:
        c.wait()
    out_ref[...] = (total + own_ref[0].astype(F32) + own_ref[1].astype(F32)).astype(BF)


def space_sum(keep, got, moved):
    shape = moved[0].shape
    return pl.pallas_call(
        sum_kernel,
        in_specs=[HBM, HBM] + [VMEM] * len(moved),
        out_specs=VMEM,
        out_shape=pltpu.VMEM(shape, BF),
        scratch_shapes=[pltpu.VMEM((2,) + shape, BF), pltpu.SemaphoreType.DMA((2,))],
        compiler_params=pltpu.CompilerParams(vmem_limit_bytes=8 * 2**20),
        name="space_sum",
    )(in_hbm(keep), in_hbm(got), *[in_vmem(p) for p in moved])


def per_device(
    clip_tokens,
    frame_order,
    row_reach,
    spatial_gain,
    spatial_heads,
    spatial_merge,
    temporal_gain,
    temporal_heads,
    temporal_merge,
    cotangent,
):
    tm, space = lax.axis_size("tm"), lax.axis_size("space")
    _, frame_count, rows, cols, _ = clip_tokens.shape
    frames = frame_count // tm
    wide = tm * cols
    tokens = rows * wide
    exchange = lambda v, axis: lax.all_to_all(v, axis, split_axis=0, concat_axis=0, tiled=True)

    here = lax.axis_index("space").astype(jnp.int32)
    half = here >> 1
    parity = (here & 1) ^ (1 - half)
    reach = jnp.where(parity == 0, row_reach[0, 0], row_reach[0, 1])
    info = jnp.stack([reach, half]).astype(jnp.int32)
    halves = [[t * space + s for t in range(tm) for s in pair] for pair in ((1, 0), (2, 3))]
    swap = lambda v: lax.all_to_all(v, ("tm", "space"), split_axis=0, concat_axis=0, axis_index_groups=halves, tiled=True)
    arrived = swap(clip_tokens.reshape(frame_count, rows, cols, D))
    cot = cotangent.reshape(frames, rows, wide, D).swapaxes(0, 1)
    tok, normed, edge_rows = norm_reorder(info, arrived.reshape(tm, frames, rows, cols, D), spatial_gain)
    halo = lax.ppermute(edge_rows, "space", [(i, space - 1 - i) for i in range(space)])
    cot, normed = lax.optimization_barrier((cot, normed))
    cot = exchange(cot, "tm")
    qkv = qkv_own(normed.reshape(frames * tokens, D), spatial_heads)
    middle = spatial_phase(info, halo, qkv, tok, spatial_heads, spatial_merge)
    mid = swap(middle.reshape(frame_count, wide, D))
    core = jnp.stack([lax.axis_index("batch") & 1, here]).astype(jnp.int32)
    out, send, keep = temporal_phase(
        core, mid, frame_order.reshape(frame_count), temporal_gain, cot.reshape(frame_count, wide, D),
        temporal_heads, temporal_merge, space, tm,
    )
    batch = lax.axis_size("batch")
    got = lax.ppermute(send, "batch", [(i, i ^ 1) for i in range(batch)])
    output = exchange(out.reshape(tm, frames, wide, D), "tm").swapaxes(0, 1)
    chip = [keep[k].astype(F32) + got[k].astype(F32) for k in range(1, space)]
    moved = [lax.ppermute(chip[k - 1].astype(BF), "space", [(i, (i + k) % space) for i in range(space)])
             for k in range(1, space)]
    over_space = space_sum(keep, got, moved)
    over_tm = exchange(over_space, "tm")
    over_tm = over_tm.astype(F32).sum(0).astype(BF)
    block = over_tm.shape[0]
    parts = lax.all_gather(over_tm, "batch").astype(F32).reshape(batch // 2, 2, block, D // 2).sum(0)
    weight_grad = parts.swapaxes(0, 1).reshape(block, D)
    return (output.reshape(1, frames, rows, wide, D), weight_grad)


def solution(mesh):
    in_specs = (
        P("batch", None, "space", "tm", None),
        P("batch", None),
        P("batch", "tm"),
        P(),
        P(),
        P(),
        P(),
        P(),
        P(),
        P("batch", "tm", "space", None, None),
    )
    out_specs = (P("batch", "tm", "space", None, None), P(("tm", "space"), None))

    return jax.shard_map(per_device, mesh=mesh, in_specs=in_specs, out_specs=out_specs, check_vma=False)
```

```python
import jax
import jax.numpy as jnp
from jax import lax
from jax.experimental import pallas as pl
from jax.experimental.pallas import tpu as pltpu
from jax.sharding import PartitionSpec as P


HALO = 4
D = 1024
HEADS = 16
HEAD_DIM = 64
PAIRS = HEADS // 2
WIDE = 2 * HEAD_DIM
FLOOR = 0.5
SCALE = HEAD_DIM ** (-0.5) * 1.4426950408889634
BF = jnp.bfloat16
F32 = jnp.float32
MASKED = -1e30


def normalized(x, gain):
    return x * lax.rsqrt(jnp.mean(x * x, axis=-1, keepdims=True) + FLOOR) * gain


def in_vmem(x):
    return pltpu.with_memory_space_constraint(x, pltpu.VMEM)


def in_hbm(x):
    return pltpu.with_memory_space_constraint(x, pltpu.HBM)


VMEM = pl.BlockSpec(memory_space=pltpu.VMEM)
SMEM = pl.BlockSpec(memory_space=pltpu.SMEM)
HBM = pl.BlockSpec(memory_space=pltpu.HBM)


def edge_kernel(info_ref, x_ref, gain_ref, edge_ref):
    times, _, rows, cols, _ = x_ref.shape
    start = jnp.where(info_ref[1] == 0, rows - HALO, 0)
    gain = gain_ref[...]
    for r in range(HALO):
        for t in range(times):
            y = normalized(x_ref[t, 0, start + r].astype(F32), gain)
            edge_ref[r, t * cols:(t + 1) * cols, :] = y.astype(BF)


def edge_norm(info, arrived, gain):
    times, _, _, cols, _ = arrived.shape
    return pl.pallas_call(
        edge_kernel,
        in_specs=[SMEM, VMEM, VMEM],
        out_specs=VMEM,
        out_shape=pltpu.VMEM((HALO, times * cols, D), BF),
        compiler_params=pltpu.CompilerParams(vmem_limit_bytes=4 * 2**20),
        name="edge_norm",
    )(info, in_vmem(arrived), gain.reshape(1, D))


def column_copies(w_ref, buf, sems, columns):
    return [pltpu.make_async_copy(w_ref.at[:, c * D:(c + 1) * D], buf.at[i], sems.at[i]) for i, c in enumerate(columns)]


QKV_PIECE = 1024


def qkv_kernel(info_ref, arrived_ref, gain_ref, w_ref, out_ref, tok_out, x_ref, tok_ref, buf, y_ref, sems, out_sems, tok_sems):
    pieces = buf.shape[0]
    copies = [pltpu.make_async_copy(w_ref.at[:, i * QKV_PIECE:(i + 1) * QKV_PIECE], buf.at[i], sems.at[i])
              for i in range(pieces)]
    for c in copies:
        c.start()
    times, parities, rows, cols, _ = arrived_ref.shape
    wide = times * cols
    half = info_ref[1]
    gain = gain_ref[...]
    kept = []
    for o in range(parities):
        first = jnp.where(half == 0, 1 - o, o) * rows

        def one_row(r, carry):
            for t in range(times):
                x = arrived_ref[t, o, r]
                y = normalized(x.astype(F32), gain).astype(BF)
                tok_ref[first + r, t * cols:(t + 1) * cols, :] = x
                x_ref[first + r, t * cols:(t + 1) * cols, :] = y
            return carry

        lax.fori_loop(0, rows, one_row, 0)
        done = pl.ds(first, rows)
        kept.append(pltpu.make_async_copy(tok_ref.at[done], tok_out.at[done], tok_sems.at[o]))
        kept[o].start()
    sent = []
    x = x_ref[...].reshape(parities * rows * wide, D)
    for i, c in enumerate(copies):
        c.wait()
        y_ref[i] = jnp.dot(x, buf[i], preferred_element_type=F32).astype(BF)
        third, at = divmod(i * QKV_PIECE, D)
        sent.append(pltpu.make_async_copy(y_ref.at[i], out_ref.at[third, :, at:at + QKV_PIECE], out_sems.at[i]))
        sent[i].start()
    for c in sent + kept:
        c.wait()


def qkv_own(info, arrived, gain, heads):
    times, parities, rows, cols, _ = arrived.shape
    shape = (parities * rows, times * cols, D)
    tokens = shape[0] * shape[1]
    pieces = 3 * D // QKV_PIECE
    return pl.pallas_call(
        qkv_kernel,
        in_specs=[SMEM, VMEM, VMEM, HBM],
        out_specs=[HBM, HBM],
        out_shape=[pltpu.HBM((3, tokens, D), BF), pltpu.HBM(shape, BF)],
        scratch_shapes=[pltpu.VMEM(shape, BF), pltpu.VMEM(shape, BF),
                        pltpu.VMEM((pieces, D, QKV_PIECE), BF), pltpu.VMEM((pieces, tokens, QKV_PIECE), BF),
                        pltpu.SemaphoreType.DMA((pieces,)), pltpu.SemaphoreType.DMA((pieces,)),
                        pltpu.SemaphoreType.DMA((2,))],
        compiler_params=pltpu.CompilerParams(vmem_limit_bytes=28 * 2**20),
        name="qkv_own",
    )(info, in_vmem(arrived), gain.reshape(1, D), in_hbm(heads))


def staged_attention(items):
    n = items[0][0]().shape[0]
    low = lax.broadcasted_iota(jnp.int32, (n, WIDE), 1) < HEAD_DIM
    scores, weights = [], []
    for q, k, v, bias, ref, at in items:
        q = q()
        zero = jnp.zeros_like(q)
        both = jnp.concatenate([jnp.where(low, q, zero), jnp.where(low, zero, q)], axis=0)
        scores.append(lax.dot_general(both, k(), (((1,), (1,)), ((), ())), preferred_element_type=F32))
    for s, (q, k, v, bias, ref, at) in zip(scores, items):
        b = bias()
        s = s * SCALE + jnp.concatenate([b, b], axis=0)
        weights.append(jnp.exp2(s - jnp.max(s, axis=-1, keepdims=True)).astype(BF))
    for p, (q, k, v, bias, ref, at) in zip(weights, items):
        v = v()
        o = jnp.dot(p, jnp.concatenate([v, jnp.ones_like(v)], axis=1), preferred_element_type=F32)
        o = o[:, :WIDE] / o[:, WIDE:]
        ref[at] = jnp.where(low, o[:n], o[n:]).astype(BF)


def reader(ref, *at):
    return lambda: ref[at]


SPATIAL_STAGE = 4
TEMPORAL_STAGE = 16


def spatial_kernel(info_ref, halo_ref, qkv_ref, tok_ref, w_ref, wm_ref, mid_out,
                   q_ref, tok_buf, mid_buf, wkv_buf, wm_buf, k_ref, v_ref, ctx_ref, bias_ref, sems):
    rows, cols, _ = tok_buf.shape
    tokens = rows * cols
    edge = HALO * cols
    reach, half = info_ref[0], info_ref[1]
    weights = column_copies(w_ref, wkv_buf, sems, (1, 2))
    own = [pltpu.make_async_copy(qkv_ref.at[0], q_ref, sems.at[2])]
    for i, buf in ((1, k_ref), (2, v_ref)):
        own.append(pltpu.make_async_copy(qkv_ref.at[i], buf.at[edge:edge + tokens], sems.at[2 + i]))
    last = [pltpu.make_async_copy(wm_ref, wm_buf, sems.at[5]), pltpu.make_async_copy(tok_ref, tok_buf, sems.at[6])]
    for c in own + weights + last:
        c.start()
    blocks, n, extent = bias_ref.shape
    qrow = lax.broadcasted_iota(jnp.int32, (n, extent), 0) // cols
    krow = lax.broadcasted_iota(jnp.int32, (n, extent), 1) // cols - HALO
    near = jnp.abs(krow - qrow) <= reach
    for j in range(blocks):
        at = krow + (j * HALO + half * rows)
        bias_ref[j] = jnp.where(near & (at >= 0) & (at < 2 * rows), 0.0, MASKED)
    for c in own:
        c.wait()

    def attend(chosen):
        items = []
        for pair in range(PAIRS):
            at = slice(pair * WIDE, (pair + 1) * WIDE)
            for j in chosen:
                keys = slice(j * edge, j * edge + extent)
                mine = slice(j * n, (j + 1) * n)
                items.append((reader(q_ref, mine, at), reader(k_ref, keys, at), reader(v_ref, keys, at),
                              reader(bias_ref, j), ctx_ref, (mine, at)))
        for i in range(0, len(items), SPATIAL_STAGE):
            staged_attention(items[i:i + SPATIAL_STAGE])

    inner = [j for j in range(blocks) if j * edge >= edge and j * edge + extent <= edge + tokens]
    attend(inner)
    there = jnp.where(half == 0, edge + tokens, 0)
    empty = jnp.where(half == 0, 0, edge + tokens)
    halo = halo_ref[...].reshape(edge, D)
    for c, w, buf in zip(weights, range(2), (k_ref, v_ref)):
        c.wait()
        side = jnp.dot(halo, wkv_buf[w], preferred_element_type=F32).astype(BF)
        buf[pl.ds(pl.multiple_of(there, edge), edge)] = side
        buf[pl.ds(pl.multiple_of(empty, edge), edge)] = jnp.zeros_like(side)
    attend([j for j in range(blocks) if j not in inner])
    for c in last:
        c.wait()
    sent = []
    part, strip = rows // 2, tokens // 2
    for i in range(2):
        mid = jnp.dot(ctx_ref[i * strip:(i + 1) * strip], wm_buf[...], preferred_element_type=F32)
        mid = mid + tok_buf[i * part:(i + 1) * part].reshape(strip, D).astype(F32)
        mid_buf[i] = mid.astype(BF).reshape(part, cols, D)
        parity = jnp.where(half == 0, 1 - i, i)
        sent.append(pltpu.make_async_copy(mid_buf.at[i], mid_out.at[:, parity], sems.at[7 + i]))
        sent[i].start()
    for c in sent:
        c.wait()


def spatial_phase(info, halo, qkv, tok, heads, merge):
    rows, cols, _ = tok.shape
    tokens = rows * cols
    edge = HALO * cols
    extent = tokens + 2 * edge
    return pl.pallas_call(
        spatial_kernel,
        in_specs=[SMEM, VMEM, HBM, HBM, HBM, HBM],
        out_specs=HBM,
        out_shape=pltpu.HBM((rows // 2, 2, cols, D), BF),
        scratch_shapes=[pltpu.VMEM((tokens, D), BF), pltpu.VMEM((rows, cols, D), BF),
                        pltpu.VMEM((2, rows // 2, cols, D), BF),
                        pltpu.VMEM((2, D, D), BF), pltpu.VMEM((D, D), BF),
                        pltpu.VMEM((extent, D), BF), pltpu.VMEM((extent, D), BF),
                        pltpu.VMEM((tokens, D), BF), pltpu.VMEM((tokens // edge, edge, 3 * edge), F32),
                        pltpu.SemaphoreType.DMA((9,))],
        compiler_params=pltpu.CompilerParams(vmem_limit_bytes=40 * 2**20),
        name="spatial_phase",
    )(info, in_vmem(halo), *[in_hbm(v) for v in (qkv, tok, heads, merge)])


GROUP = 8


def temporal_kernel(core_ref, mid_ref, order_q_ref, order_k_ref, gain_ref, cot_ref, w_ref, wm_ref,
                    out_hbm, send_ref, keep_ref,
                    out_ref, wqkv_buf, wm_buf, cot_buf, normed_ref, q_ref, k_ref, v_ref, ctx_ref, cotb_ref, sems):
    frames, cols, _ = mid_ref.shape
    groups = cols // GROUP
    n = frames * GROUP
    copies = column_copies(w_ref, wqkv_buf, sems, range(3))
    copies.append(pltpu.make_async_copy(cot_ref, cot_buf, sems.at[3]))
    copies.append(pltpu.make_async_copy(wm_ref, wm_buf, sems.at[4]))
    for c in copies:
        c.start()
    gain = gain_ref[...]
    for g in range(groups):
        x = mid_ref[:, g * GROUP:(g + 1) * GROUP, :].astype(F32).reshape(n, D)
        normed_ref[g * n:(g + 1) * n] = normalized(x, gain).astype(BF)
    for i, buf in enumerate((q_ref, k_ref, v_ref)):
        copies[i].wait()
        buf[...] = jnp.dot(normed_ref[...], wqkv_buf[i], preferred_element_type=F32).astype(BF)
    copies[3].wait()
    for g in range(groups):
        cotb_ref[g * n:(g + 1) * n] = cot_buf[:, g * GROUP:(g + 1) * GROUP, :].astype(F32).reshape(n, D).astype(BF)
    place_q = lax.broadcasted_iota(jnp.int32, (n, n), 0) % GROUP
    place_k = lax.broadcasted_iota(jnp.int32, (n, n), 1) % GROUP
    allowed = (place_q == place_k) & (order_k_ref[...] <= order_q_ref[...])
    bias = jnp.where(allowed, 0.0, MASKED)
    items = []
    for g in range(groups):
        own = slice(g * n, (g + 1) * n)
        for pair in range(PAIRS):
            at = slice(pair * WIDE, (pair + 1) * WIDE)
            items.append((reader(q_ref, own, at), reader(k_ref, own, at), reader(v_ref, own, at), lambda: bias,
                          ctx_ref, (own, at)))
    for i in range(0, len(items), TEMPORAL_STAGE):
        staged_attention(items[i:i + TEMPORAL_STAGE])
    core = core_ref[0]
    here = core_ref[1]
    half = D // 2
    for ref, which in ((send_ref, 1 - core), (keep_ref, core)):
        cot = cotb_ref[:, pl.ds(pl.multiple_of(which * half, half), half)]
        grad = lax.dot_general(ctx_ref[...], cot, (((0,), (0,)), ((), ())), preferred_element_type=F32).astype(BF)
        spaces, times, block, _ = ref.shape
        for s in range(spaces):
            slot = lax.rem(s + spaces - here, spaces)
            for t in range(times):
                row = (t * spaces + s) * block
                ref[slot, t] = grad[row:row + block]
    copies[4].wait()
    y = jnp.dot(ctx_ref[...], wm_buf[...], preferred_element_type=F32)
    for g in range(groups):
        x = mid_ref[:, g * GROUP:(g + 1) * GROUP, :].astype(F32) + y[g * n:(g + 1) * n].reshape(frames, GROUP, D)
        out_ref[:, g * GROUP:(g + 1) * GROUP, :] = x.astype(BF)
    done = pltpu.make_async_copy(out_ref, out_hbm, sems.at[6])
    done.start()
    done.wait()


def temporal_phase(core, mid, order, gain, cot, heads, merge, spaces, times):
    frames, cols, _ = mid.shape
    n = frames * GROUP
    tokens = frames * cols
    spread = jnp.repeat(order, GROUP)
    block = D // (spaces * times)
    part = (spaces, times, block, D // 2)
    return pl.pallas_call(
        temporal_kernel,
        in_specs=[SMEM] + [VMEM] * 4 + [HBM] * 3,
        out_specs=[HBM, VMEM, VMEM],
        out_shape=[pltpu.HBM((frames, cols, D), BF), pltpu.VMEM(part, BF), pltpu.VMEM(part, BF)],
        scratch_shapes=[pltpu.VMEM((frames, cols, D), BF), pltpu.VMEM((3, D, D), BF), pltpu.VMEM((D, D), BF), pltpu.VMEM((frames, cols, D), BF)]
        + [pltpu.VMEM((tokens, D), BF)] * 6
        + [pltpu.SemaphoreType.DMA((7,))],
        compiler_params=pltpu.CompilerParams(vmem_limit_bytes=40 * 2**20),
        name="temporal_phase",
    )(core, in_vmem(mid), spread.reshape(n, 1), spread.reshape(1, n), gain.reshape(1, D),
      in_hbm(cot), in_hbm(heads), in_hbm(merge))


def sum_kernel(keep_ref, got_ref, *refs):
    parts, (out_ref, own_ref, sems) = refs[:-3], refs[-3:]
    copies = [pltpu.make_async_copy(r.at[0], own_ref.at[i], sems.at[i]) for i, r in enumerate((keep_ref, got_ref))]
    for c in copies:
        c.start()
    total = parts[0][...].astype(F32)
    for p in parts[1:]:
        total = total + p[...].astype(F32)
    for c in copies:
        c.wait()
    out_ref[...] = (total + own_ref[0].astype(F32) + own_ref[1].astype(F32)).astype(BF)


def space_sum(keep, got, moved):
    shape = moved[0].shape
    return pl.pallas_call(
        sum_kernel,
        in_specs=[HBM, HBM] + [VMEM] * len(moved),
        out_specs=VMEM,
        out_shape=pltpu.VMEM(shape, BF),
        scratch_shapes=[pltpu.VMEM((2,) + shape, BF), pltpu.SemaphoreType.DMA((2,))],
        compiler_params=pltpu.CompilerParams(vmem_limit_bytes=8 * 2**20),
        name="space_sum",
    )(in_hbm(keep), in_hbm(got), *[in_vmem(p) for p in moved])


def per_device(
    clip_tokens,
    frame_order,
    row_reach,
    spatial_gain,
    spatial_heads,
    spatial_merge,
    temporal_gain,
    temporal_heads,
    temporal_merge,
    cotangent,
):
    tm, space = lax.axis_size("tm"), lax.axis_size("space")
    _, frame_count, rows, cols, _ = clip_tokens.shape
    frames = frame_count // tm
    wide = tm * cols
    exchange = lambda v, axis: lax.all_to_all(v, axis, split_axis=0, concat_axis=0, tiled=True)

    here = lax.axis_index("space").astype(jnp.int32)
    half = here >> 1
    parity = (here & 1) ^ (1 - half)
    reach = jnp.where(parity == 0, row_reach[0, 0], row_reach[0, 1])
    info = jnp.stack([reach, half]).astype(jnp.int32)
    halves = [[t * space + s for t in range(tm) for s in pair] for pair in ((1, 0), (2, 3))]
    swap = lambda v: lax.all_to_all(v, ("tm", "space"), split_axis=0, concat_axis=0, axis_index_groups=halves, tiled=True)
    arrived = swap(clip_tokens.reshape(frame_count, rows, cols, D))
    cot = cotangent.reshape(frames, rows, wide, D).swapaxes(0, 1)
    arrived = arrived.reshape(tm, frames, rows, cols, D)
    edge_rows = edge_norm(info, arrived, spatial_gain)
    halo = lax.ppermute(edge_rows, "space", [(i, space - 1 - i) for i in range(space)])
    cot, arrived = lax.optimization_barrier((cot, arrived))
    cot = exchange(cot, "tm")
    qkv, tok = qkv_own(info, arrived, spatial_gain, spatial_heads)
    middle = spatial_phase(info, halo, qkv, tok, spatial_heads, spatial_merge)
    mid = swap(middle.reshape(frame_count, wide, D))
    core = jnp.stack([lax.axis_index("batch") & 1, here]).astype(jnp.int32)
    out, send, keep = temporal_phase(
        core, mid, frame_order.reshape(frame_count), temporal_gain, cot.reshape(frame_count, wide, D),
        temporal_heads, temporal_merge, space, tm,
    )
    batch = lax.axis_size("batch")
    got = lax.ppermute(send, "batch", [(i, i ^ 1) for i in range(batch)])
    output = exchange(out.reshape(tm, frames, wide, D), "tm").swapaxes(0, 1)
    chip = [keep[k].astype(F32) + got[k].astype(F32) for k in range(1, space)]
    moved = [lax.ppermute(chip[k - 1].astype(BF), "space", [(i, (i + k) % space) for i in range(space)])
             for k in range(1, space)]
    over_space = space_sum(keep, got, moved)
    over_tm = exchange(over_space, "tm")
    over_tm = over_tm.astype(F32).sum(0).astype(BF)
    block = over_tm.shape[0]
    parts = lax.all_gather(over_tm, "batch").astype(F32).reshape(batch // 2, 2, block, D // 2).sum(0)
    weight_grad = parts.swapaxes(0, 1).reshape(block, D)
    return (output.reshape(1, frames, rows, wide, D), weight_grad)


def solution(mesh):
    in_specs = (
        P("batch", None, "space", "tm", None),
        P("batch", None),
        P("batch", "tm"),
        P(),
        P(),
        P(),
        P(),
        P(),
        P(),
        P("batch", "tm", "space", None, None),
    )
    out_specs = (P("batch", "tm", "space", None, None), P(("tm", "space"), None))

    return jax.shard_map(per_device, mesh=mesh, in_specs=in_specs, out_specs=out_specs, check_vma=False)
```

```python
import jax
import jax.numpy as jnp
from jax import lax
from jax.experimental import pallas as pl
from jax.experimental.pallas import tpu as pltpu
from jax.sharding import PartitionSpec as P


HALO = 4
D = 1024
HEADS = 16
HEAD_DIM = 64
PAIRS = HEADS // 2
WIDE = 2 * HEAD_DIM
FLOOR = 0.5
SCALE = HEAD_DIM ** (-0.5) * 1.4426950408889634
BF = jnp.bfloat16
F32 = jnp.float32
MASKED = -1e30


def normalized(x, gain):
    return x * lax.rsqrt(jnp.mean(x * x, axis=-1, keepdims=True) + FLOOR) * gain


def in_vmem(x):
    return pltpu.with_memory_space_constraint(x, pltpu.VMEM)


def in_hbm(x):
    return pltpu.with_memory_space_constraint(x, pltpu.HBM)


VMEM = pl.BlockSpec(memory_space=pltpu.VMEM)
SMEM = pl.BlockSpec(memory_space=pltpu.SMEM)
HBM = pl.BlockSpec(memory_space=pltpu.HBM)


def edge_kernel(info_ref, x_ref, gain_ref, edge_ref):
    times, _, rows, cols, _ = x_ref.shape
    start = jnp.where(info_ref[1] == 0, rows - HALO, 0)
    gain = gain_ref[...]
    for r in range(HALO):
        for t in range(times):
            y = normalized(x_ref[t, 0, start + r].astype(F32), gain)
            edge_ref[r, t * cols:(t + 1) * cols, :] = y.astype(BF)


def edge_norm(info, arrived, gain):
    times, _, _, cols, _ = arrived.shape
    return pl.pallas_call(
        edge_kernel,
        in_specs=[SMEM, VMEM, VMEM],
        out_specs=VMEM,
        out_shape=pltpu.VMEM((HALO, times * cols, D), BF),
        compiler_params=pltpu.CompilerParams(vmem_limit_bytes=4 * 2**20),
        name="edge_norm",
    )(info, in_vmem(arrived), gain.reshape(1, D))


def column_copies(w_ref, buf, sems, columns):
    return [pltpu.make_async_copy(w_ref.at[:, c * D:(c + 1) * D], buf.at[i], sems.at[i]) for i, c in enumerate(columns)]


QKV_PIECE = 1024


def qkv_kernel(info_ref, arrived_ref, gain_ref, w_ref, out_ref, tok_out, x_ref, tok_ref, buf, y_ref, sems, out_sems, tok_sems):
    pieces = buf.shape[0]
    copies = [pltpu.make_async_copy(w_ref.at[:, i * QKV_PIECE:(i + 1) * QKV_PIECE], buf.at[i], sems.at[i])
              for i in range(pieces)]
    for c in copies:
        c.start()
    times, parities, rows, cols, _ = arrived_ref.shape
    wide = times * cols
    half = info_ref[1]
    gain = gain_ref[...]
    kept = []
    for o in range(parities):
        first = jnp.where(half == 0, 1 - o, o) * rows

        def one_row(r, carry):
            for t in range(times):
                x = arrived_ref[t, o, r]
                y = normalized(x.astype(F32), gain).astype(BF)
                tok_ref[first + r, t * cols:(t + 1) * cols, :] = x
                x_ref[first + r, t * cols:(t + 1) * cols, :] = y
            return carry

        lax.fori_loop(0, rows, one_row, 0)
        done = pl.ds(first, rows)
        kept.append(pltpu.make_async_copy(tok_ref.at[done], tok_out.at[done], tok_sems.at[o]))
        kept[o].start()
    sent = []
    x = x_ref[...].reshape(parities * rows * wide, D)
    for i, c in enumerate(copies):
        c.wait()
        y_ref[i] = jnp.dot(x, buf[i], preferred_element_type=F32).astype(BF)
        third, at = divmod(i * QKV_PIECE, D)
        sent.append(pltpu.make_async_copy(y_ref.at[i], out_ref.at[third, :, at:at + QKV_PIECE], out_sems.at[i]))
        sent[i].start()
    for c in sent + kept:
        c.wait()


def qkv_own(info, arrived, gain, heads):
    times, parities, rows, cols, _ = arrived.shape
    shape = (parities * rows, times * cols, D)
    tokens = shape[0] * shape[1]
    pieces = 3 * D // QKV_PIECE
    return pl.pallas_call(
        qkv_kernel,
        in_specs=[SMEM, VMEM, VMEM, HBM],
        out_specs=[HBM, HBM],
        out_shape=[pltpu.HBM((3, tokens, D), BF), pltpu.HBM(shape, BF)],
        scratch_shapes=[pltpu.VMEM(shape, BF), pltpu.VMEM(shape, BF),
                        pltpu.VMEM((pieces, D, QKV_PIECE), BF), pltpu.VMEM((pieces, tokens, QKV_PIECE), BF),
                        pltpu.SemaphoreType.DMA((pieces,)), pltpu.SemaphoreType.DMA((pieces,)),
                        pltpu.SemaphoreType.DMA((2,))],
        compiler_params=pltpu.CompilerParams(vmem_limit_bytes=28 * 2**20),
        name="qkv_own",
    )(info, in_vmem(arrived), gain.reshape(1, D), in_hbm(heads))


def staged_attention(items):
    n = items[0][0]().shape[0]
    low = lax.broadcasted_iota(jnp.int32, (n, WIDE), 1) < HEAD_DIM
    scores, weights = [], []
    for q, k, v, bias, ref, at in items:
        q = q()
        zero = jnp.zeros_like(q)
        both = jnp.concatenate([jnp.where(low, q, zero), jnp.where(low, zero, q)], axis=0)
        scores.append(lax.dot_general(both, k(), (((1,), (1,)), ((), ())), preferred_element_type=F32))
    for s, (q, k, v, bias, ref, at) in zip(scores, items):
        b = bias()
        s = s * SCALE + jnp.concatenate([b, b], axis=0)
        weights.append(jnp.exp2(s - jnp.max(s, axis=-1, keepdims=True)).astype(BF))
    for p, (q, k, v, bias, ref, at) in zip(weights, items):
        v = v()
        o = jnp.dot(p, jnp.concatenate([v, jnp.ones_like(v)], axis=1), preferred_element_type=F32)
        o = o[:, :WIDE] / o[:, WIDE:]
        ref[at] = jnp.where(low, o[:n], o[n:]).astype(BF)


def reader(ref, *at):
    return lambda: ref[at]


SPATIAL_STAGE = 4
TEMPORAL_STAGE = 16


def spatial_kernel(info_ref, halo_ref, qkv_ref, tok_ref, w_ref, wm_ref, mid_out,
                   q_ref, tok_buf, mid_buf, wkv_buf, wm_buf, k_ref, v_ref, ctx_ref, bias_ref, sems):
    rows, cols, _ = tok_buf.shape
    tokens = rows * cols
    edge = HALO * cols
    reach, half = info_ref[0], info_ref[1]
    weights = column_copies(w_ref, wkv_buf, sems, (1, 2))
    own = [pltpu.make_async_copy(qkv_ref.at[0], q_ref, sems.at[2])]
    for i, buf in ((1, k_ref), (2, v_ref)):
        own.append(pltpu.make_async_copy(qkv_ref.at[i], buf.at[edge:edge + tokens], sems.at[2 + i]))
    last = [pltpu.make_async_copy(wm_ref, wm_buf, sems.at[5]), pltpu.make_async_copy(tok_ref, tok_buf, sems.at[6])]
    for c in own + weights + last:
        c.start()
    blocks, n, extent = bias_ref.shape
    qrow = lax.broadcasted_iota(jnp.int32, (n, extent), 0) // cols
    krow = lax.broadcasted_iota(jnp.int32, (n, extent), 1) // cols - HALO
    near = jnp.abs(krow - qrow) <= reach
    for j in range(blocks):
        at = krow + (j * HALO + half * rows)
        bias_ref[j] = jnp.where(near & (at >= 0) & (at < 2 * rows), 0.0, MASKED)
    for c in own:
        c.wait()

    def attend(chosen):
        items = []
        for pair in range(PAIRS):
            at = slice(pair * WIDE, (pair + 1) * WIDE)
            for j in chosen:
                keys = slice(j * edge, j * edge + extent)
                mine = slice(j * n, (j + 1) * n)
                items.append((reader(q_ref, mine, at), reader(k_ref, keys, at), reader(v_ref, keys, at),
                              reader(bias_ref, j), ctx_ref, (mine, at)))
        for i in range(0, len(items), SPATIAL_STAGE):
            staged_attention(items[i:i + SPATIAL_STAGE])

    inner = [j for j in range(blocks) if j * edge >= edge and j * edge + extent <= edge + tokens]
    attend(inner)
    there = jnp.where(half == 0, edge + tokens, 0)
    empty = jnp.where(half == 0, 0, edge + tokens)
    halo = halo_ref[...].reshape(edge, D)
    for c, w, buf in zip(weights, range(2), (k_ref, v_ref)):
        c.wait()
        side = jnp.dot(halo, wkv_buf[w], preferred_element_type=F32).astype(BF)
        buf[pl.ds(pl.multiple_of(there, edge), edge)] = side
        buf[pl.ds(pl.multiple_of(empty, edge), edge)] = jnp.zeros_like(side)
    attend([j for j in range(blocks) if j not in inner])
    for c in last:
        c.wait()
    sent = []
    part, strip = rows // 2, tokens // 2
    for i in range(2):
        mid = jnp.dot(ctx_ref[i * strip:(i + 1) * strip], wm_buf[...], preferred_element_type=F32)
        mid = mid + tok_buf[i * part:(i + 1) * part].reshape(strip, D).astype(F32)
        mid_buf[i] = mid.astype(BF).reshape(part, cols, D)
        parity = jnp.where(half == 0, 1 - i, i)
        sent.append(pltpu.make_async_copy(mid_buf.at[i], mid_out.at[:, parity], sems.at[7 + i]))
        sent[i].start()
    for c in sent:
        c.wait()


def spatial_phase(info, halo, qkv, tok, heads, merge):
    rows, cols, _ = tok.shape
    tokens = rows * cols
    edge = HALO * cols
    extent = tokens + 2 * edge
    return pl.pallas_call(
        spatial_kernel,
        in_specs=[SMEM, VMEM, HBM, HBM, HBM, HBM],
        out_specs=HBM,
        out_shape=pltpu.HBM((rows // 2, 2, cols, D), BF),
        scratch_shapes=[pltpu.VMEM((tokens, D), BF), pltpu.VMEM((rows, cols, D), BF),
                        pltpu.VMEM((2, rows // 2, cols, D), BF),
                        pltpu.VMEM((2, D, D), BF), pltpu.VMEM((D, D), BF),
                        pltpu.VMEM((extent, D), BF), pltpu.VMEM((extent, D), BF),
                        pltpu.VMEM((tokens, D), BF), pltpu.VMEM((tokens // edge, edge, 3 * edge), F32),
                        pltpu.SemaphoreType.DMA((9,))],
        compiler_params=pltpu.CompilerParams(vmem_limit_bytes=40 * 2**20),
        name="spatial_phase",
    )(info, in_vmem(halo), *[in_hbm(v) for v in (qkv, tok, heads, merge)])


GROUP = 8


def temporal_kernel(core_ref, mid_ref, order_q_ref, order_k_ref, gain_ref, wq_ref, cot_ref, w_ref, wm_ref,
                    out_hbm, send_ref, keep_hbm,
                    out_ref, keep_ref, wqkv_buf, wm_buf, cot_buf, normed_ref, q_ref, k_ref, v_ref, ctx_ref, cotb_ref, sems):
    frames, cols, _ = mid_ref.shape
    groups = cols // GROUP
    n = frames * GROUP
    copies = column_copies(w_ref, wqkv_buf, sems, (1, 2))
    copies.append(pltpu.make_async_copy(cot_ref, cot_buf, sems.at[3]))
    copies.append(pltpu.make_async_copy(wm_ref, wm_buf, sems.at[4]))
    for c in copies:
        c.start()
    gain = gain_ref[...]
    for g in range(groups):
        x = mid_ref[:, g * GROUP:(g + 1) * GROUP, :].astype(F32).reshape(n, D)
        normed_ref[g * n:(g + 1) * n] = normalized(x, gain).astype(BF)
    q_ref[...] = jnp.dot(normed_ref[...], wq_ref[...], preferred_element_type=F32).astype(BF)
    for i, buf in enumerate((k_ref, v_ref)):
        copies[i].wait()
        buf[...] = jnp.dot(normed_ref[...], wqkv_buf[i], preferred_element_type=F32).astype(BF)
    copies[2].wait()
    for g in range(groups):
        cotb_ref[g * n:(g + 1) * n] = cot_buf[:, g * GROUP:(g + 1) * GROUP, :].astype(F32).reshape(n, D).astype(BF)
    place_q = lax.broadcasted_iota(jnp.int32, (n, n), 0) % GROUP
    place_k = lax.broadcasted_iota(jnp.int32, (n, n), 1) % GROUP
    allowed = (place_q == place_k) & (order_k_ref[...] <= order_q_ref[...])
    bias = jnp.where(allowed, 0.0, MASKED)
    items = []
    for g in range(groups):
        own = slice(g * n, (g + 1) * n)
        for pair in range(PAIRS):
            at = slice(pair * WIDE, (pair + 1) * WIDE)
            items.append((reader(q_ref, own, at), reader(k_ref, own, at), reader(v_ref, own, at), lambda: bias,
                          ctx_ref, (own, at)))
    for i in range(0, len(items), TEMPORAL_STAGE):
        staged_attention(items[i:i + TEMPORAL_STAGE])
    core = core_ref[0]
    here = core_ref[1]
    half = D // 2
    for ref, which in ((send_ref, 1 - core), (keep_ref, core)):
        cot = cotb_ref[:, pl.ds(pl.multiple_of(which * half, half), half)]
        grad = lax.dot_general(ctx_ref[...], cot, (((0,), (0,)), ((), ())), preferred_element_type=F32).astype(BF)
        spaces, times, block, _ = ref.shape
        for s in range(spaces):
            slot = lax.rem(s + spaces - here, spaces)
            for t in range(times):
                row = (t * spaces + s) * block
                ref[slot, t] = grad[row:row + block]
    kept = pltpu.make_async_copy(keep_ref, keep_hbm, sems.at[5])
    kept.start()
    copies[3].wait()
    y = jnp.dot(ctx_ref[...], wm_buf[...], preferred_element_type=F32)
    for g in range(groups):
        x = mid_ref[:, g * GROUP:(g + 1) * GROUP, :].astype(F32) + y[g * n:(g + 1) * n].reshape(frames, GROUP, D)
        out_ref[:, g * GROUP:(g + 1) * GROUP, :] = x.astype(BF)
    done = pltpu.make_async_copy(out_ref, out_hbm, sems.at[6])
    done.start()
    done.wait()
    kept.wait()


def temporal_phase(core, mid, order, gain, cot, heads, merge, spaces, times):
    frames, cols, _ = mid.shape
    n = frames * GROUP
    tokens = frames * cols
    spread = jnp.repeat(order, GROUP)
    block = D // (spaces * times)
    part = (spaces, times, block, D // 2)
    first_third = heads[:, :D]
    return pl.pallas_call(
        temporal_kernel,
        in_specs=[SMEM] + [VMEM] * 5 + [HBM] * 3,
        out_specs=[HBM, VMEM, HBM],
        out_shape=[pltpu.HBM((frames, cols, D), BF), pltpu.VMEM(part, BF), pltpu.HBM(part, BF)],
        scratch_shapes=[pltpu.VMEM((frames, cols, D), BF), pltpu.VMEM(part, BF), pltpu.VMEM((2, D, D), BF), pltpu.VMEM((D, D), BF), pltpu.VMEM((frames, cols, D), BF)]
        + [pltpu.VMEM((tokens, D), BF)] * 6
        + [pltpu.SemaphoreType.DMA((7,))],
        compiler_params=pltpu.CompilerParams(vmem_limit_bytes=40 * 2**20),
        name="temporal_phase",
    )(core, in_vmem(mid), spread.reshape(n, 1), spread.reshape(1, n), gain.reshape(1, D),
      in_vmem(first_third), in_hbm(cot), in_hbm(heads), in_hbm(merge))


def own_kernel(keep_ref, got_ref, out_ref):
    out_ref[...] = keep_ref[...].astype(F32) + got_ref[...].astype(F32)


def own_slot(keep, got):
    shape = keep.shape[1:]
    first = pl.BlockSpec((None,) + shape, lambda i: (0, 0, 0, 0))
    return pl.pallas_call(
        own_kernel,
        grid=(1,),
        in_specs=[first, first],
        out_specs=pl.BlockSpec(shape, lambda i: (0, 0, 0)),
        out_shape=jax.ShapeDtypeStruct(shape, F32),
        compiler_params=pltpu.CompilerParams(vmem_limit_bytes=8 * 2**20),
        name="own_slot",
    )(in_hbm(keep), got)


def sum_kernel(own_ref, *refs):
    total = own_ref[...]
    for p in refs[:-1]:
        total = total + p[...].astype(F32)
    refs[-1][...] = total.astype(BF)


def space_sum(own, moved):
    return pl.pallas_call(
        sum_kernel,
        in_specs=[VMEM] * (1 + len(moved)),
        out_specs=VMEM,
        out_shape=pltpu.VMEM(own.shape, BF),
        compiler_params=pltpu.CompilerParams(vmem_limit_bytes=8 * 2**20),
        name="space_sum",
    )(in_vmem(own), *[in_vmem(p) for p in moved])


def per_device(
    clip_tokens,
    frame_order,
    row_reach,
    spatial_gain,
    spatial_heads,
    spatial_merge,
    temporal_gain,
    temporal_heads,
    temporal_merge,
    cotangent,
):
    tm, space = lax.axis_size("tm"), lax.axis_size("space")
    _, frame_count, rows, cols, _ = clip_tokens.shape
    frames = frame_count // tm
    wide = tm * cols
    exchange = lambda v, axis: lax.all_to_all(v, axis, split_axis=0, concat_axis=0, tiled=True)

    here = lax.axis_index("space").astype(jnp.int32)
    half = here >> 1
    parity = (here & 1) ^ (1 - half)
    reach = jnp.where(parity == 0, row_reach[0, 0], row_reach[0, 1])
    info = jnp.stack([reach, half]).astype(jnp.int32)
    halves = [[t * space + s for t in range(tm) for s in pair] for pair in ((1, 0), (2, 3))]
    swap = lambda v: lax.all_to_all(v, ("tm", "space"), split_axis=0, concat_axis=0, axis_index_groups=halves, tiled=True)
    arrived = swap(clip_tokens.reshape(frame_count, rows, cols, D))
    cot = cotangent.reshape(frames, rows, wide, D).swapaxes(0, 1)
    arrived = arrived.reshape(tm, frames, rows, cols, D)
    edge_rows = edge_norm(info, arrived, spatial_gain)
    halo = lax.ppermute(edge_rows, "space", [(i, space - 1 - i) for i in range(space)])
    cot, arrived = lax.optimization_barrier((cot, arrived))
    cot = exchange(cot, "tm")
    qkv, tok = qkv_own(info, arrived, spatial_gain, spatial_heads)
    middle = spatial_phase(info, halo, qkv, tok, spatial_heads, spatial_merge)
    mid = swap(middle.reshape(frame_count, wide, D))
    core = jnp.stack([lax.axis_index("batch") & 1, here]).astype(jnp.int32)
    out, send, keep = temporal_phase(
        core, mid, frame_order.reshape(frame_count), temporal_gain, cot.reshape(frame_count, wide, D),
        temporal_heads, temporal_merge, space, tm,
    )
    batch = lax.axis_size("batch")
    got = lax.ppermute(send, "batch", [(i, i ^ 1) for i in range(batch)])
    output = exchange(out.reshape(tm, frames, wide, D), "tm").swapaxes(0, 1)
    chip = [keep[k].astype(F32) + got[k].astype(F32) for k in range(1, space)]
    moved = [lax.ppermute(chip[k - 1].astype(BF), "space", [(i, (i + k) % space) for i in range(space)])
             for k in range(1, space)]
    own = own_slot(keep, got)
    over_space = space_sum(own, moved)
    over_tm = exchange(over_space, "tm")
    over_tm = over_tm.astype(F32).sum(0).astype(BF)
    block = over_tm.shape[0]
    parts = lax.all_gather(over_tm, "batch").astype(F32).reshape(batch // 2, 2, block, D // 2).sum(0)
    weight_grad = parts.swapaxes(0, 1).reshape(block, D)
    return (output.reshape(1, frames, rows, wide, D), weight_grad)


def solution(mesh):
    in_specs = (
        P("batch", None, "space", "tm", None),
        P("batch", None),
        P("batch", "tm"),
        P(),
        P(),
        P(),
        P(),
        P(),
        P(),
        P("batch", "tm", "space", None, None),
    )
    out_specs = (P("batch", "tm", "space", None, None), P(("tm", "space"), None))

    return jax.shard_map(per_device, mesh=mesh, in_specs=in_specs, out_specs=out_specs, check_vma=False)
```

```python
import jax
import jax.numpy as jnp
from jax import lax
from jax.experimental import pallas as pl
from jax.experimental.pallas import tpu as pltpu
from jax.sharding import PartitionSpec as P


HALO = 4
D = 1024
HEADS = 16
HEAD_DIM = 64
PAIRS = HEADS // 2
WIDE = 2 * HEAD_DIM
FLOOR = 0.5
SCALE = HEAD_DIM ** (-0.5) * 1.4426950408889634
BF = jnp.bfloat16
F32 = jnp.float32
MASKED = -1e30


def normalized(x, gain):
    return x * lax.rsqrt(jnp.mean(x * x, axis=-1, keepdims=True) + FLOOR) * gain


def in_vmem(x):
    return pltpu.with_memory_space_constraint(x, pltpu.VMEM)


def in_hbm(x):
    return pltpu.with_memory_space_constraint(x, pltpu.HBM)


VMEM = pl.BlockSpec(memory_space=pltpu.VMEM)
SMEM = pl.BlockSpec(memory_space=pltpu.SMEM)
HBM = pl.BlockSpec(memory_space=pltpu.HBM)


def edge_kernel(info_ref, x_ref, gain_ref, edge_ref):
    times, _, rows, cols, _ = x_ref.shape
    start = jnp.where(info_ref[1] == 0, rows - HALO, 0)
    gain = gain_ref[...]
    for r in range(HALO):
        for t in range(times):
            y = normalized(x_ref[t, 0, start + r].astype(F32), gain)
            edge_ref[r, t * cols:(t + 1) * cols, :] = y.astype(BF)


def edge_norm(info, arrived, gain):
    times, _, _, cols, _ = arrived.shape
    return pl.pallas_call(
        edge_kernel,
        in_specs=[SMEM, VMEM, VMEM],
        out_specs=VMEM,
        out_shape=pltpu.VMEM((HALO, times * cols, D), BF),
        compiler_params=pltpu.CompilerParams(vmem_limit_bytes=4 * 2**20),
        name="edge_norm",
    )(info, in_vmem(arrived), gain.reshape(1, D))


def column_copies(w_ref, buf, sems, columns):
    return [pltpu.make_async_copy(w_ref.at[:, c * D:(c + 1) * D], buf.at[i], sems.at[i]) for i, c in enumerate(columns)]


QKV_PIECE = 1024


def qkv_kernel(info_ref, arrived_ref, gain_ref, w_ref, out_ref, tok_out, x_ref, tok_ref, buf, y_ref, sems, out_sems, tok_sems):
    pieces = buf.shape[0]
    copies = [pltpu.make_async_copy(w_ref.at[:, i * QKV_PIECE:(i + 1) * QKV_PIECE], buf.at[i], sems.at[i])
              for i in range(pieces)]
    for c in copies:
        c.start()
    times, parities, rows, cols, _ = arrived_ref.shape
    wide = times * cols
    half = info_ref[1]
    gain = gain_ref[...]
    kept = []
    for o in range(parities):
        first = jnp.where(half == 0, 1 - o, o) * rows

        def one_row(r, carry):
            for t in range(times):
                x = arrived_ref[t, o, r]
                y = normalized(x.astype(F32), gain).astype(BF)
                tok_ref[first + r, t * cols:(t + 1) * cols, :] = x
                x_ref[first + r, t * cols:(t + 1) * cols, :] = y
            return carry

        lax.fori_loop(0, rows, one_row, 0)
        done = pl.ds(first, rows)
        kept.append(pltpu.make_async_copy(tok_ref.at[done], tok_out.at[done], tok_sems.at[o]))
        kept[o].start()
    sent = []
    x = x_ref[...].reshape(parities * rows * wide, D)
    for i, c in enumerate(copies):
        c.wait()
        y_ref[i] = jnp.dot(x, buf[i], preferred_element_type=F32).astype(BF)
        third, at = divmod(i * QKV_PIECE, D)
        sent.append(pltpu.make_async_copy(y_ref.at[i], out_ref.at[third, :, at:at + QKV_PIECE], out_sems.at[i]))
        sent[i].start()
    for c in sent + kept:
        c.wait()


def qkv_own(info, arrived, gain, heads):
    times, parities, rows, cols, _ = arrived.shape
    shape = (parities * rows, times * cols, D)
    tokens = shape[0] * shape[1]
    pieces = 3 * D // QKV_PIECE
    return pl.pallas_call(
        qkv_kernel,
        in_specs=[SMEM, VMEM, VMEM, HBM],
        out_specs=[HBM, HBM],
        out_shape=[pltpu.HBM((3, tokens, D), BF), pltpu.HBM(shape, BF)],
        scratch_shapes=[pltpu.VMEM(shape, BF), pltpu.VMEM(shape, BF),
                        pltpu.VMEM((pieces, D, QKV_PIECE), BF), pltpu.VMEM((pieces, tokens, QKV_PIECE), BF),
                        pltpu.SemaphoreType.DMA((pieces,)), pltpu.SemaphoreType.DMA((pieces,)),
                        pltpu.SemaphoreType.DMA((2,))],
        compiler_params=pltpu.CompilerParams(vmem_limit_bytes=28 * 2**20),
        name="qkv_own",
    )(info, in_vmem(arrived), gain.reshape(1, D), in_hbm(heads))


def staged_attention(items):
    n = items[0][0]().shape[0]
    low = lax.broadcasted_iota(jnp.int32, (n, WIDE), 1) < HEAD_DIM
    scores, weights = [], []
    for q, k, v, bias, ref, at in items:
        q = q()
        zero = jnp.zeros_like(q)
        both = jnp.concatenate([jnp.where(low, q, zero), jnp.where(low, zero, q)], axis=0)
        scores.append(lax.dot_general(both, k(), (((1,), (1,)), ((), ())), preferred_element_type=F32))
    for s, (q, k, v, bias, ref, at) in zip(scores, items):
        b = bias()
        s = s * SCALE + jnp.concatenate([b, b], axis=0)
        weights.append(jnp.exp2(s - jnp.max(s, axis=-1, keepdims=True)).astype(BF))
    for p, (q, k, v, bias, ref, at) in zip(weights, items):
        v = v()
        o = jnp.dot(p, jnp.concatenate([v, jnp.ones_like(v)], axis=1), preferred_element_type=F32)
        o = o[:, :WIDE] / o[:, WIDE:]
        ref[at] = jnp.where(low, o[:n], o[n:]).astype(BF)


def reader(ref, *at):
    return lambda: ref[at]


SPATIAL_STAGE = 4
TEMPORAL_STAGE = 16


def spatial_kernel(info_ref, halo_ref, qkv_ref, tok_ref, w_ref, wm_ref, mid_out,
                   q_ref, tok_buf, mid_buf, wkv_buf, wm_buf, k_ref, v_ref, ctx_ref, bias_ref, sems):
    rows, cols, _ = tok_buf.shape
    tokens = rows * cols
    edge = HALO * cols
    reach, half = info_ref[0], info_ref[1]
    weights = column_copies(w_ref, wkv_buf, sems, (1, 2))
    own = [pltpu.make_async_copy(qkv_ref.at[0], q_ref, sems.at[2])]
    for i, buf in ((1, k_ref), (2, v_ref)):
        own.append(pltpu.make_async_copy(qkv_ref.at[i], buf.at[edge:edge + tokens], sems.at[2 + i]))
    last = [pltpu.make_async_copy(wm_ref, wm_buf, sems.at[5]), pltpu.make_async_copy(tok_ref, tok_buf, sems.at[6])]
    for c in own + weights + last:
        c.start()
    blocks, n, extent = bias_ref.shape
    qrow = lax.broadcasted_iota(jnp.int32, (n, extent), 0) // cols
    krow = lax.broadcasted_iota(jnp.int32, (n, extent), 1) // cols - HALO
    near = jnp.abs(krow - qrow) <= reach
    for j in range(blocks):
        at = krow + (j * HALO + half * rows)
        bias_ref[j] = jnp.where(near & (at >= 0) & (at < 2 * rows), 0.0, MASKED)
    for c in own:
        c.wait()

    def attend(chosen):
        items = []
        for pair in range(PAIRS):
            at = slice(pair * WIDE, (pair + 1) * WIDE)
            for j in chosen:
                keys = slice(j * edge, j * edge + extent)
                mine = slice(j * n, (j + 1) * n)
                items.append((reader(q_ref, mine, at), reader(k_ref, keys, at), reader(v_ref, keys, at),
                              reader(bias_ref, j), ctx_ref, (mine, at)))
        for i in range(0, len(items), SPATIAL_STAGE):
            staged_attention(items[i:i + SPATIAL_STAGE])

    inner = [j for j in range(blocks) if j * edge >= edge and j * edge + extent <= edge + tokens]
    attend(inner)
    there = jnp.where(half == 0, edge + tokens, 0)
    empty = jnp.where(half == 0, 0, edge + tokens)
    halo = halo_ref[...].reshape(edge, D)
    for c, w, buf in zip(weights, range(2), (k_ref, v_ref)):
        c.wait()
        side = jnp.dot(halo, wkv_buf[w], preferred_element_type=F32).astype(BF)
        buf[pl.ds(pl.multiple_of(there, edge), edge)] = side
        buf[pl.ds(pl.multiple_of(empty, edge), edge)] = jnp.zeros_like(side)
    attend([j for j in range(blocks) if j not in inner])
    for c in last:
        c.wait()
    sent = []
    part, strip = rows // 2, tokens // 2
    for i in range(2):
        mid = jnp.dot(ctx_ref[i * strip:(i + 1) * strip], wm_buf[...], preferred_element_type=F32)
        mid = mid + tok_buf[i * part:(i + 1) * part].reshape(strip, D).astype(F32)
        mid_buf[i] = mid.astype(BF).reshape(part, cols, D)
        parity = jnp.where(half == 0, 1 - i, i)
        sent.append(pltpu.make_async_copy(mid_buf.at[i], mid_out.at[:, parity], sems.at[7 + i]))
        sent[i].start()
    for c in sent:
        c.wait()


def spatial_phase(info, halo, qkv, tok, heads, merge):
    rows, cols, _ = tok.shape
    tokens = rows * cols
    edge = HALO * cols
    extent = tokens + 2 * edge
    return pl.pallas_call(
        spatial_kernel,
        in_specs=[SMEM, VMEM, HBM, HBM, HBM, HBM],
        out_specs=HBM,
        out_shape=pltpu.HBM((rows // 2, 2, cols, D), BF),
        scratch_shapes=[pltpu.VMEM((tokens, D), BF), pltpu.VMEM((rows, cols, D), BF),
                        pltpu.VMEM((2, rows // 2, cols, D), BF),
                        pltpu.VMEM((2, D, D), BF), pltpu.VMEM((D, D), BF),
                        pltpu.VMEM((extent, D), BF), pltpu.VMEM((extent, D), BF),
                        pltpu.VMEM((tokens, D), BF), pltpu.VMEM((tokens // edge, edge, 3 * edge), F32),
                        pltpu.SemaphoreType.DMA((9,))],
        compiler_params=pltpu.CompilerParams(vmem_limit_bytes=40 * 2**20),
        name="spatial_phase",
    )(info, in_vmem(halo), *[in_hbm(v) for v in (qkv, tok, heads, merge)])


GROUP = 8


def temporal_kernel(core_ref, mid_ref, order_q_ref, order_k_ref, gain_ref, w_ref, wm_ref, *refs):
    cot_refs, refs = refs[:-15], refs[-15:]
    (out_hbm, send_ref, keep_hbm, out_ref, keep_ref, wqkv_buf, wm_buf, cot_buf, normed_ref,
     q_ref, k_ref, v_ref, ctx_ref, cotb_ref, sems) = refs
    frames, cols, _ = mid_ref.shape
    groups = cols // GROUP
    n = frames * GROUP
    copies = column_copies(w_ref, wqkv_buf, sems, range(3))
    copies.append(pltpu.make_async_copy(wm_ref, wm_buf, sems.at[4]))
    times = len(cot_refs)
    pair = frames // times
    for i, ref in enumerate(cot_refs):
        source = lax.rem(core_ref[2] + times - i, times)
        copies.append(pltpu.make_async_copy(ref, cot_buf.at[pl.ds(source * pair, pair)], sems.at[7 + i]))
    for c in copies:
        c.start()
    gain = gain_ref[...]
    for g in range(groups):
        x = mid_ref[:, g * GROUP:(g + 1) * GROUP, :].astype(F32).reshape(n, D)
        normed_ref[g * n:(g + 1) * n] = normalized(x, gain).astype(BF)
    for i, buf in enumerate((q_ref, k_ref, v_ref)):
        copies[i].wait()
        buf[...] = jnp.dot(normed_ref[...], wqkv_buf[i], preferred_element_type=F32).astype(BF)
    for c in copies[4:]:
        c.wait()
    for g in range(groups):
        cotb_ref[g * n:(g + 1) * n] = cot_buf[:, g * GROUP:(g + 1) * GROUP, :].astype(F32).reshape(n, D).astype(BF)
    place_q = lax.broadcasted_iota(jnp.int32, (n, n), 0) % GROUP
    place_k = lax.broadcasted_iota(jnp.int32, (n, n), 1) % GROUP
    allowed = (place_q == place_k) & (order_k_ref[...] <= order_q_ref[...])
    bias = jnp.where(allowed, 0.0, MASKED)
    items = []
    for g in range(groups):
        own = slice(g * n, (g + 1) * n)
        for pair in range(PAIRS):
            at = slice(pair * WIDE, (pair + 1) * WIDE)
            items.append((reader(q_ref, own, at), reader(k_ref, own, at), reader(v_ref, own, at), lambda: bias,
                          ctx_ref, (own, at)))
    for i in range(0, len(items), TEMPORAL_STAGE):
        staged_attention(items[i:i + TEMPORAL_STAGE])
    core = core_ref[0]
    here = core_ref[1]
    half = D // 2
    for ref, which in ((send_ref, 1 - core), (keep_ref, core)):
        cot = cotb_ref[:, pl.ds(pl.multiple_of(which * half, half), half)]
        grad = lax.dot_general(ctx_ref[...], cot, (((0,), (0,)), ((), ())), preferred_element_type=F32).astype(BF)
        spaces, times, block, _ = ref.shape
        for s in range(spaces):
            slot = lax.rem(s + spaces - here, spaces)
            for t in range(times):
                row = (t * spaces + s) * block
                ref[slot, t] = grad[row:row + block]
    kept = pltpu.make_async_copy(keep_ref, keep_hbm, sems.at[5])
    kept.start()
    copies[3].wait()
    y = jnp.dot(ctx_ref[...], wm_buf[...], preferred_element_type=F32)
    for g in range(groups):
        x = mid_ref[:, g * GROUP:(g + 1) * GROUP, :].astype(F32) + y[g * n:(g + 1) * n].reshape(frames, GROUP, D)
        out_ref[:, g * GROUP:(g + 1) * GROUP, :] = x.astype(BF)
    done = pltpu.make_async_copy(out_ref, out_hbm, sems.at[6])
    done.start()
    done.wait()
    kept.wait()


def temporal_phase(core, mid, order, gain, cot, heads, merge, spaces, times):
    frames, cols, _ = mid.shape
    n = frames * GROUP
    tokens = frames * cols
    spread = jnp.repeat(order, GROUP)
    block = D // (spaces * times)
    part = (spaces, times, block, D // 2)
    return pl.pallas_call(
        temporal_kernel,
        in_specs=[SMEM] + [VMEM] * 4 + [HBM] * (2 + len(cot)),
        out_specs=[HBM, VMEM, HBM],
        out_shape=[pltpu.HBM((frames, cols, D), BF), pltpu.VMEM(part, BF), pltpu.HBM(part, BF)],
        scratch_shapes=[pltpu.VMEM((frames, cols, D), BF), pltpu.VMEM(part, BF), pltpu.VMEM((3, D, D), BF), pltpu.VMEM((D, D), BF), pltpu.VMEM((frames, cols, D), BF)]
        + [pltpu.VMEM((tokens, D), BF)] * 6
        + [pltpu.SemaphoreType.DMA((7 + len(cot),))],
        compiler_params=pltpu.CompilerParams(vmem_limit_bytes=40 * 2**20),
        name="temporal_phase",
    )(core, in_vmem(mid), spread.reshape(n, 1), spread.reshape(1, n), gain.reshape(1, D),
      in_hbm(heads), in_hbm(merge), *[in_hbm(c) for c in cot])


def own_kernel(keep_ref, got_ref, out_ref):
    out_ref[...] = keep_ref[...].astype(F32) + got_ref[...].astype(F32)


def own_slot(keep, got):
    shape = keep.shape[1:]
    first = pl.BlockSpec((None,) + shape, lambda i: (0, 0, 0, 0))
    return pl.pallas_call(
        own_kernel,
        grid=(1,),
        in_specs=[first, first],
        out_specs=pl.BlockSpec(shape, lambda i: (0, 0, 0)),
        out_shape=jax.ShapeDtypeStruct(shape, F32),
        compiler_params=pltpu.CompilerParams(vmem_limit_bytes=8 * 2**20),
        name="own_slot",
    )(in_hbm(keep), got)


def sum_kernel(own_ref, *refs):
    total = own_ref[...]
    for p in refs[:-1]:
        total = total + p[...].astype(F32)
    refs[-1][0] = total.astype(BF)
    refs[-1][1] = refs[-1][0]


def space_sum(own, moved):
    return pl.pallas_call(
        sum_kernel,
        in_specs=[VMEM] * (1 + len(moved)),
        out_specs=VMEM,
        out_shape=pltpu.VMEM((2,) + own.shape, BF),
        compiler_params=pltpu.CompilerParams(vmem_limit_bytes=8 * 2**20),
        name="space_sum",
    )(in_vmem(own), *[in_vmem(p) for p in moved])


def per_device(
    clip_tokens,
    frame_order,
    row_reach,
    spatial_gain,
    spatial_heads,
    spatial_merge,
    temporal_gain,
    temporal_heads,
    temporal_merge,
    cotangent,
):
    tm, space = lax.axis_size("tm"), lax.axis_size("space")
    _, frame_count, rows, cols, _ = clip_tokens.shape
    frames = frame_count // tm
    wide = tm * cols
    exchange = lambda v, axis: lax.all_to_all(v, axis, split_axis=0, concat_axis=0, tiled=True)

    here = lax.axis_index("space").astype(jnp.int32)
    half = here >> 1
    parity = (here & 1) ^ (1 - half)
    reach = jnp.where(parity == 0, row_reach[0, 0], row_reach[0, 1])
    info = jnp.stack([reach, half]).astype(jnp.int32)
    halves = [[t * space + s for t in range(tm) for s in pair] for pair in ((1, 0), (2, 3))]
    swap = lambda v: lax.all_to_all(v, ("tm", "space"), split_axis=0, concat_axis=0, axis_index_groups=halves, tiled=True)
    arrived = swap(clip_tokens.reshape(frame_count, rows, cols, D))
    time = lax.axis_index("tm").astype(jnp.int32)
    rows_of = cotangent.reshape(frames, rows, wide, D)
    cot = [lax.dynamic_index_in_dim(rows_of, (time + k) % tm, 1, keepdims=False) for k in range(tm)]
    cot[1:] = [lax.ppermute(cot[k], "tm", [(i, (i + k) % tm) for i in range(tm)]) for k in range(1, tm)]
    arrived = arrived.reshape(tm, frames, rows, cols, D)
    edge_rows = edge_norm(info, arrived, spatial_gain)
    halo = lax.ppermute(edge_rows, "space", [(i, space - 1 - i) for i in range(space)])
    qkv, tok = qkv_own(info, arrived, spatial_gain, spatial_heads)
    middle = spatial_phase(info, halo, qkv, tok, spatial_heads, spatial_merge)
    mid = swap(middle.reshape(frame_count, wide, D))
    core = jnp.stack([lax.axis_index("batch") & 1, here, time]).astype(jnp.int32)
    out, send, keep = temporal_phase(
        core, mid, frame_order.reshape(frame_count), temporal_gain, cot,
        temporal_heads, temporal_merge, space, tm,
    )
    batch = lax.axis_size("batch")
    got = lax.ppermute(send, "batch", [(i, i ^ 1) for i in range(batch)])
    output = exchange(out.reshape(tm, frames, wide, D), "tm").swapaxes(0, 1)
    chip = [keep[k].astype(F32) + got[k].astype(F32) for k in range(1, space)]
    moved = [lax.ppermute(chip[k - 1].astype(BF), "space", [(i, (i + k) % space) for i in range(space)])
             for k in range(1, space)]
    own = own_slot(keep, got)
    over_space = space_sum(own, moved)
    planes = [[(2 * y + c) * tm + t for y in range(batch // 2) for t in range(tm)] for c in range(2)]
    pieces = lax.all_to_all(
        over_space.reshape(2 * tm, *over_space.shape[2:]), ("batch", "tm"), split_axis=0, concat_axis=0,
        axis_index_groups=planes, tiled=True,
    )
    mine = pieces.astype(F32).sum(0).astype(BF)
    other = lax.ppermute(mine, "batch", [(i, i ^ 1) for i in range(batch)])
    weight_grad = jnp.where(
        core[0] == 0, jnp.concatenate([mine, other], axis=1), jnp.concatenate([other, mine], axis=1)
    ).astype(F32)
    return (output.reshape(1, frames, rows, wide, D), weight_grad)


def solution(mesh):
    in_specs = (
        P("batch", None, "space", "tm", None),
        P("batch", None),
        P("batch", "tm"),
        P(),
        P(),
        P(),
        P(),
        P(),
        P(),
        P("batch", "tm", "space", None, None),
    )
    out_specs = (P("batch", "tm", "space", None, None), P(("tm", "space"), None))

    return jax.shard_map(per_device, mesh=mesh, in_specs=in_specs, out_specs=out_specs, check_vma=False)
```

```python
import jax
import jax.numpy as jnp
from jax import lax
from jax.experimental import pallas as pl
from jax.experimental.pallas import tpu as pltpu
from jax.sharding import PartitionSpec as P


HALO = 4
D = 1024
HEADS = 16
HEAD_DIM = 64
PAIRS = HEADS // 2
WIDE = 2 * HEAD_DIM
FLOOR = 0.5
SCALE = HEAD_DIM ** (-0.5) * 1.4426950408889634
BF = jnp.bfloat16
F32 = jnp.float32
MASKED = -1e30


def normalized(x, gain):
    return x * lax.rsqrt(jnp.mean(x * x, axis=-1, keepdims=True) + FLOOR) * gain


def in_vmem(x):
    return pltpu.with_memory_space_constraint(x, pltpu.VMEM)


def in_hbm(x):
    return pltpu.with_memory_space_constraint(x, pltpu.HBM)


VMEM = pl.BlockSpec(memory_space=pltpu.VMEM)
SMEM = pl.BlockSpec(memory_space=pltpu.SMEM)
HBM = pl.BlockSpec(memory_space=pltpu.HBM)


def edge_kernel(info_ref, x_ref, gain_ref, edge_ref):
    times, _, rows, cols, _ = x_ref.shape
    start = jnp.where(info_ref[1] == 0, rows - HALO, 0)
    gain = gain_ref[...]
    for r in range(HALO):
        for t in range(times):
            y = normalized(x_ref[t, 0, start + r].astype(F32), gain)
            edge_ref[r, t * cols:(t + 1) * cols, :] = y.astype(BF)


def edge_norm(info, arrived, gain):
    times, _, _, cols, _ = arrived.shape
    return pl.pallas_call(
        edge_kernel,
        in_specs=[SMEM, VMEM, VMEM],
        out_specs=VMEM,
        out_shape=pltpu.VMEM((HALO, times * cols, D), BF),
        compiler_params=pltpu.CompilerParams(vmem_limit_bytes=4 * 2**20),
        name="edge_norm",
    )(info, in_vmem(arrived), gain.reshape(1, D))


def column_copies(w_ref, buf, sems, columns):
    return [pltpu.make_async_copy(w_ref.at[:, c * D:(c + 1) * D], buf.at[i], sems.at[i]) for i, c in enumerate(columns)]


QKV_PIECE = 1024


def qkv_kernel(info_ref, arrived_ref, gain_ref, w_ref, out_ref, tok_out, x_ref, tok_ref, buf, y_ref, sems, out_sems, tok_sems):
    pieces = buf.shape[0]
    copies = [pltpu.make_async_copy(w_ref.at[:, i * QKV_PIECE:(i + 1) * QKV_PIECE], buf.at[i], sems.at[i])
              for i in range(pieces)]
    for c in copies:
        c.start()
    times, parities, rows, cols, _ = arrived_ref.shape
    wide = times * cols
    half = info_ref[1]
    gain = gain_ref[...]
    kept = []
    for o in range(parities):
        first = jnp.where(half == 0, 1 - o, o) * rows

        def one_row(r, carry):
            for t in range(times):
                x = arrived_ref[t, o, r]
                y = normalized(x.astype(F32), gain).astype(BF)
                tok_ref[first + r, t * cols:(t + 1) * cols, :] = x
                x_ref[first + r, t * cols:(t + 1) * cols, :] = y
            return carry

        lax.fori_loop(0, rows, one_row, 0)
        done = pl.ds(first, rows)
        kept.append(pltpu.make_async_copy(tok_ref.at[done], tok_out.at[done], tok_sems.at[o]))
        kept[o].start()
    sent = []
    x = x_ref[...].reshape(parities * rows * wide, D)
    for i, c in enumerate(copies):
        c.wait()
        y_ref[i] = jnp.dot(x, buf[i], preferred_element_type=F32).astype(BF)
        third, at = divmod(i * QKV_PIECE, D)
        sent.append(pltpu.make_async_copy(y_ref.at[i], out_ref.at[third, :, at:at + QKV_PIECE], out_sems.at[i]))
        sent[i].start()
    for c in sent + kept:
        c.wait()


def qkv_own(info, arrived, gain, heads):
    times, parities, rows, cols, _ = arrived.shape
    shape = (parities * rows, times * cols, D)
    tokens = shape[0] * shape[1]
    pieces = 3 * D // QKV_PIECE
    return pl.pallas_call(
        qkv_kernel,
        in_specs=[SMEM, VMEM, VMEM, HBM],
        out_specs=[HBM, HBM],
        out_shape=[pltpu.HBM((3, tokens, D), BF), pltpu.HBM(shape, BF)],
        scratch_shapes=[pltpu.VMEM(shape, BF), pltpu.VMEM(shape, BF),
                        pltpu.VMEM((pieces, D, QKV_PIECE), BF), pltpu.VMEM((pieces, tokens, QKV_PIECE), BF),
                        pltpu.SemaphoreType.DMA((pieces,)), pltpu.SemaphoreType.DMA((pieces,)),
                        pltpu.SemaphoreType.DMA((2,))],
        compiler_params=pltpu.CompilerParams(vmem_limit_bytes=28 * 2**20),
        name="qkv_own",
    )(info, in_vmem(arrived), gain.reshape(1, D), in_hbm(heads))


def staged_attention(items):
    n = items[0][0]().shape[0]
    low = lax.broadcasted_iota(jnp.int32, (n, WIDE), 1) < HEAD_DIM
    scores, weights = [], []
    for q, k, v, bias, ref, at in items:
        q = q()
        zero = jnp.zeros_like(q)
        both = jnp.concatenate([jnp.where(low, q, zero), jnp.where(low, zero, q)], axis=0)
        scores.append(lax.dot_general(both, k(), (((1,), (1,)), ((), ())), preferred_element_type=F32))
    for s, (q, k, v, bias, ref, at) in zip(scores, items):
        b = bias()
        s = s * SCALE + jnp.concatenate([b, b], axis=0)
        weights.append(jnp.exp2(s - jnp.max(s, axis=-1, keepdims=True)).astype(BF))
    for p, (q, k, v, bias, ref, at) in zip(weights, items):
        v = v()
        o = jnp.dot(p, jnp.concatenate([v, jnp.ones_like(v)], axis=1), preferred_element_type=F32)
        o = o[:, :WIDE] / o[:, WIDE:]
        ref[at] = jnp.where(low, o[:n], o[n:]).astype(BF)


def reader(ref, *at):
    return lambda: ref[at]


SPATIAL_STAGE = 4
TEMPORAL_STAGE = 16


def spatial_kernel(info_ref, halo_ref, qkv_ref, tok_ref, w_ref, wm_ref, mid_out,
                   q_ref, tok_buf, mid_buf, wkv_buf, wm_buf, k_ref, v_ref, ctx_ref, bias_ref, sems):
    rows, cols, _ = tok_buf.shape
    tokens = rows * cols
    edge = HALO * cols
    reach, half = info_ref[0], info_ref[1]
    weights = column_copies(w_ref, wkv_buf, sems, (1, 2))
    own = [pltpu.make_async_copy(qkv_ref.at[0], q_ref, sems.at[2])]
    for i, buf in ((1, k_ref), (2, v_ref)):
        own.append(pltpu.make_async_copy(qkv_ref.at[i], buf.at[edge:edge + tokens], sems.at[2 + i]))
    last = [pltpu.make_async_copy(wm_ref, wm_buf, sems.at[5]), pltpu.make_async_copy(tok_ref, tok_buf, sems.at[6])]
    for c in own + weights + last:
        c.start()
    blocks, n, extent = bias_ref.shape
    qrow = lax.broadcasted_iota(jnp.int32, (n, extent), 0) // cols
    krow = lax.broadcasted_iota(jnp.int32, (n, extent), 1) // cols - HALO
    near = jnp.abs(krow - qrow) <= reach
    for j in range(blocks):
        at = krow + (j * HALO + half * rows)
        bias_ref[j] = jnp.where(near & (at >= 0) & (at < 2 * rows), 0.0, MASKED)
    for c in own:
        c.wait()

    def attend(chosen):
        items = []
        for pair in range(PAIRS):
            at = slice(pair * WIDE, (pair + 1) * WIDE)
            for j in chosen:
                keys = slice(j * edge, j * edge + extent)
                mine = slice(j * n, (j + 1) * n)
                items.append((reader(q_ref, mine, at), reader(k_ref, keys, at), reader(v_ref, keys, at),
                              reader(bias_ref, j), ctx_ref, (mine, at)))
        for i in range(0, len(items), SPATIAL_STAGE):
            staged_attention(items[i:i + SPATIAL_STAGE])

    inner = [j for j in range(blocks) if j * edge >= edge and j * edge + extent <= edge + tokens]
    attend(inner)
    there = jnp.where(half == 0, edge + tokens, 0)
    empty = jnp.where(half == 0, 0, edge + tokens)
    halo = halo_ref[...].reshape(edge, D)
    for c, w, buf in zip(weights, range(2), (k_ref, v_ref)):
        c.wait()
        side = jnp.dot(halo, wkv_buf[w], preferred_element_type=F32).astype(BF)
        buf[pl.ds(pl.multiple_of(there, edge), edge)] = side
        buf[pl.ds(pl.multiple_of(empty, edge), edge)] = jnp.zeros_like(side)
    attend([j for j in range(blocks) if j not in inner])
    for c in last:
        c.wait()
    sent = []
    part, strip = rows // 2, tokens // 2
    for i in range(2):
        mid = jnp.dot(ctx_ref[i * strip:(i + 1) * strip], wm_buf[...], preferred_element_type=F32)
        mid = mid + tok_buf[i * part:(i + 1) * part].reshape(strip, D).astype(F32)
        mid_buf[i] = mid.astype(BF).reshape(part, cols, D)
        parity = jnp.where(half == 0, 1 - i, i)
        sent.append(pltpu.make_async_copy(mid_buf.at[i], mid_out.at[:, parity], sems.at[7 + i]))
        sent[i].start()
    for c in sent:
        c.wait()


def spatial_phase(info, halo, qkv, tok, heads, merge):
    rows, cols, _ = tok.shape
    tokens = rows * cols
    edge = HALO * cols
    extent = tokens + 2 * edge
    return pl.pallas_call(
        spatial_kernel,
        in_specs=[SMEM, VMEM, HBM, HBM, HBM, HBM],
        out_specs=HBM,
        out_shape=pltpu.HBM((rows // 2, 2, cols, D), BF),
        scratch_shapes=[pltpu.VMEM((tokens, D), BF), pltpu.VMEM((rows, cols, D), BF),
                        pltpu.VMEM((2, rows // 2, cols, D), BF),
                        pltpu.VMEM((2, D, D), BF), pltpu.VMEM((D, D), BF),
                        pltpu.VMEM((extent, D), BF), pltpu.VMEM((extent, D), BF),
                        pltpu.VMEM((tokens, D), BF), pltpu.VMEM((tokens // edge, edge, 3 * edge), F32),
                        pltpu.SemaphoreType.DMA((9,))],
        compiler_params=pltpu.CompilerParams(vmem_limit_bytes=40 * 2**20),
        name="spatial_phase",
    )(info, in_vmem(halo), *[in_hbm(v) for v in (qkv, tok, heads, merge)])


GROUP = 8


def temporal_kernel(core_ref, mid_ref, order_q_ref, order_k_ref, gain_ref, cot_ref, w_ref, wm_ref,
                    out_hbm, send_ref, keep_hbm,
                    out_ref, keep_ref, wqkv_buf, wm_buf, cot_buf, normed_ref, q_ref, k_ref, v_ref, ctx_ref, cotb_ref, sems):
    frames, cols, _ = mid_ref.shape
    groups = cols // GROUP
    n = frames * GROUP
    copies = column_copies(w_ref, wqkv_buf, sems, range(3))
    copies.append(pltpu.make_async_copy(cot_ref, cot_buf, sems.at[3]))
    copies.append(pltpu.make_async_copy(wm_ref, wm_buf, sems.at[4]))
    for c in copies:
        c.start()
    gain = gain_ref[...]
    for g in range(groups):
        x = mid_ref[:, g * GROUP:(g + 1) * GROUP, :].astype(F32).reshape(n, D)
        normed_ref[g * n:(g + 1) * n] = normalized(x, gain).astype(BF)
    for i, buf in enumerate((q_ref, k_ref, v_ref)):
        copies[i].wait()
        buf[...] = jnp.dot(normed_ref[...], wqkv_buf[i], preferred_element_type=F32).astype(BF)
    copies[3].wait()
    for g in range(groups):
        cotb_ref[g * n:(g + 1) * n] = cot_buf[:, g * GROUP:(g + 1) * GROUP, :].astype(F32).reshape(n, D).astype(BF)
    place_q = lax.broadcasted_iota(jnp.int32, (n, n), 0) % GROUP
    place_k = lax.broadcasted_iota(jnp.int32, (n, n), 1) % GROUP
    allowed = (place_q == place_k) & (order_k_ref[...] <= order_q_ref[...])
    bias = jnp.where(allowed, 0.0, MASKED)
    items = []
    for g in range(groups):
        own = slice(g * n, (g + 1) * n)
        for pair in range(PAIRS):
            at = slice(pair * WIDE, (pair + 1) * WIDE)
            items.append((reader(q_ref, own, at), reader(k_ref, own, at), reader(v_ref, own, at), lambda: bias,
                          ctx_ref, (own, at)))
    for i in range(0, len(items), TEMPORAL_STAGE):
        staged_attention(items[i:i + TEMPORAL_STAGE])
    core = core_ref[0]
    here = core_ref[1]
    half = D // 2
    for ref, which in ((send_ref, 1 - core), (keep_ref, core)):
        cot = cotb_ref[:, pl.ds(pl.multiple_of(which * half, half), half)]
        grad = lax.dot_general(ctx_ref[...], cot, (((0,), (0,)), ((), ())), preferred_element_type=F32).astype(BF)
        spaces, times, block, _ = ref.shape
        for s in range(spaces):
            slot = lax.rem(s + spaces - here, spaces)
            for t in range(times):
                row = (t * spaces + s) * block
                ref[slot, t] = grad[row:row + block]
    kept = pltpu.make_async_copy(keep_ref, keep_hbm, sems.at[5])
    kept.start()
    copies[4].wait()
    y = jnp.dot(ctx_ref[...], wm_buf[...], preferred_element_type=F32)
    for g in range(groups):
        x = mid_ref[:, g * GROUP:(g + 1) * GROUP, :].astype(F32) + y[g * n:(g + 1) * n].reshape(frames, GROUP, D)
        out_ref[:, g * GROUP:(g + 1) * GROUP, :] = x.astype(BF)
    done = pltpu.make_async_copy(out_ref, out_hbm, sems.at[6])
    done.start()
    done.wait()
    kept.wait()


def temporal_phase(core, mid, order, gain, cot, heads, merge, spaces, times):
    frames, cols, _ = mid.shape
    n = frames * GROUP
    tokens = frames * cols
    spread = jnp.repeat(order, GROUP)
    block = D // (spaces * times)
    part = (spaces, times, block, D // 2)
    return pl.pallas_call(
        temporal_kernel,
        in_specs=[SMEM] + [VMEM] * 4 + [HBM] * 3,
        out_specs=[HBM, VMEM, HBM],
        out_shape=[pltpu.HBM((frames, cols, D), BF), pltpu.VMEM(part, BF), pltpu.HBM(part, BF)],
        scratch_shapes=[pltpu.VMEM((frames, cols, D), BF), pltpu.VMEM(part, BF), pltpu.VMEM((3, D, D), BF), pltpu.VMEM((D, D), BF), pltpu.VMEM((frames, cols, D), BF)]
        + [pltpu.VMEM((tokens, D), BF)] * 6
        + [pltpu.SemaphoreType.DMA((7,))],
        compiler_params=pltpu.CompilerParams(vmem_limit_bytes=40 * 2**20),
        name="temporal_phase",
    )(core, in_vmem(mid), spread.reshape(n, 1), spread.reshape(1, n), gain.reshape(1, D),
      in_hbm(cot), in_hbm(heads), in_hbm(merge))


def own_kernel(keep_ref, got_ref, out_ref):
    out_ref[...] = keep_ref[...].astype(F32) + got_ref[...].astype(F32)


def own_slot(keep, got):
    shape = keep.shape[1:]
    first = pl.BlockSpec((None,) + shape, lambda i: (0, 0, 0, 0))
    return pl.pallas_call(
        own_kernel,
        grid=(1,),
        in_specs=[first, first],
        out_specs=pl.BlockSpec(shape, lambda i: (0, 0, 0)),
        out_shape=jax.ShapeDtypeStruct(shape, F32),
        compiler_params=pltpu.CompilerParams(vmem_limit_bytes=8 * 2**20),
        name="own_slot",
    )(in_hbm(keep), got)


def sum_kernel(own_ref, *refs):
    total = own_ref[...]
    for p in refs[:-1]:
        total = total + p[...].astype(F32)
    refs[-1][...] = total.astype(BF)


def space_sum(own, moved):
    return pl.pallas_call(
        sum_kernel,
        in_specs=[VMEM] * (1 + len(moved)),
        out_specs=VMEM,
        out_shape=pltpu.VMEM(own.shape, BF),
        compiler_params=pltpu.CompilerParams(vmem_limit_bytes=8 * 2**20),
        name="space_sum",
    )(in_vmem(own), *[in_vmem(p) for p in moved])


def per_device(
    clip_tokens,
    frame_order,
    row_reach,
    spatial_gain,
    spatial_heads,
    spatial_merge,
    temporal_gain,
    temporal_heads,
    temporal_merge,
    cotangent,
):
    tm, space = lax.axis_size("tm"), lax.axis_size("space")
    _, frame_count, rows, cols, _ = clip_tokens.shape
    frames = frame_count // tm
    wide = tm * cols
    exchange = lambda v, axis: lax.all_to_all(v, axis, split_axis=0, concat_axis=0, tiled=True)

    here = lax.axis_index("space").astype(jnp.int32)
    half = here >> 1
    parity = (here & 1) ^ (1 - half)
    reach = jnp.where(parity == 0, row_reach[0, 0], row_reach[0, 1])
    info = jnp.stack([reach, half]).astype(jnp.int32)
    halves = [[t * space + s for t in range(tm) for s in pair] for pair in ((1, 0), (2, 3))]
    swap = lambda v: lax.all_to_all(v, ("tm", "space"), split_axis=0, concat_axis=0, axis_index_groups=halves, tiled=True)
    arrived = swap(clip_tokens.reshape(frame_count, rows, cols, D))
    cot = cotangent.reshape(frames, rows, wide, D).swapaxes(0, 1)
    arrived = arrived.reshape(tm, frames, rows, cols, D)
    edge_rows = edge_norm(info, arrived, spatial_gain)
    halo = lax.ppermute(edge_rows, "space", [(i, space - 1 - i) for i in range(space)])
    cot, arrived = lax.optimization_barrier((cot, arrived))
    cot = exchange(cot, "tm")
    qkv, tok = qkv_own(info, arrived, spatial_gain, spatial_heads)
    middle = spatial_phase(info, halo, qkv, tok, spatial_heads, spatial_merge)
    mid = swap(middle.reshape(frame_count, wide, D))
    core = jnp.stack([lax.axis_index("batch") & 1, here]).astype(jnp.int32)
    out, send, keep = temporal_phase(
        core, mid, frame_order.reshape(frame_count), temporal_gain, cot.reshape(frame_count, wide, D),
        temporal_heads, temporal_merge, space, tm,
    )
    batch = lax.axis_size("batch")
    got = lax.ppermute(send, "batch", [(i, i ^ 1) for i in range(batch)])
    output = exchange(out.reshape(tm, frames, wide, D), "tm").swapaxes(0, 1)
    chip = [keep[k].astype(F32) + got[k].astype(F32) for k in range(1, space)]
    moved = [lax.ppermute(chip[k - 1].astype(BF), "space", [(i, (i + k) % space) for i in range(space)])
             for k in range(1, space)]
    own = own_slot(keep, got)
    over_space = space_sum(own, moved)
    pieces = exchange(over_space, "tm")
    mine = pieces.astype(F32).sum(0).astype(BF)
    swapped = [lax.ppermute(mine, "batch", [(i, i ^ m) for i in range(batch)]).astype(F32) for m in (2, 3, 1)]
    own_half = mine.astype(F32) + swapped[0]
    other_half = swapped[1] + swapped[2]
    weight_grad = jnp.where(
        core[0] == 0,
        jnp.concatenate([own_half, other_half], axis=1),
        jnp.concatenate([other_half, own_half], axis=1),
    )
    return (output.reshape(1, frames, rows, wide, D), weight_grad)


def solution(mesh):
    in_specs = (
        P("batch", None, "space", "tm", None),
        P("batch", None),
        P("batch", "tm"),
        P(),
        P(),
        P(),
        P(),
        P(),
        P(),
        P("batch", "tm", "space", None, None),
    )
    out_specs = (P("batch", "tm", "space", None, None), P(("tm", "space"), None))

    return jax.shard_map(per_device, mesh=mesh, in_specs=in_specs, out_specs=out_specs, check_vma=False)
```

```python
import jax
import jax.numpy as jnp
from jax import lax
from jax.experimental import pallas as pl
from jax.experimental.pallas import tpu as pltpu
from jax.sharding import PartitionSpec as P


HALO = 4
D = 1024
HEADS = 16
HEAD_DIM = 64
PAIRS = HEADS // 2
WIDE = 2 * HEAD_DIM
FLOOR = 0.5
SCALE = HEAD_DIM ** (-0.5) * 1.4426950408889634
BF = jnp.bfloat16
F32 = jnp.float32
MASKED = -1e30


def normalized(x, gain):
    return x * lax.rsqrt(jnp.mean(x * x, axis=-1, keepdims=True) + FLOOR) * gain


def in_vmem(x):
    return pltpu.with_memory_space_constraint(x, pltpu.VMEM)


def in_hbm(x):
    return pltpu.with_memory_space_constraint(x, pltpu.HBM)


VMEM = pl.BlockSpec(memory_space=pltpu.VMEM)
SMEM = pl.BlockSpec(memory_space=pltpu.SMEM)
HBM = pl.BlockSpec(memory_space=pltpu.HBM)


def edge_kernel(info_ref, x_ref, gain_ref, edge_ref):
    times, _, rows, cols, _ = x_ref.shape
    start = jnp.where(info_ref[1] == 0, rows - HALO, 0)
    gain = gain_ref[...]
    for r in range(HALO):
        for t in range(times):
            y = normalized(x_ref[t, 0, start + r].astype(F32), gain)
            edge_ref[r, t * cols:(t + 1) * cols, :] = y.astype(BF)


def edge_norm(info, arrived, gain):
    times, _, _, cols, _ = arrived.shape
    return pl.pallas_call(
        edge_kernel,
        in_specs=[SMEM, VMEM, VMEM],
        out_specs=VMEM,
        out_shape=pltpu.VMEM((HALO, times * cols, D), BF),
        compiler_params=pltpu.CompilerParams(vmem_limit_bytes=4 * 2**20),
        name="edge_norm",
    )(info, in_vmem(arrived), gain.reshape(1, D))


def column_copies(w_ref, buf, sems, columns):
    return [pltpu.make_async_copy(w_ref.at[:, c * D:(c + 1) * D], buf.at[i], sems.at[i]) for i, c in enumerate(columns)]


QKV_PIECE = 1024


def qkv_kernel(info_ref, arrived_ref, gain_ref, w_ref, out_ref, tok_out, x_ref, tok_ref, buf, y_ref, sems, out_sems, tok_sems):
    pieces = buf.shape[0]
    copies = [pltpu.make_async_copy(w_ref.at[:, i * QKV_PIECE:(i + 1) * QKV_PIECE], buf.at[i], sems.at[i])
              for i in range(pieces)]
    for c in copies:
        c.start()
    times, parities, rows, cols, _ = arrived_ref.shape
    wide = times * cols
    half = info_ref[1]
    gain = gain_ref[...]
    kept = []
    for o in range(parities):
        first = jnp.where(half == 0, 1 - o, o) * rows

        def one_row(r, carry):
            for t in range(times):
                x = arrived_ref[t, o, r]
                y = normalized(x.astype(F32), gain).astype(BF)
                tok_ref[first + r, t * cols:(t + 1) * cols, :] = x
                x_ref[first + r, t * cols:(t + 1) * cols, :] = y
            return carry

        lax.fori_loop(0, rows, one_row, 0)
        done = pl.ds(first, rows)
        kept.append(pltpu.make_async_copy(tok_ref.at[done], tok_out.at[done], tok_sems.at[o]))
        kept[o].start()
    sent = []
    x = x_ref[...].reshape(parities * rows * wide, D)
    for i, c in enumerate(copies):
        c.wait()
        y_ref[i] = jnp.dot(x, buf[i], preferred_element_type=F32).astype(BF)
        third, at = divmod(i * QKV_PIECE, D)
        sent.append(pltpu.make_async_copy(y_ref.at[i], out_ref.at[third, :, at:at + QKV_PIECE], out_sems.at[i]))
        sent[i].start()
    for c in sent + kept:
        c.wait()


def qkv_own(info, arrived, gain, heads):
    times, parities, rows, cols, _ = arrived.shape
    shape = (parities * rows, times * cols, D)
    tokens = shape[0] * shape[1]
    pieces = 3 * D // QKV_PIECE
    return pl.pallas_call(
        qkv_kernel,
        in_specs=[SMEM, VMEM, VMEM, HBM],
        out_specs=[HBM, HBM],
        out_shape=[pltpu.HBM((3, tokens, D), BF), pltpu.HBM(shape, BF)],
        scratch_shapes=[pltpu.VMEM(shape, BF), pltpu.VMEM(shape, BF),
                        pltpu.VMEM((pieces, D, QKV_PIECE), BF), pltpu.VMEM((pieces, tokens, QKV_PIECE), BF),
                        pltpu.SemaphoreType.DMA((pieces,)), pltpu.SemaphoreType.DMA((pieces,)),
                        pltpu.SemaphoreType.DMA((2,))],
        compiler_params=pltpu.CompilerParams(vmem_limit_bytes=28 * 2**20),
        name="qkv_own",
    )(info, in_vmem(arrived), gain.reshape(1, D), in_hbm(heads))


def staged_attention(items):
    n = items[0][0]().shape[0]
    low = lax.broadcasted_iota(jnp.int32, (n, WIDE), 1) < HEAD_DIM
    scores, weights = [], []
    for q, k, v, bias, ref, at in items:
        q = q()
        zero = jnp.zeros_like(q)
        both = jnp.concatenate([jnp.where(low, q, zero), jnp.where(low, zero, q)], axis=0)
        scores.append(lax.dot_general(both, k(), (((1,), (1,)), ((), ())), preferred_element_type=F32))
    for s, (q, k, v, bias, ref, at) in zip(scores, items):
        b = bias()
        s = s * SCALE + jnp.concatenate([b, b], axis=0)
        weights.append(jnp.exp2(s - jnp.max(s, axis=-1, keepdims=True)).astype(BF))
    for p, (q, k, v, bias, ref, at) in zip(weights, items):
        v = v()
        o = jnp.dot(p, jnp.concatenate([v, jnp.ones_like(v)], axis=1), preferred_element_type=F32)
        o = o[:, :WIDE] / o[:, WIDE:]
        ref[at] = jnp.where(low, o[:n], o[n:]).astype(BF)


def reader(ref, *at):
    return lambda: ref[at]


SPATIAL_STAGE = 4
TEMPORAL_STAGE = 16


def spatial_kernel(info_ref, halo_ref, qkv_ref, tok_ref, w_ref, wm_ref, mid_out,
                   q_ref, tok_buf, mid_buf, wkv_buf, wm_buf, k_ref, v_ref, ctx_ref, bias_ref, sems):
    rows, cols, _ = tok_buf.shape
    tokens = rows * cols
    edge = HALO * cols
    reach, half = info_ref[0], info_ref[1]
    weights = column_copies(w_ref, wkv_buf, sems, (1, 2))
    own = [pltpu.make_async_copy(qkv_ref.at[0], q_ref, sems.at[2])]
    for i, buf in ((1, k_ref), (2, v_ref)):
        own.append(pltpu.make_async_copy(qkv_ref.at[i], buf.at[edge:edge + tokens], sems.at[2 + i]))
    last = [pltpu.make_async_copy(wm_ref, wm_buf, sems.at[5]), pltpu.make_async_copy(tok_ref, tok_buf, sems.at[6])]
    for c in own + weights + last:
        c.start()
    blocks, n, extent = bias_ref.shape
    qrow = lax.broadcasted_iota(jnp.int32, (n, extent), 0) // cols
    krow = lax.broadcasted_iota(jnp.int32, (n, extent), 1) // cols - HALO
    near = jnp.abs(krow - qrow) <= reach
    for j in range(blocks):
        at = krow + (j * HALO + half * rows)
        bias_ref[j] = jnp.where(near & (at >= 0) & (at < 2 * rows), 0.0, MASKED)
    for c in own:
        c.wait()

    def attend(chosen):
        items = []
        for pair in range(PAIRS):
            at = slice(pair * WIDE, (pair + 1) * WIDE)
            for j in chosen:
                keys = slice(j * edge, j * edge + extent)
                mine = slice(j * n, (j + 1) * n)
                items.append((reader(q_ref, mine, at), reader(k_ref, keys, at), reader(v_ref, keys, at),
                              reader(bias_ref, j), ctx_ref, (mine, at)))
        for i in range(0, len(items), SPATIAL_STAGE):
            staged_attention(items[i:i + SPATIAL_STAGE])

    inner = [j for j in range(blocks) if j * edge >= edge and j * edge + extent <= edge + tokens]
    attend(inner)
    there = jnp.where(half == 0, edge + tokens, 0)
    empty = jnp.where(half == 0, 0, edge + tokens)
    halo = halo_ref[...].reshape(edge, D)
    for c, w, buf in zip(weights, range(2), (k_ref, v_ref)):
        c.wait()
        side = jnp.dot(halo, wkv_buf[w], preferred_element_type=F32).astype(BF)
        buf[pl.ds(pl.multiple_of(there, edge), edge)] = side
        buf[pl.ds(pl.multiple_of(empty, edge), edge)] = jnp.zeros_like(side)
    attend([j for j in range(blocks) if j not in inner])
    for c in last:
        c.wait()
    sent = []
    part, strip = rows // 2, tokens // 2
    for i in range(2):
        mid = jnp.dot(ctx_ref[i * strip:(i + 1) * strip], wm_buf[...], preferred_element_type=F32)
        mid = mid + tok_buf[i * part:(i + 1) * part].reshape(strip, D).astype(F32)
        mid_buf[i] = mid.astype(BF).reshape(part, cols, D)
        parity = jnp.where(half == 0, 1 - i, i)
        sent.append(pltpu.make_async_copy(mid_buf.at[i], mid_out.at[:, parity], sems.at[7 + i]))
        sent[i].start()
    for c in sent:
        c.wait()


def spatial_phase(info, halo, qkv, tok, heads, merge):
    rows, cols, _ = tok.shape
    tokens = rows * cols
    edge = HALO * cols
    extent = tokens + 2 * edge
    return pl.pallas_call(
        spatial_kernel,
        in_specs=[SMEM, VMEM, HBM, HBM, HBM, HBM],
        out_specs=HBM,
        out_shape=pltpu.HBM((rows // 2, 2, cols, D), BF),
        scratch_shapes=[pltpu.VMEM((tokens, D), BF), pltpu.VMEM((rows, cols, D), BF),
                        pltpu.VMEM((2, rows // 2, cols, D), BF),
                        pltpu.VMEM((2, D, D), BF), pltpu.VMEM((D, D), BF),
                        pltpu.VMEM((extent, D), BF), pltpu.VMEM((extent, D), BF),
                        pltpu.VMEM((tokens, D), BF), pltpu.VMEM((tokens // edge, edge, 3 * edge), F32),
                        pltpu.SemaphoreType.DMA((9,))],
        compiler_params=pltpu.CompilerParams(vmem_limit_bytes=40 * 2**20),
        name="spatial_phase",
    )(info, in_vmem(halo), *[in_hbm(v) for v in (qkv, tok, heads, merge)])


GROUP = 8


def temporal_kernel(core_ref, mid_ref, order_q_ref, order_k_ref, gain_ref, cot_ref, w_ref, wm_ref,
                    out_hbm, send_ref, keep_hbm,
                    out_ref, keep_ref, wqkv_buf, wm_buf, cot_buf, normed_ref, q_ref, k_ref, v_ref, ctx_ref, cotb_ref, sems):
    frames, cols, _ = mid_ref.shape
    groups = cols // GROUP
    n = frames * GROUP
    copies = column_copies(w_ref, wqkv_buf, sems, range(3))
    copies.append(pltpu.make_async_copy(cot_ref, cot_buf, sems.at[3]))
    copies.append(pltpu.make_async_copy(wm_ref, wm_buf, sems.at[4]))
    for c in copies:
        c.start()
    gain = gain_ref[...]
    for g in range(groups):
        x = mid_ref[:, g * GROUP:(g + 1) * GROUP, :].astype(F32).reshape(n, D)
        normed_ref[g * n:(g + 1) * n] = normalized(x, gain).astype(BF)
    for i, buf in enumerate((q_ref, k_ref, v_ref)):
        copies[i].wait()
        buf[...] = jnp.dot(normed_ref[...], wqkv_buf[i], preferred_element_type=F32).astype(BF)
    copies[3].wait()
    for g in range(groups):
        cotb_ref[g * n:(g + 1) * n] = cot_buf[:, g * GROUP:(g + 1) * GROUP, :].astype(F32).reshape(n, D).astype(BF)
    place_q = lax.broadcasted_iota(jnp.int32, (n, n), 0) % GROUP
    place_k = lax.broadcasted_iota(jnp.int32, (n, n), 1) % GROUP
    allowed = (place_q == place_k) & (order_k_ref[...] <= order_q_ref[...])
    bias = jnp.where(allowed, 0.0, MASKED)
    items = []
    for g in range(groups):
        own = slice(g * n, (g + 1) * n)
        for pair in range(PAIRS):
            at = slice(pair * WIDE, (pair + 1) * WIDE)
            items.append((reader(q_ref, own, at), reader(k_ref, own, at), reader(v_ref, own, at), lambda: bias,
                          ctx_ref, (own, at)))
    for i in range(0, len(items), TEMPORAL_STAGE):
        staged_attention(items[i:i + TEMPORAL_STAGE])
    core = core_ref[0]
    here = core_ref[1]
    half = D // 2
    for ref, which in ((send_ref, 1 - core), (keep_ref, core)):
        cot = cotb_ref[:, pl.ds(pl.multiple_of(which * half, half), half)]
        grad = lax.dot_general(ctx_ref[...], cot, (((0,), (0,)), ((), ())), preferred_element_type=F32).astype(BF)
        spaces, times, block, _ = ref.shape
        for s in range(spaces):
            slot = lax.rem(s + spaces - here, spaces)
            for t in range(times):
                row = (t * spaces + s) * block
                ref[slot, t] = grad[row:row + block]
    kept = pltpu.make_async_copy(keep_ref, keep_hbm, sems.at[5])
    kept.start()
    copies[4].wait()
    y = jnp.dot(ctx_ref[...], wm_buf[...], preferred_element_type=F32)
    for g in range(groups):
        x = mid_ref[:, g * GROUP:(g + 1) * GROUP, :].astype(F32) + y[g * n:(g + 1) * n].reshape(frames, GROUP, D)
        out_ref[:, g * GROUP:(g + 1) * GROUP, :] = x.astype(BF)
    done = pltpu.make_async_copy(out_ref, out_hbm, sems.at[6])
    done.start()
    done.wait()
    kept.wait()


def temporal_phase(core, mid, order, gain, cot, heads, merge, spaces, times):
    frames, cols, _ = mid.shape
    n = frames * GROUP
    tokens = frames * cols
    spread = jnp.repeat(order, GROUP)
    block = D // (spaces * times)
    part = (spaces, times, block, D // 2)
    return pl.pallas_call(
        temporal_kernel,
        in_specs=[SMEM] + [VMEM] * 4 + [HBM] * 3,
        out_specs=[HBM, VMEM, HBM],
        out_shape=[pltpu.HBM((frames, cols, D), BF), pltpu.VMEM(part, BF), pltpu.HBM(part, BF)],
        scratch_shapes=[pltpu.VMEM((frames, cols, D), BF), pltpu.VMEM(part, BF), pltpu.VMEM((3, D, D), BF), pltpu.VMEM((D, D), BF), pltpu.VMEM((frames, cols, D), BF)]
        + [pltpu.VMEM((tokens, D), BF)] * 6
        + [pltpu.SemaphoreType.DMA((7,))],
        compiler_params=pltpu.CompilerParams(vmem_limit_bytes=40 * 2**20),
        name="temporal_phase",
    )(core, in_vmem(mid), spread.reshape(n, 1), spread.reshape(1, n), gain.reshape(1, D),
      in_hbm(cot), in_hbm(heads), in_hbm(merge))


def own_kernel(keep_ref, got_ref, out_ref):
    out_ref[...] = keep_ref[...].astype(F32) + got_ref[...].astype(F32)


def own_slot(keep, got):
    shape = keep.shape[1:]
    first = pl.BlockSpec((None,) + shape, lambda i: (0, 0, 0, 0))
    return pl.pallas_call(
        own_kernel,
        grid=(1,),
        in_specs=[first, first],
        out_specs=pl.BlockSpec(shape, lambda i: (0, 0, 0)),
        out_shape=jax.ShapeDtypeStruct(shape, F32),
        compiler_params=pltpu.CompilerParams(vmem_limit_bytes=8 * 2**20),
        name="own_slot",
    )(in_hbm(keep), got)


def sum_kernel(own_ref, *refs):
    total = own_ref[...]
    for p in refs[:-1]:
        total = total + p[...].astype(F32)
    refs[-1][0] = total.astype(BF)
    refs[-1][1] = refs[-1][0]


def space_sum(own, moved):
    return pl.pallas_call(
        sum_kernel,
        in_specs=[VMEM] * (1 + len(moved)),
        out_specs=VMEM,
        out_shape=pltpu.VMEM((2,) + own.shape, BF),
        compiler_params=pltpu.CompilerParams(vmem_limit_bytes=8 * 2**20),
        name="space_sum",
    )(in_vmem(own), *[in_vmem(p) for p in moved])


def per_device(
    clip_tokens,
    frame_order,
    row_reach,
    spatial_gain,
    spatial_heads,
    spatial_merge,
    temporal_gain,
    temporal_heads,
    temporal_merge,
    cotangent,
):
    tm, space = lax.axis_size("tm"), lax.axis_size("space")
    _, frame_count, rows, cols, _ = clip_tokens.shape
    frames = frame_count // tm
    wide = tm * cols
    exchange = lambda v, axis: lax.all_to_all(v, axis, split_axis=0, concat_axis=0, tiled=True)

    here = lax.axis_index("space").astype(jnp.int32)
    half = here >> 1
    parity = (here & 1) ^ (1 - half)
    reach = jnp.where(parity == 0, row_reach[0, 0], row_reach[0, 1])
    info = jnp.stack([reach, half]).astype(jnp.int32)
    halves = [[t * space + s for t in range(tm) for s in pair] for pair in ((1, 0), (2, 3))]
    swap = lambda v: lax.all_to_all(v, ("tm", "space"), split_axis=0, concat_axis=0, axis_index_groups=halves, tiled=True)
    arrived = swap(clip_tokens.reshape(frame_count, rows, cols, D))
    cot = cotangent.reshape(frames, rows, wide, D).swapaxes(0, 1)
    arrived = arrived.reshape(tm, frames, rows, cols, D)
    edge_rows = edge_norm(info, arrived, spatial_gain)
    halo = lax.ppermute(edge_rows, "space", [(i, space - 1 - i) for i in range(space)])
    cot, arrived = lax.optimization_barrier((cot, arrived))
    cot = exchange(cot, "tm")
    qkv, tok = qkv_own(info, arrived, spatial_gain, spatial_heads)
    middle = spatial_phase(info, halo, qkv, tok, spatial_heads, spatial_merge)
    mid = swap(middle.reshape(frame_count, wide, D))
    core = jnp.stack([lax.axis_index("batch") & 1, here]).astype(jnp.int32)
    out, send, keep = temporal_phase(
        core, mid, frame_order.reshape(frame_count), temporal_gain, cot.reshape(frame_count, wide, D),
        temporal_heads, temporal_merge, space, tm,
    )
    batch = lax.axis_size("batch")
    got = lax.ppermute(send, "batch", [(i, i ^ 1) for i in range(batch)])
    output = exchange(out.reshape(tm, frames, wide, D), "tm").swapaxes(0, 1)
    chip = [keep[k].astype(F32) + got[k].astype(F32) for k in range(1, space)]
    moved = [lax.ppermute(chip[k - 1].astype(BF), "space", [(i, (i + k) % space) for i in range(space)])
             for k in sorted(range(1, space), key=lambda k: -min(k, space - k))]
    own = own_slot(keep, got)
    over_space = space_sum(own, moved)
    planes = [[(2 * y + c) * tm + t for y in range(batch // 2) for t in range(tm)] for c in range(2)]
    pieces = lax.all_to_all(
        over_space.reshape(2 * tm, *over_space.shape[2:]), ("batch", "tm"), split_axis=0, concat_axis=0,
        axis_index_groups=planes, tiled=True,
    )
    mine = pieces.astype(F32).sum(0).astype(BF)
    other = lax.ppermute(mine, "batch", [(i, i ^ 1) for i in range(batch)])
    weight_grad = jnp.where(
        core[0] == 0, jnp.concatenate([mine, other], axis=1), jnp.concatenate([other, mine], axis=1)
    ).astype(F32)
    return (output.reshape(1, frames, rows, wide, D), weight_grad)


def solution(mesh):
    in_specs = (
        P("batch", None, "space", "tm", None),
        P("batch", None),
        P("batch", "tm"),
        P(),
        P(),
        P(),
        P(),
        P(),
        P(),
        P("batch", "tm", "space", None, None),
    )
    out_specs = (P("batch", "tm", "space", None, None), P(("tm", "space"), None))

    return jax.shard_map(per_device, mesh=mesh, in_specs=in_specs, out_specs=out_specs, check_vma=False)
```

```python
import jax
import jax.numpy as jnp
from jax import lax
from jax.experimental import pallas as pl
from jax.experimental.pallas import tpu as pltpu
from jax.sharding import PartitionSpec as P


HALO = 4
D = 1024
HEADS = 16
HEAD_DIM = 64
PAIRS = HEADS // 2
WIDE = 2 * HEAD_DIM
FLOOR = 0.5
SCALE = HEAD_DIM ** (-0.5) * 1.4426950408889634
BF = jnp.bfloat16
F32 = jnp.float32
MASKED = -1e30


def normalized(x, gain):
    return x * lax.rsqrt(jnp.mean(x * x, axis=-1, keepdims=True) + FLOOR) * gain


def in_vmem(x):
    return pltpu.with_memory_space_constraint(x, pltpu.VMEM)


def in_hbm(x):
    return pltpu.with_memory_space_constraint(x, pltpu.HBM)


VMEM = pl.BlockSpec(memory_space=pltpu.VMEM)
SMEM = pl.BlockSpec(memory_space=pltpu.SMEM)
HBM = pl.BlockSpec(memory_space=pltpu.HBM)


def edge_kernel(info_ref, x_ref, gain_ref, edge_ref):
    times, _, rows, cols, _ = x_ref.shape
    start = jnp.where(info_ref[1] == 0, rows - HALO, 0)
    gain = gain_ref[...]
    for r in range(HALO):
        for t in range(times):
            y = normalized(x_ref[t, 0, start + r].astype(F32), gain)
            edge_ref[r, t * cols:(t + 1) * cols, :] = y.astype(BF)


def edge_norm(info, arrived, gain):
    times, _, _, cols, _ = arrived.shape
    return pl.pallas_call(
        edge_kernel,
        in_specs=[SMEM, VMEM, VMEM],
        out_specs=VMEM,
        out_shape=pltpu.VMEM((HALO, times * cols, D), BF),
        compiler_params=pltpu.CompilerParams(vmem_limit_bytes=4 * 2**20),
        name="edge_norm",
    )(info, in_vmem(arrived), gain.reshape(1, D))


def column_copies(w_ref, buf, sems, columns):
    return [pltpu.make_async_copy(w_ref.at[:, c * D:(c + 1) * D], buf.at[i], sems.at[i]) for i, c in enumerate(columns)]


QKV_PIECE = 1024


def qkv_kernel(info_ref, arrived_ref, gain_ref, w_ref, out_ref, tok_out, x_ref, tok_ref, buf, y_ref, sems, out_sems, tok_sems):
    pieces = buf.shape[0]
    copies = [pltpu.make_async_copy(w_ref.at[:, i * QKV_PIECE:(i + 1) * QKV_PIECE], buf.at[i], sems.at[i])
              for i in range(pieces)]
    for c in copies:
        c.start()
    times, parities, rows, cols, _ = arrived_ref.shape
    wide = times * cols
    half = info_ref[1]
    gain = gain_ref[...]
    kept = []
    for o in range(parities):
        first = jnp.where(half == 0, 1 - o, o) * rows

        def one_row(r, carry):
            for t in range(0, times, 2):
                at = slice(t * cols, (t + 2) * cols)
                x = jnp.concatenate([arrived_ref[t + i, o, r].astype(F32) for i in range(2)], axis=0)
                tok_ref[first + r, at, :] = x.astype(BF)
                x_ref[first + r, at, :] = normalized(x, gain).astype(BF)
            return carry

        lax.fori_loop(0, rows, one_row, 0)
        done = pl.ds(first, rows)
        kept.append(pltpu.make_async_copy(tok_ref.at[done], tok_out.at[done], tok_sems.at[o]))
        kept[o].start()
    sent = []
    x = x_ref[...].reshape(parities * rows * wide, D)
    for i, c in enumerate(copies):
        c.wait()
        y_ref[i] = jnp.dot(x, buf[i], preferred_element_type=F32).astype(BF)
        third, at = divmod(i * QKV_PIECE, D)
        sent.append(pltpu.make_async_copy(y_ref.at[i], out_ref.at[third, :, at:at + QKV_PIECE], out_sems.at[i]))
        sent[i].start()
    for c in sent + kept:
        c.wait()


def qkv_own(info, arrived, gain, heads):
    times, parities, rows, cols, _ = arrived.shape
    shape = (parities * rows, times * cols, D)
    tokens = shape[0] * shape[1]
    pieces = 3 * D // QKV_PIECE
    return pl.pallas_call(
        qkv_kernel,
        in_specs=[SMEM, VMEM, VMEM, HBM],
        out_specs=[HBM, HBM],
        out_shape=[pltpu.HBM((3, tokens, D), BF), pltpu.HBM(shape, BF)],
        scratch_shapes=[pltpu.VMEM(shape, BF), pltpu.VMEM(shape, BF),
                        pltpu.VMEM((pieces, D, QKV_PIECE), BF), pltpu.VMEM((pieces, tokens, QKV_PIECE), BF),
                        pltpu.SemaphoreType.DMA((pieces,)), pltpu.SemaphoreType.DMA((pieces,)),
                        pltpu.SemaphoreType.DMA((2,))],
        compiler_params=pltpu.CompilerParams(vmem_limit_bytes=28 * 2**20),
        name="qkv_own",
    )(info, in_vmem(arrived), gain.reshape(1, D), in_hbm(heads))


def staged_attention(items):
    n = items[0][0]().shape[0]
    low = lax.broadcasted_iota(jnp.int32, (n, WIDE), 1) < HEAD_DIM
    scores, weights = [], []
    for q, k, v, bias, ref, at in items:
        q = q()
        zero = jnp.zeros_like(q)
        both = jnp.concatenate([jnp.where(low, q, zero), jnp.where(low, zero, q)], axis=0)
        scores.append(lax.dot_general(both, k(), (((1,), (1,)), ((), ())), preferred_element_type=F32))
    for s, (q, k, v, bias, ref, at) in zip(scores, items):
        b = bias()
        s = s * SCALE + jnp.concatenate([b, b], axis=0)
        weights.append(jnp.exp2(s - jnp.max(s, axis=-1, keepdims=True)).astype(BF))
    for p, (q, k, v, bias, ref, at) in zip(weights, items):
        v = v()
        o = jnp.dot(p, jnp.concatenate([v, jnp.ones_like(v)], axis=1), preferred_element_type=F32)
        o = o[:, :WIDE] / o[:, WIDE:]
        ref[at] = jnp.where(low, o[:n], o[n:]).astype(BF)


def reader(ref, *at):
    return lambda: ref[at]


SPATIAL_STAGE = 4
TEMPORAL_STAGE = 16


def spatial_kernel(info_ref, halo_ref, qkv_ref, tok_ref, w_ref, wm_ref, mid_out,
                   q_ref, tok_buf, mid_buf, wkv_buf, wm_buf, k_ref, v_ref, ctx_ref, bias_ref, sems):
    rows, cols, _ = tok_buf.shape
    tokens = rows * cols
    edge = HALO * cols
    reach, half = info_ref[0], info_ref[1]
    weights = column_copies(w_ref, wkv_buf, sems, (1, 2))
    own = [pltpu.make_async_copy(qkv_ref.at[0], q_ref, sems.at[2])]
    for i, buf in ((1, k_ref), (2, v_ref)):
        own.append(pltpu.make_async_copy(qkv_ref.at[i], buf.at[edge:edge + tokens], sems.at[2 + i]))
    last = [pltpu.make_async_copy(wm_ref, wm_buf, sems.at[5]), pltpu.make_async_copy(tok_ref, tok_buf, sems.at[6])]
    for c in own + weights + last:
        c.start()
    blocks, n, extent = bias_ref.shape
    qrow = lax.broadcasted_iota(jnp.int32, (n, extent), 0) // cols
    krow = lax.broadcasted_iota(jnp.int32, (n, extent), 1) // cols - HALO
    near = jnp.abs(krow - qrow) <= reach
    for j in range(blocks):
        at = krow + (j * HALO + half * rows)
        bias_ref[j] = jnp.where(near & (at >= 0) & (at < 2 * rows), 0.0, MASKED)
    for c in own:
        c.wait()

    def attend(chosen):
        items = []
        for pair in range(PAIRS):
            at = slice(pair * WIDE, (pair + 1) * WIDE)
            for j in chosen:
                keys = slice(j * edge, j * edge + extent)
                mine = slice(j * n, (j + 1) * n)
                items.append((reader(q_ref, mine, at), reader(k_ref, keys, at), reader(v_ref, keys, at),
                              reader(bias_ref, j), ctx_ref, (mine, at)))
        for i in range(0, len(items), SPATIAL_STAGE):
            staged_attention(items[i:i + SPATIAL_STAGE])

    inner = [j for j in range(blocks) if j * edge >= edge and j * edge + extent <= edge + tokens]
    attend(inner)
    there = jnp.where(half == 0, edge + tokens, 0)
    empty = jnp.where(half == 0, 0, edge + tokens)
    halo = halo_ref[...].reshape(edge, D)
    for c, w, buf in zip(weights, range(2), (k_ref, v_ref)):
        c.wait()
        side = jnp.dot(halo, wkv_buf[w], preferred_element_type=F32).astype(BF)
        buf[pl.ds(pl.multiple_of(there, edge), edge)] = side
        buf[pl.ds(pl.multiple_of(empty, edge), edge)] = jnp.zeros_like(side)
    attend([j for j in range(blocks) if j not in inner])
    for c in last:
        c.wait()
    sent = []
    part, strip = rows // 2, tokens // 2
    for i in range(2):
        mid = jnp.dot(ctx_ref[i * strip:(i + 1) * strip], wm_buf[...], preferred_element_type=F32)
        mid = mid + tok_buf[i * part:(i + 1) * part].reshape(strip, D).astype(F32)
        mid_buf[i] = mid.astype(BF).reshape(part, cols, D)
        parity = jnp.where(half == 0, 1 - i, i)
        sent.append(pltpu.make_async_copy(mid_buf.at[i], mid_out.at[:, parity], sems.at[7 + i]))
        sent[i].start()
    for c in sent:
        c.wait()


def spatial_phase(info, halo, qkv, tok, heads, merge):
    rows, cols, _ = tok.shape
    tokens = rows * cols
    edge = HALO * cols
    extent = tokens + 2 * edge
    return pl.pallas_call(
        spatial_kernel,
        in_specs=[SMEM, VMEM, HBM, HBM, HBM, HBM],
        out_specs=HBM,
        out_shape=pltpu.HBM((rows // 2, 2, cols, D), BF),
        scratch_shapes=[pltpu.VMEM((tokens, D), BF), pltpu.VMEM((rows, cols, D), BF),
                        pltpu.VMEM((2, rows // 2, cols, D), BF),
                        pltpu.VMEM((2, D, D), BF), pltpu.VMEM((D, D), BF),
                        pltpu.VMEM((extent, D), BF), pltpu.VMEM((extent, D), BF),
                        pltpu.VMEM((tokens, D), BF), pltpu.VMEM((tokens // edge, edge, 3 * edge), F32),
                        pltpu.SemaphoreType.DMA((9,))],
        compiler_params=pltpu.CompilerParams(vmem_limit_bytes=40 * 2**20),
        name="spatial_phase",
    )(info, in_vmem(halo), *[in_hbm(v) for v in (qkv, tok, heads, merge)])


GROUP = 8


def temporal_kernel(core_ref, mid_ref, order_q_ref, order_k_ref, gain_ref, cot_ref, w_ref, wm_ref,
                    out_hbm, send_ref, keep_hbm,
                    out_ref, keep_ref, wqkv_buf, wm_buf, cot_buf, normed_ref, q_ref, k_ref, v_ref, ctx_ref, cotb_ref, sems):
    frames, cols, _ = mid_ref.shape
    groups = cols // GROUP
    n = frames * GROUP
    copies = column_copies(w_ref, wqkv_buf, sems, range(3))
    copies.append(pltpu.make_async_copy(cot_ref, cot_buf, sems.at[3]))
    copies.append(pltpu.make_async_copy(wm_ref, wm_buf, sems.at[4]))
    for c in copies:
        c.start()
    gain = gain_ref[...]
    for g in range(groups):
        x = mid_ref[:, g * GROUP:(g + 1) * GROUP, :].astype(F32).reshape(n, D)
        normed_ref[g * n:(g + 1) * n] = normalized(x, gain).astype(BF)
    for i, buf in enumerate((q_ref, k_ref, v_ref)):
        copies[i].wait()
        buf[...] = jnp.dot(normed_ref[...], wqkv_buf[i], preferred_element_type=F32).astype(BF)
    copies[3].wait()
    for g in range(groups):
        cotb_ref[g * n:(g + 1) * n] = cot_buf[:, g * GROUP:(g + 1) * GROUP, :].astype(F32).reshape(n, D).astype(BF)
    place_q = lax.broadcasted_iota(jnp.int32, (n, n), 0) % GROUP
    place_k = lax.broadcasted_iota(jnp.int32, (n, n), 1) % GROUP
    allowed = (place_q == place_k) & (order_k_ref[...] <= order_q_ref[...])
    bias = jnp.where(allowed, 0.0, MASKED)
    items = []
    for g in range(groups):
        own = slice(g * n, (g + 1) * n)
        for pair in range(PAIRS):
            at = slice(pair * WIDE, (pair + 1) * WIDE)
            items.append((reader(q_ref, own, at), reader(k_ref, own, at), reader(v_ref, own, at), lambda: bias,
                          ctx_ref, (own, at)))
    for i in range(0, len(items), TEMPORAL_STAGE):
        staged_attention(items[i:i + TEMPORAL_STAGE])
    core = core_ref[0]
    here = core_ref[1]
    half = D // 2
    for ref, which in ((send_ref, 1 - core), (keep_ref, core)):
        cot = cotb_ref[:, pl.ds(pl.multiple_of(which * half, half), half)]
        grad = lax.dot_general(ctx_ref[...], cot, (((0,), (0,)), ((), ())), preferred_element_type=F32).astype(BF)
        spaces, times, block, _ = ref.shape
        for s in range(spaces):
            slot = lax.rem(s + spaces - here, spaces)
            for t in range(times):
                row = (t * spaces + s) * block
                ref[slot, t] = grad[row:row + block]
    kept = pltpu.make_async_copy(keep_ref, keep_hbm, sems.at[5])
    kept.start()
    copies[4].wait()
    y = jnp.dot(ctx_ref[...], wm_buf[...], preferred_element_type=F32)
    for g in range(groups):
        x = mid_ref[:, g * GROUP:(g + 1) * GROUP, :].astype(F32) + y[g * n:(g + 1) * n].reshape(frames, GROUP, D)
        out_ref[:, g * GROUP:(g + 1) * GROUP, :] = x.astype(BF)
    done = pltpu.make_async_copy(out_ref, out_hbm, sems.at[6])
    done.start()
    done.wait()
    kept.wait()


def temporal_phase(core, mid, order, gain, cot, heads, merge, spaces, times):
    frames, cols, _ = mid.shape
    n = frames * GROUP
    tokens = frames * cols
    spread = jnp.repeat(order, GROUP)
    block = D // (spaces * times)
    part = (spaces, times, block, D // 2)
    return pl.pallas_call(
        temporal_kernel,
        in_specs=[SMEM] + [VMEM] * 4 + [HBM] * 3,
        out_specs=[HBM, VMEM, HBM],
        out_shape=[pltpu.HBM((frames, cols, D), BF), pltpu.VMEM(part, BF), pltpu.HBM(part, BF)],
        scratch_shapes=[pltpu.VMEM((frames, cols, D), BF), pltpu.VMEM(part, BF), pltpu.VMEM((3, D, D), BF), pltpu.VMEM((D, D), BF), pltpu.VMEM((frames, cols, D), BF)]
        + [pltpu.VMEM((tokens, D), BF)] * 6
        + [pltpu.SemaphoreType.DMA((7,))],
        compiler_params=pltpu.CompilerParams(vmem_limit_bytes=40 * 2**20),
        name="temporal_phase",
    )(core, in_vmem(mid), spread.reshape(n, 1), spread.reshape(1, n), gain.reshape(1, D),
      in_hbm(cot), in_hbm(heads), in_hbm(merge))


def own_kernel(keep_ref, got_ref, out_ref):
    out_ref[...] = keep_ref[...].astype(F32) + got_ref[...].astype(F32)


def own_slot(keep, got):
    shape = keep.shape[1:]
    first = pl.BlockSpec((None,) + shape, lambda i: (0, 0, 0, 0))
    return pl.pallas_call(
        own_kernel,
        grid=(1,),
        in_specs=[first, first],
        out_specs=pl.BlockSpec(shape, lambda i: (0, 0, 0)),
        out_shape=jax.ShapeDtypeStruct(shape, F32),
        compiler_params=pltpu.CompilerParams(vmem_limit_bytes=8 * 2**20),
        name="own_slot",
    )(in_hbm(keep), got)


def sum_kernel(own_ref, *refs):
    total = own_ref[...]
    for p in refs[:-1]:
        total = total + p[...].astype(F32)
    refs[-1][0] = total.astype(BF)
    refs[-1][1] = refs[-1][0]


def space_sum(own, moved):
    return pl.pallas_call(
        sum_kernel,
        in_specs=[VMEM] * (1 + len(moved)),
        out_specs=VMEM,
        out_shape=pltpu.VMEM((2,) + own.shape, BF),
        compiler_params=pltpu.CompilerParams(vmem_limit_bytes=8 * 2**20),
        name="space_sum",
    )(in_vmem(own), *[in_vmem(p) for p in moved])


def per_device(
    clip_tokens,
    frame_order,
    row_reach,
    spatial_gain,
    spatial_heads,
    spatial_merge,
    temporal_gain,
    temporal_heads,
    temporal_merge,
    cotangent,
):
    tm, space = lax.axis_size("tm"), lax.axis_size("space")
    _, frame_count, rows, cols, _ = clip_tokens.shape
    frames = frame_count // tm
    wide = tm * cols
    exchange = lambda v, axis: lax.all_to_all(v, axis, split_axis=0, concat_axis=0, tiled=True)

    here = lax.axis_index("space").astype(jnp.int32)
    half = here >> 1
    parity = (here & 1) ^ (1 - half)
    reach = jnp.where(parity == 0, row_reach[0, 0], row_reach[0, 1])
    info = jnp.stack([reach, half]).astype(jnp.int32)
    halves = [[t * space + s for t in range(tm) for s in pair] for pair in ((1, 0), (2, 3))]
    swap = lambda v: lax.all_to_all(v, ("tm", "space"), split_axis=0, concat_axis=0, axis_index_groups=halves, tiled=True)
    arrived = swap(clip_tokens.reshape(frame_count, rows, cols, D))
    cot = cotangent.reshape(frames, rows, wide, D).swapaxes(0, 1)
    arrived = arrived.reshape(tm, frames, rows, cols, D)
    edge_rows = edge_norm(info, arrived, spatial_gain)
    halo = lax.ppermute(edge_rows, "space", [(i, space - 1 - i) for i in range(space)])
    cot, arrived = lax.optimization_barrier((cot, arrived))
    cot = exchange(cot, "tm")
    qkv, tok = qkv_own(info, arrived, spatial_gain, spatial_heads)
    middle = spatial_phase(info, halo, qkv, tok, spatial_heads, spatial_merge)
    mid = swap(middle.reshape(frame_count, wide, D))
    core = jnp.stack([lax.axis_index("batch") & 1, here]).astype(jnp.int32)
    out, send, keep = temporal_phase(
        core, mid, frame_order.reshape(frame_count), temporal_gain, cot.reshape(frame_count, wide, D),
        temporal_heads, temporal_merge, space, tm,
    )
    batch = lax.axis_size("batch")
    got = lax.ppermute(send, "batch", [(i, i ^ 1) for i in range(batch)])
    output = exchange(out.reshape(tm, frames, wide, D), "tm").swapaxes(0, 1)
    chip = [keep[k].astype(F32) + got[k].astype(F32) for k in range(1, space)]
    moved = [lax.ppermute(chip[k - 1].astype(BF), "space", [(i, (i + k) % space) for i in range(space)])
             for k in range(1, space)]
    own = own_slot(keep, got)
    over_space = space_sum(own, moved)
    planes = [[(2 * y + c) * tm + t for y in range(batch // 2) for t in range(tm)] for c in range(2)]
    pieces = lax.all_to_all(
        over_space.reshape(2 * tm, *over_space.shape[2:]), ("batch", "tm"), split_axis=0, concat_axis=0,
        axis_index_groups=planes, tiled=True,
    )
    mine = pieces.astype(F32).sum(0).astype(BF)
    other = lax.ppermute(mine, "batch", [(i, i ^ 1) for i in range(batch)])
    weight_grad = jnp.where(
        core[0] == 0, jnp.concatenate([mine, other], axis=1), jnp.concatenate([other, mine], axis=1)
    ).astype(F32)
    return (output.reshape(1, frames, rows, wide, D), weight_grad)


def solution(mesh):
    in_specs = (
        P("batch", None, "space", "tm", None),
        P("batch", None),
        P("batch", "tm"),
        P(),
        P(),
        P(),
        P(),
        P(),
        P(),
        P("batch", "tm", "space", None, None),
    )
    out_specs = (P("batch", "tm", "space", None, None), P(("tm", "space"), None))

    return jax.shard_map(per_device, mesh=mesh, in_specs=in_specs, out_specs=out_specs, check_vma=False)
```
